32 devices in a mesh: stage: 1 (over z), dp: 4 (over y), fsdp: 4 (over x), tp: 2 (over core).
Axes of the slice: x: 4, y: 4, z: 1, core: 2. Of those that a mesh axis runs over, the one named last changes fastest.
The devices are a block of a 4x4x8 slice.
Arguments:
- weights: float32 [4, 512, 16384], P('stage', ('fsdp', 'dp'), 'tp')
- momenta: float32 [4, 512, 16384], P('stage', ('fsdp', 'dp'), 'tp')
- gradients: bfloat16 [4, 4, 512, 16384], P(('stage', 'dp'), None, 'fsdp', 'tp')
Outputs:
- output 1: float32 [4, 512, 16384], P('stage', ('fsdp', 'dp'), 'tp')
- output 2: float32 [4, 512, 16384], P('stage', ('fsdp', 'dp'), 'tp')
All inputs are finite; a program needn't handle non-finite values.
Results may differ from the reference program's by a relative error of at most 0.02.
Values are sent between devices in bfloat16 or wider.
A program may use at most 768 MiB of HBM per device.

```python
import math
import jax
import jax.numpy as jnp
from jax import lax

MATRICES = 4
ROW_DIM = 512
COL_DIM = 16384
REPLICAS = 4
RANK_LOW = 8
NS_STEPS = 5

MOMENTUM = 0.95
LEARN_RATE = 0.1
WEIGHT_DECAY = 0.1
COEF_A = 3.4445
COEF_B = -4.7750
COEF_C = 2.0315
NORM_EPS = 1e-7
UPDATE_SCALE = LEARN_RATE * 0.2 * math.sqrt(COL_DIM)
DECAY_FACTOR = 1.0 - LEARN_RATE * WEIGHT_DECAY


def spectral_draw(base_key, lead_shape):
    key_left, key_right, key_noise = jax.random.split(base_key, 3)
    left_fac = jax.random.normal(key_left, lead_shape + (ROW_DIM, RANK_LOW), jnp.float32)
    right_fac = jax.random.normal(key_right, lead_shape + (RANK_LOW, COL_DIM), jnp.float32)
    noise_part = jax.random.normal(key_noise, lead_shape + (ROW_DIM, COL_DIM), jnp.float32)
    low_part = jnp.einsum('...ir,...rj->...ij', left_fac, right_fac) / math.sqrt(RANK_LOW)
    return (low_part + noise_part) / math.sqrt(2.0)


def setup_inputs(seed: int = 0, part: int = 0) -> dict:
    base_key = jax.random.fold_in(jax.random.key(seed), part)
    key_w, key_m, key_g = jax.random.split(base_key, 3)
    weights = 0.02 * jax.random.normal(key_w, (MATRICES, ROW_DIM, COL_DIM), jnp.float32)
    momenta = 2.0 * spectral_draw(key_m, (MATRICES,))
    gradients = spectral_draw(key_g, (REPLICAS, MATRICES)) / math.sqrt(REPLICAS)
    return {'weights': weights, 'momenta': momenta, 'gradients': gradients.astype(jnp.bfloat16)}


def newton_schulz(x_mat):
    def ns_step(x_cur, unused):
        gram = jnp.dot(x_cur, x_cur.T, preferred_element_type=jnp.float32).astype(jnp.bfloat16)
        gram_sq = jnp.dot(gram, gram, preferred_element_type=jnp.float32).astype(jnp.bfloat16)
        poly_mat = (COEF_B * gram.astype(jnp.float32) + COEF_C * gram_sq.astype(jnp.float32)).astype(jnp.bfloat16)
        product = jnp.dot(poly_mat, x_cur, preferred_element_type=jnp.float32)
        x_next = (COEF_A * x_cur.astype(jnp.float32) + product).astype(jnp.bfloat16)
        return x_next, None
    return lax.scan(ns_step, x_mat, None, length=NS_STEPS)[0]


def muon_matrix(mat_trio):
    w_mat, m_mat, g_mat = mat_trio
    m_new = MOMENTUM * m_mat + g_mat
    x_zero = g_mat + MOMENTUM * m_new
    norm_val = jnp.sqrt(jnp.sum(x_zero * x_zero))
    x_mat = (x_zero / (norm_val + NORM_EPS)).astype(jnp.bfloat16)
    x_fin = newton_schulz(x_mat)
    w_new = DECAY_FACTOR * w_mat - UPDATE_SCALE * x_fin.astype(jnp.float32)
    return w_new, m_new


def reference(weights, momenta, gradients):
    grad_sum = jnp.sum(gradients.astype(jnp.float32), axis=0)
    w_new, m_new = lax.map(muon_matrix, (weights, momenta, grad_sum))
    return w_new, m_new
```

```python
import functools
import math
import jax
import jax.numpy as jnp
from jax import lax
from jax.experimental import pallas as pl
from jax.experimental.pallas import tpu as pltpu
from jax.sharding import PartitionSpec as P

MOMENTUM = 0.95
LEARN_RATE = 0.1
WEIGHT_DECAY = 0.1
COEF_A = 3.4445
COEF_B = -4.7750
COEF_C = 2.0315
NORM_EPS = 1e-7
NS_STEPS = 5
ROW_AXES = ('fsdp', 'dp')
F32 = jnp.float32
BF16 = jnp.bfloat16
MESH = pl.DeviceIdType.MESH
SIDE = 4
BLK = 128
TRI = ((0, 0), (0, 1), (1, 1), (0, 2), (0, 3), (1, 2), (1, 3), (2, 2), (2, 3), (3, 3))
SLOT = {ij: n for n, ij in enumerate(TRI)}
HALF = len(TRI) // 2


def muon_kernel(m_hbm, g_hbm, mnew_hbm, xfin_hbm,
                gown, grecv, relay, mbuf, x0, xrow, xfull, xfin,
                nown, npair, nall, part, drecv, red, rsrecv, agbuf, amat, bmat,
                load_sem, out_sem, gsend, grcv, nsend, nrcv, csend, crcv, bsend, brcv,
                dsend, drcv, rssend, rsrcv, agsend, agrcv, fwsend, fwrcv):
    n_mat, rows, cols = mbuf.shape
    quarter = cols // SIDE
    half = cols // 2
    y = lax.axis_index('dp')
    x = lax.axis_index('fsdp')
    t = lax.axis_index('tp')
    partner = {'tp': 1 - t}
    up = lax.rem(y + 1, SIDE)
    down = lax.rem(y + SIDE - 1, SIDE)
    far = lax.rem(y + 2, SIDE)

    def row_ds(i):
        return pl.ds(pl.multiple_of(i * rows, rows), rows)

    def quarter_ds(i):
        return pl.ds(pl.multiple_of(i * quarter, quarter), quarter)

    def mat_of(yy, xx):
        return (yy // 2) * 2 + xx // 2

    def pos_of(yy, xx):
        return (yy % 2) * 2 + xx % 2

    loads = []
    for k in range(n_mat):
        loads.append((pltpu.make_async_copy(g_hbm.at[k, row_ds(y), :], gown.at[k], load_sem.at[0, k]),
                      pltpu.make_async_copy(m_hbm.at[k], mbuf.at[k], load_sem.at[1, k])))
        for c in loads[-1]:
            c.start()

    others = [(oy, ox) for oy in range(SIDE) for ox in range(SIDE) if (oy, ox) != (0, 0)]

    def peer(off):
        return lax.rem(y + off[0], SIDE), lax.rem(x + off[1], SIDE)

    barrier = pltpu.get_barrier_semaphore()
    pl.semaphore_signal(barrier, inc=1, device_id=partner, device_id_type=MESH)
    for off in others:
        py, px = peer(off)
        pl.semaphore_signal(barrier, inc=1, device_id={'dp': py, 'fsdp': px}, device_id_type=MESH)
    pl.semaphore_wait(barrier, 1 + len(others))

    def remote(src, dst, ssem, rsem, dev):
        return pltpu.make_async_remote_copy(src_ref=src, dst_ref=dst, send_sem=ssem, recv_sem=rsem,
                                            device_id=dev, device_id_type=MESH)

    lo, hi = pl.ds(0, half), pl.ds(half, half)

    def grad_copies(k):
        to_up, to_down = {'dp': up}, {'dp': down}
        return (
            remote(g_hbm.at[k, row_ds(up), :], grecv.at[k, 0], gsend.at[k, 0], grcv.at[k, 0], to_up),
            remote(g_hbm.at[k, row_ds(down), :], grecv.at[k, 1], gsend.at[k, 1], grcv.at[k, 1], to_down),
            remote(g_hbm.at[k, row_ds(far), lo], relay.at[k, 0], gsend.at[k, 2], grcv.at[k, 2], to_up),
            remote(g_hbm.at[k, row_ds(far), hi], relay.at[k, 1], gsend.at[k, 3], grcv.at[k, 3], to_down),
            remote(relay.at[k, 0], grecv.at[k, 2, :, lo], gsend.at[k, 4], grcv.at[k, 4], to_up),
            remote(relay.at[k, 1], grecv.at[k, 2, :, hi], gsend.at[k, 5], grcv.at[k, 5], to_down),
        )

    gcopies = [grad_copies(k) for k in range(n_mat)]

    def issue_grad(k):
        for j in (2, 3, 0, 1):
            gcopies[k][j].start()

    issue_grad(0)
    issue_grad(1)
    step = min(512, cols)
    out_copies = []
    tile_rows = lax.broadcasted_iota(jnp.int32, (8, 128), 0)
    norm_tile = jnp.zeros((8, 128), F32)
    for k in range(n_mat):
        gcopies[k][2].wait_recv()
        gcopies[k][4].start()
        gcopies[k][3].wait_recv()
        gcopies[k][5].start()
        if k + 2 < n_mat:
            issue_grad(k + 2)
        for c in loads[k]:
            c.wait()
        for j in (0, 1, 4, 5):
            gcopies[k][j].wait_recv()

        def col_step(i, acc, k=k):
            cs = pl.ds(pl.multiple_of(i * step, step), step)
            g_sum = (gown[k, :, cs].astype(F32) + grecv[k, 0, :, cs].astype(F32)) + (
                grecv[k, 1, :, cs].astype(F32) + grecv[k, 2, :, cs].astype(F32))
            m_new = MOMENTUM * mbuf[k, :, cs] + g_sum
            mbuf[k, :, cs] = m_new
            x_zero = g_sum + MOMENTUM * m_new
            x0[k, :, cs] = x_zero
            return acc + x_zero * x_zero

        acc = lax.fori_loop(0, cols // step, col_step, jnp.zeros((rows, step), F32))
        norm_tile = jnp.where(tile_rows == k, jnp.sum(acc), norm_tile)
        oc = pltpu.make_async_copy(mbuf.at[k], mnew_hbm.at[k], out_sem.at[k])
        oc.start()
        out_copies.append(oc)

    nown[...] = norm_tile
    pair_copy = remote(nown, npair, nsend.at[0], nrcv.at[0], partner)
    pair_copy.start()
    pair_copy.wait_recv()
    here = y * SIDE + x
    nall[here] = nown[...] + npair[...]
    norm_copies = []
    for n, off in enumerate(others):
        py, px = peer(off)
        c = remote(nall.at[here], nall.at[here], nsend.at[1 + n], nrcv.at[1 + n], {'dp': py, 'fsdp': px})
        c.start()
        norm_copies.append(c)
    for c in norm_copies:
        c.wait_recv()
    sq_all = jnp.sum(nall[...], axis=0)
    denom_all = jnp.sqrt(sq_all) + NORM_EPS

    for k in range(n_mat):
        denom = denom_all[k:k + 1, 0:1]

        def div_step(i, carry, k=k, denom=denom):
            cs = pl.ds(pl.multiple_of(i * step, step), step)
            xrow[k, :, cs] = (x0[k, :, cs] / denom).astype(BF16)
            return carry

        lax.fori_loop(0, cols // step, div_step, 0)

    my_mat, my_pos, my_rows = mat_of(y, x), pos_of(y, x), x * SIDE + y
    col_copies = []
    for n, off in enumerate(others):
        py, px = peer(off)
        c = remote(xrow.at[mat_of(py, px), :, quarter_ds(pos_of(py, px))], xfull.at[row_ds(my_rows), :],
                   csend.at[n], crcv.at[n], {'dp': py, 'fsdp': px})
        c.start()
        col_copies.append(c)
    own = pltpu.make_async_copy(xrow.at[my_mat, :, quarter_ds(my_pos)], xfull.at[row_ds(my_rows), :], load_sem.at[0, 0])
    own.start()
    own.wait()
    for c in col_copies:
        c.wait_recv()

    fy, fx = y + 1 - 2 * (y % 2), x + 1 - 2 * (x % 2)
    square = ((y, fx), (fy, x), (fy, fx))
    chunk = HALF * BLK // 4

    def chunk_ds(pos):
        return pl.ds(pl.multiple_of(pos * chunk, chunk), chunk)

    def packed_ds(core, pos):
        return pl.ds(pl.multiple_of(core * (HALF * BLK) + pos * chunk, chunk), chunk)

    bcol = min(256, quarter)

    def pair_of(it):
        return remote(part.at[it, 1 - t], drecv.at[it], dsend.at[it], drcv.at[it], partner)

    def scatter_of(it, n):
        py, px = square[n]
        return remote(red.at[it, chunk_ds(pos_of(py, px)), :], rsrecv.at[it, n], rssend.at[it, n], rsrcv.at[it, n],
                      {'dp': py, 'fsdp': px})

    def gather_of(it, n):
        mine = agbuf.at[it, packed_ds(t, my_pos), :]
        py, px = square[n]
        return remote(mine, mine, agsend.at[it, n], agrcv.at[it, n], {'dp': py, 'fsdp': px})

    def forward_of(it, n):
        pos = my_pos if n == 0 else pos_of(*square[n - 1])
        held = agbuf.at[it, packed_ds(t, pos), :]
        return remote(held, held, fwsend.at[it, n], fwrcv.at[it, n], partner)

    def iteration(it, carry):
        for bi, bj in ((0, 0), (0, 1), (1, 1)):
            gram = lax.dot_general(xfull[2 * BLK * bi:2 * BLK * (bi + 1), :], xfull[2 * BLK * bj:2 * BLK * (bj + 1), :],
                                   (((1,), (1,)), ((), ())), preferred_element_type=F32)
            for a in range(2):
                for b in range(2):
                    n = SLOT.get((2 * bi + a, 2 * bj + b))
                    if n is not None:
                        part[it, n // HALF, (n % HALF) * BLK:(n % HALF + 1) * BLK, :] = (
                            gram[a * BLK:(a + 1) * BLK, b * BLK:(b + 1) * BLK])
        pair = pair_of(it)
        pair.start()
        pair.wait_recv()
        red[it] = part[it, t] + drecv[it]
        for n in range(3):
            scatter_of(it, n).start()
        for n in range(3):
            scatter_of(it, n).wait_recv()
        total = (red[it, chunk_ds(my_pos), :] + rsrecv[it, 0]) + (rsrecv[it, 1] + rsrecv[it, 2])
        agbuf[it, packed_ds(t, my_pos), :] = total.astype(BF16)
        for n in range(3):
            gather_of(it, n).start()
        forward_of(it, 0).start()
        for n in range(3):
            gather_of(it, n).wait_recv()
            forward_of(it, n + 1).start()
        for n in range(4):
            forward_of(it, n).wait_recv()
        for n, (bi, bj) in enumerate(TRI):
            block = agbuf[it, n * BLK:(n + 1) * BLK, :]
            amat[bi * BLK:(bi + 1) * BLK, bj * BLK:(bj + 1) * BLK] = block
            if bi != bj:
                amat[bj * BLK:(bj + 1) * BLK, bi * BLK:(bi + 1) * BLK] = block.astype(F32).T.astype(BF16)
        for bi in range(2):
            rs = slice(2 * BLK * bi, 2 * BLK * (bi + 1))
            sq = jnp.dot(amat[rs, :], amat[...], preferred_element_type=F32).astype(BF16)
            bmat[rs, :] = (COEF_B * amat[rs, :].astype(F32) + COEF_C * sq.astype(F32)).astype(BF16)

        def col_block(i, c2):
            cs = pl.ds(pl.multiple_of(i * bcol, bcol), bcol)
            x_old = xfull[:, cs]
            prod = jnp.dot(bmat[...], x_old, preferred_element_type=F32)
            xfull[:, cs] = (COEF_A * x_old.astype(F32) + prod).astype(BF16)
            return c2

        lax.fori_loop(0, quarter // bcol, col_block, 0)
        return carry

    for c in col_copies:
        c.wait_send()
    lax.fori_loop(0, NS_STEPS, iteration, 0)

    back_copies = []
    for n, off in enumerate(others):
        py, px = peer(off)
        c = remote(xfull.at[row_ds(px * SIDE + py), :], xfin.at[my_mat, :, quarter_ds(my_pos)],
                   bsend.at[n], brcv.at[n], {'dp': py, 'fsdp': px})
        c.start()
        back_copies.append(c)
    own = pltpu.make_async_copy(xfull.at[row_ds(my_rows), :], xfin.at[my_mat, :, quarter_ds(my_pos)], load_sem.at[0, 0])
    own.start()
    own.wait()
    for c in back_copies:
        c.wait_recv()
    fin = pltpu.make_async_copy(xfin, xfin_hbm, load_sem.at[0, 0])
    fin.start()

    for k in range(n_mat):
        for c in gcopies[k]:
            c.wait_send()
        out_copies[k].wait()
    pair_copy.wait_send()
    for c in norm_copies + back_copies:
        c.wait_send()

    def drain(it, carry):
        pair_of(it).wait_send()
        for n in range(3):
            scatter_of(it, n).wait_send()
            gather_of(it, n).wait_send()
        for n in range(4):
            forward_of(it, n).wait_send()
        return carry

    lax.fori_loop(0, NS_STEPS, drain, 0)
    fin.wait()


def run_kernel(m_blk, g_blk):
    n_mat, rows, cols = m_blk.shape
    all_rows = rows * SIDE * SIDE
    quarter = cols // SIDE
    packed = len(TRI) * BLK
    chunk = packed // 8
    n_oth = SIDE * SIDE - 1
    dma = pltpu.SemaphoreType.DMA
    scratch = [
        pltpu.VMEM((n_mat, rows, cols), BF16),
        pltpu.VMEM((n_mat, 3, rows, cols), BF16),
        pltpu.VMEM((n_mat, 2, rows, cols // 2), BF16),
        pltpu.VMEM((n_mat, rows, cols), F32),
        pltpu.VMEM((n_mat, rows, cols), F32),
        pltpu.VMEM((n_mat, rows, cols), BF16),
        pltpu.VMEM((all_rows, quarter), BF16),
        pltpu.VMEM((n_mat, rows, cols), BF16),
        pltpu.VMEM((8, 128), F32),
        pltpu.VMEM((8, 128), F32),
        pltpu.VMEM((SIDE * SIDE, 8, 128), F32),
        pltpu.VMEM((NS_STEPS, 2, packed // 2, BLK), F32),
        pltpu.VMEM((NS_STEPS, packed // 2, BLK), F32),
        pltpu.VMEM((NS_STEPS, packed // 2, BLK), F32),
        pltpu.VMEM((NS_STEPS, 3, chunk, BLK), F32),
        pltpu.VMEM((NS_STEPS, packed, BLK), BF16),
        pltpu.VMEM((all_rows, all_rows), BF16),
        pltpu.VMEM((all_rows, all_rows), BF16),
        dma((2, n_mat)), dma((n_mat,)), dma((n_mat, 6)), dma((n_mat, 6)),
        dma((n_oth + 1,)), dma((n_oth + 1,)), dma((n_oth,)), dma((n_oth,)), dma((n_oth,)), dma((n_oth,)),
        dma((NS_STEPS,)), dma((NS_STEPS,)), dma((NS_STEPS, 3)), dma((NS_STEPS, 3)),
        dma((NS_STEPS, 3)), dma((NS_STEPS, 3)), dma((NS_STEPS, 4)), dma((NS_STEPS, 4)),
    ]
    anyspace = pl.BlockSpec(memory_space=pl.ANY)
    return pl.pallas_call(
        muon_kernel,
        out_shape=(jax.ShapeDtypeStruct(m_blk.shape, F32), jax.ShapeDtypeStruct(m_blk.shape, BF16)),
        in_specs=[anyspace, anyspace],
        out_specs=(anyspace, anyspace),
        scratch_shapes=scratch,
        compiler_params=pltpu.CompilerParams(collective_id=0, has_side_effects=True, vmem_limit_bytes=60 * 2 ** 20),
        name='muon_group',
    )(m_blk, g_blk)


def solution(mesh):
    mat_spec = P('stage', ROW_AXES, 'tp')
    grad_spec = P(('stage', 'dp'), None, 'fsdp', 'tp')
    tp_size = mesh.shape['tp']

    def local_step(w_blk, m_blk, g_blk):
        m_new, x_fin = run_kernel(m_blk, g_blk.reshape(g_blk.shape[1:]))
        col_count = w_blk.shape[2] * tp_size
        update_scale = LEARN_RATE * 0.2 * math.sqrt(col_count)
        decay_factor = 1.0 - LEARN_RATE * WEIGHT_DECAY
        w_new = decay_factor * w_blk - update_scale * x_fin.astype(F32)
        return w_new, m_new

    return jax.shard_map(local_step, mesh=mesh, in_specs=(mat_spec, mat_spec, grad_spec), out_specs=(mat_spec, mat_spec), check_vma=False)
```

```python
import functools
import math
import jax
import jax.numpy as jnp
from jax import lax
from jax.experimental import pallas as pl
from jax.experimental.pallas import tpu as pltpu
from jax.sharding import PartitionSpec as P

MOMENTUM = 0.95
LEARN_RATE = 0.1
WEIGHT_DECAY = 0.1
COEF_A = 3.4445
COEF_B = -4.7750
COEF_C = 2.0315
NORM_EPS = 1e-7
NS_STEPS = 5
ROW_AXES = ('fsdp', 'dp')
F32 = jnp.float32
BF16 = jnp.bfloat16
MESH = pl.DeviceIdType.MESH
VMEM_MIB = 44
SIDE = 4
BLK = 128
TRI = ((0, 0), (0, 1), (1, 1), (0, 2), (0, 3), (1, 2), (1, 3), (2, 2), (2, 3), (3, 3))
SLOT = {ij: n for n, ij in enumerate(TRI)}
HALF = len(TRI) // 2
RELAYED = (((0, 3), (0, 2)), ((0, 3), (1, 2)), ((3, 0), (2, 0)), ((3, 0), (2, 1)))


def muon_kernel(m_hbm, g_hbm, mnew_hbm, xfin_hbm,
                gown, grecv, relay, mbuf, x0, xrow, xfull, xfin,
                nown, npair, nall, part, drecv, red, rsrecv, agbuf, amat, bmat, cheld, bheld,
                load_sem, out_sem, gsend, grcv, nsend, nrcv, csend, crcv, bsend, brcv,
                dsend, drcv, rssend, rsrcv, agsend, agrcv, fwsend, fwrcv, chsem, bhsem):
    n_mat, rows, cols = mbuf.shape
    quarter = cols // SIDE
    half = cols // 2
    y = lax.axis_index('dp')
    x = lax.axis_index('fsdp')
    t = lax.axis_index('tp')
    partner = {'tp': 1 - t}
    up = lax.rem(y + 1, SIDE)
    down = lax.rem(y + SIDE - 1, SIDE)
    far = lax.rem(y + 2, SIDE)

    def row_ds(i):
        return pl.ds(pl.multiple_of(i * rows, rows), rows)

    def quarter_ds(i):
        return pl.ds(pl.multiple_of(i * quarter, quarter), quarter)

    def mat_of(yy, xx):
        return (yy // 2) * 2 + xx // 2

    def pos_of(yy, xx):
        return (yy % 2) * 2 + xx % 2

    loads = []
    for k in range(n_mat):
        loads.append((pltpu.make_async_copy(g_hbm.at[k, row_ds(y), :], gown.at[k], load_sem.at[0, k]),
                      pltpu.make_async_copy(m_hbm.at[k], mbuf.at[k], load_sem.at[1, k])))
        for c in loads[-1]:
            c.start()

    others = [(oy, ox) for oy in range(SIDE) for ox in range(SIDE) if (oy, ox) != (0, 0)]

    def peer(off):
        return lax.rem(y + off[0], SIDE), lax.rem(x + off[1], SIDE)

    barrier = pltpu.get_barrier_semaphore()
    pl.semaphore_signal(barrier, inc=1, device_id=partner, device_id_type=MESH)
    for off in others:
        py, px = peer(off)
        pl.semaphore_signal(barrier, inc=1, device_id={'dp': py, 'fsdp': px}, device_id_type=MESH)
    pl.semaphore_wait(barrier, 1 + len(others))

    def remote(src, dst, ssem, rsem, dev):
        return pltpu.make_async_remote_copy(src_ref=src, dst_ref=dst, send_sem=ssem, recv_sem=rsem,
                                            device_id=dev, device_id_type=MESH)

    lo, hi = pl.ds(0, half), pl.ds(half, half)

    def grad_copies(k):
        to_up, to_down = {'dp': up}, {'dp': down}
        return (
            remote(g_hbm.at[k, row_ds(up), :], grecv.at[k, 0], gsend.at[k, 0], grcv.at[k, 0], to_up),
            remote(g_hbm.at[k, row_ds(down), :], grecv.at[k, 1], gsend.at[k, 1], grcv.at[k, 1], to_down),
            remote(g_hbm.at[k, row_ds(far), lo], relay.at[k, 0], gsend.at[k, 2], grcv.at[k, 2], to_up),
            remote(g_hbm.at[k, row_ds(far), hi], relay.at[k, 1], gsend.at[k, 3], grcv.at[k, 3], to_down),
            remote(relay.at[k, 0], grecv.at[k, 2, :, lo], gsend.at[k, 4], grcv.at[k, 4], to_up),
            remote(relay.at[k, 1], grecv.at[k, 2, :, hi], gsend.at[k, 5], grcv.at[k, 5], to_down),
        )

    gcopies = [grad_copies(k) for k in range(n_mat)]

    def issue_grad(k):
        for j in (2, 3, 0, 1):
            gcopies[k][j].start()

    issue_grad(0)
    issue_grad(1)
    step = min(512, cols)
    out_copies = []
    tile_rows = lax.broadcasted_iota(jnp.int32, (8, 128), 0)
    norm_tile = jnp.zeros((8, 128), F32)
    for k in range(n_mat):
        gcopies[k][2].wait_recv()
        gcopies[k][4].start()
        gcopies[k][3].wait_recv()
        gcopies[k][5].start()
        if k + 2 < n_mat:
            issue_grad(k + 2)
        for c in loads[k]:
            c.wait()
        for j in (0, 1, 4, 5):
            gcopies[k][j].wait_recv()

        def col_step(i, acc, k=k):
            cs = pl.ds(pl.multiple_of(i * step, step), step)
            g_sum = (gown[k, :, cs].astype(F32) + grecv[k, 0, :, cs].astype(F32)) + (
                grecv[k, 1, :, cs].astype(F32) + grecv[k, 2, :, cs].astype(F32))
            m_new = MOMENTUM * mbuf[k, :, cs] + g_sum
            mbuf[k, :, cs] = m_new
            x_zero = g_sum + MOMENTUM * m_new
            x0[k, :, cs] = x_zero
            return acc + x_zero * x_zero

        acc = lax.fori_loop(0, cols // step, col_step, jnp.zeros((rows, step), F32))
        norm_tile = jnp.where(tile_rows == k, jnp.sum(acc), norm_tile)
        oc = pltpu.make_async_copy(mbuf.at[k], mnew_hbm.at[k], out_sem.at[k])
        oc.start()
        out_copies.append(oc)

    nown[...] = norm_tile
    pair_copy = remote(nown, npair, nsend.at[0], nrcv.at[0], partner)
    pair_copy.start()
    pair_copy.wait_recv()
    here = y * SIDE + x
    nall[here] = nown[...] + npair[...]
    norm_copies = []
    for n, off in enumerate(others):
        py, px = peer(off)
        c = remote(nall.at[here], nall.at[here], nsend.at[1 + n], nrcv.at[1 + n], {'dp': py, 'fsdp': px})
        c.start()
        norm_copies.append(c)
    for c in norm_copies:
        c.wait_recv()
    sq_all = jnp.sum(nall[...], axis=0)
    denom_all = jnp.sqrt(sq_all) + NORM_EPS

    for k in range(n_mat):
        denom = denom_all[k:k + 1, 0:1]

        def div_step(i, carry, k=k, denom=denom):
            cs = pl.ds(pl.multiple_of(i * step, step), step)
            xrow[k, :, cs] = (x0[k, :, cs] / denom).astype(BF16)
            return carry

        lax.fori_loop(0, cols // step, div_step, 0)

    def exchange(src_of, dst_of, held, ssem, rsem, hsem):
        def to(off):
            py, px = peer(off)
            return {'dp': py, 'fsdp': px}

        def origin(off):
            return lax.rem(y + SIDE - off[0], SIDE), lax.rem(x + SIDE - off[1], SIDE)

        first, second, direct = [], [], []
        for n, (station, off) in enumerate(RELAYED):
            i = others.index(off)
            first.append(remote(src_of(*peer(off)), held.at[n], hsem.at[0, n], hsem.at[1, n], to(station)))
            hop = ((off[0] - station[0]) % SIDE, (off[1] - station[1]) % SIDE)
            second.append(remote(held.at[n], dst_of(*origin(station)), ssem.at[i], rsem.at[i], to(hop)))
        relayed = [off for _, off in RELAYED]
        for i, off in enumerate(others):
            if off not in relayed:
                direct.append(remote(src_of(*peer(off)), dst_of(y, x), ssem.at[i], rsem.at[i], to(off)))
        for c in first + direct:
            c.start()
        own = pltpu.make_async_copy(src_of(y, x), dst_of(y, x), load_sem.at[0, 0])
        own.start()
        for c, f in zip(first, second):
            c.wait_recv()
            f.start()
        own.wait()
        for c in direct + second:
            c.wait_recv()
        return first + second + direct

    my_mat, my_pos, my_rows = mat_of(y, x), pos_of(y, x), x * SIDE + y
    col_copies = exchange(lambda py, px: xrow.at[mat_of(py, px), :, quarter_ds(pos_of(py, px))],
                          lambda oy, ox: xfull.at[row_ds(ox * SIDE + oy), :], cheld, csend, crcv, chsem)

    fy, fx = y + 1 - 2 * (y % 2), x + 1 - 2 * (x % 2)
    square = ((y, fx), (fy, x), (fy, fx))
    chunk = HALF * BLK // 4

    def chunk_ds(pos):
        return pl.ds(pl.multiple_of(pos * chunk, chunk), chunk)

    def packed_ds(core, pos):
        return pl.ds(pl.multiple_of(core * (HALF * BLK) + pos * chunk, chunk), chunk)

    bcol = min(256, quarter)

    def pair_of(it):
        return remote(part.at[it, 1 - t], drecv.at[it], dsend.at[it], drcv.at[it], partner)

    def scatter_of(it, n):
        py, px = square[n]
        return remote(red.at[it, chunk_ds(pos_of(py, px)), :], rsrecv.at[it, n], rssend.at[it, n], rsrcv.at[it, n],
                      {'dp': py, 'fsdp': px})

    def gather_of(it, n):
        mine = agbuf.at[it, packed_ds(t, my_pos), :]
        py, px = square[n]
        return remote(mine, mine, agsend.at[it, n], agrcv.at[it, n], {'dp': py, 'fsdp': px})

    def forward_of(it, n):
        pos = my_pos if n == 0 else pos_of(*square[n - 1])
        held = agbuf.at[it, packed_ds(t, pos), :]
        return remote(held, held, fwsend.at[it, n], fwrcv.at[it, n], partner)

    def iteration(it, carry):
        for bi, bj in ((0, 0), (0, 1), (1, 1)):
            gram = lax.dot_general(xfull[2 * BLK * bi:2 * BLK * (bi + 1), :], xfull[2 * BLK * bj:2 * BLK * (bj + 1), :],
                                   (((1,), (1,)), ((), ())), preferred_element_type=F32)
            for a in range(2):
                for b in range(2):
                    n = SLOT.get((2 * bi + a, 2 * bj + b))
                    if n is not None:
                        part[it, n // HALF, (n % HALF) * BLK:(n % HALF + 1) * BLK, :] = (
                            gram[a * BLK:(a + 1) * BLK, b * BLK:(b + 1) * BLK])
        pair = pair_of(it)
        pair.start()
        pair.wait_recv()
        red[it] = part[it, t] + drecv[it]
        for n in range(3):
            scatter_of(it, n).start()
        for n in range(3):
            scatter_of(it, n).wait_recv()
        total = (red[it, chunk_ds(my_pos), :] + rsrecv[it, 0]) + (rsrecv[it, 1] + rsrecv[it, 2])
        agbuf[it, packed_ds(t, my_pos), :] = total.astype(BF16)
        for n in range(3):
            gather_of(it, n).start()
        forward_of(it, 0).start()
        for n in range(3):
            gather_of(it, n).wait_recv()
            forward_of(it, n + 1).start()
        for n in range(4):
            forward_of(it, n).wait_recv()
        for n, (bi, bj) in enumerate(TRI):
            block = agbuf[it, n * BLK:(n + 1) * BLK, :]
            amat[bi * BLK:(bi + 1) * BLK, bj * BLK:(bj + 1) * BLK] = block
            if bi != bj:
                amat[bj * BLK:(bj + 1) * BLK, bi * BLK:(bi + 1) * BLK] = block.astype(F32).T.astype(BF16)
        for bi in range(2):
            rs = slice(2 * BLK * bi, 2 * BLK * (bi + 1))
            sq = jnp.dot(amat[rs, :], amat[...], preferred_element_type=F32).astype(BF16)
            bmat[rs, :] = (COEF_B * amat[rs, :].astype(F32) + COEF_C * sq.astype(F32)).astype(BF16)

        for i in range(quarter // bcol):
            cs = slice(i * bcol, (i + 1) * bcol)
            x_old = xfull[:, cs]
            prod = jnp.dot(bmat[...], x_old, preferred_element_type=F32)
            xfull[:, cs] = (COEF_A * x_old.astype(F32) + prod).astype(BF16)
        return carry

    for c in col_copies:
        c.wait_send()
    lax.fori_loop(0, NS_STEPS, iteration, 0)

    back_copies = exchange(lambda py, px: xfull.at[row_ds(px * SIDE + py), :],
                           lambda oy, ox: xfin.at[mat_of(oy, ox), :, quarter_ds(pos_of(oy, ox))], bheld, bsend, brcv, bhsem)
    fin = pltpu.make_async_copy(xfin, xfin_hbm, load_sem.at[0, 0])
    fin.start()

    for k in range(n_mat):
        for c in gcopies[k]:
            c.wait_send()
        out_copies[k].wait()
    pair_copy.wait_send()
    for c in norm_copies + back_copies:
        c.wait_send()

    def drain(it, carry):
        pair_of(it).wait_send()
        for n in range(3):
            scatter_of(it, n).wait_send()
            gather_of(it, n).wait_send()
        for n in range(4):
            forward_of(it, n).wait_send()
        return carry

    lax.fori_loop(0, NS_STEPS, drain, 0)
    fin.wait()


def run_kernel(m_blk, g_blk):
    n_mat, rows, cols = m_blk.shape
    all_rows = rows * SIDE * SIDE
    quarter = cols // SIDE
    packed = len(TRI) * BLK
    chunk = packed // 8
    n_oth = SIDE * SIDE - 1
    dma = pltpu.SemaphoreType.DMA
    scratch = [
        pltpu.VMEM((n_mat, rows, cols), BF16),
        pltpu.VMEM((n_mat, 3, rows, cols), BF16),
        pltpu.VMEM((n_mat, 2, rows, cols // 2), BF16),
        pltpu.VMEM((n_mat, rows, cols), F32),
        pltpu.VMEM((n_mat, rows, cols), F32),
        pltpu.VMEM((n_mat, rows, cols), BF16),
        pltpu.VMEM((all_rows, quarter), BF16),
        pltpu.VMEM((n_mat, rows, cols), BF16),
        pltpu.VMEM((8, 128), F32),
        pltpu.VMEM((8, 128), F32),
        pltpu.VMEM((SIDE * SIDE, 8, 128), F32),
        pltpu.VMEM((NS_STEPS, 2, packed // 2, BLK), F32),
        pltpu.VMEM((NS_STEPS, packed // 2, BLK), F32),
        pltpu.VMEM((NS_STEPS, packed // 2, BLK), F32),
        pltpu.VMEM((NS_STEPS, 3, chunk, BLK), F32),
        pltpu.VMEM((NS_STEPS, packed, BLK), BF16),
        pltpu.VMEM((all_rows, all_rows), BF16),
        pltpu.VMEM((all_rows, all_rows), BF16),
        pltpu.VMEM((len(RELAYED), rows, quarter), BF16),
        pltpu.VMEM((len(RELAYED), rows, quarter), BF16),
        dma((2, n_mat)), dma((n_mat,)), dma((n_mat, 6)), dma((n_mat, 6)),
        dma((n_oth + 1,)), dma((n_oth + 1,)), dma((n_oth,)), dma((n_oth,)), dma((n_oth,)), dma((n_oth,)),
        dma((NS_STEPS,)), dma((NS_STEPS,)), dma((NS_STEPS, 3)), dma((NS_STEPS, 3)),
        dma((NS_STEPS, 3)), dma((NS_STEPS, 3)), dma((NS_STEPS, 4)), dma((NS_STEPS, 4)),
        dma((2, len(RELAYED))), dma((2, len(RELAYED))),
    ]
    anyspace = pl.BlockSpec(memory_space=pl.ANY)
    return pl.pallas_call(
        muon_kernel,
        out_shape=(jax.ShapeDtypeStruct(m_blk.shape, F32), jax.ShapeDtypeStruct(m_blk.shape, BF16)),
        in_specs=[anyspace, anyspace],
        out_specs=(anyspace, anyspace),
        scratch_shapes=scratch,
        compiler_params=pltpu.CompilerParams(collective_id=0, has_side_effects=True, vmem_limit_bytes=VMEM_MIB * 2 ** 20),
        name='muon_group',
    )(m_blk, g_blk)


def solution(mesh):
    mat_spec = P('stage', ROW_AXES, 'tp')
    grad_spec = P(('stage', 'dp'), None, 'fsdp', 'tp')
    tp_size = mesh.shape['tp']

    def local_step(w_blk, m_blk, g_blk):
        m_new, x_fin = run_kernel(m_blk, g_blk.reshape(g_blk.shape[1:]))
        col_count = w_blk.shape[2] * tp_size
        update_scale = LEARN_RATE * 0.2 * math.sqrt(col_count)
        decay_factor = 1.0 - LEARN_RATE * WEIGHT_DECAY
        w_new = decay_factor * w_blk - update_scale * x_fin.astype(F32)
        return w_new, m_new

    return jax.shard_map(local_step, mesh=mesh, in_specs=(mat_spec, mat_spec, grad_spec), out_specs=(mat_spec, mat_spec), check_vma=False)
```

```python
import functools
import math
import jax
import jax.numpy as jnp
from jax import lax
from jax.experimental import pallas as pl
from jax.experimental.pallas import tpu as pltpu
from jax.sharding import PartitionSpec as P

MOMENTUM = 0.95
LEARN_RATE = 0.1
WEIGHT_DECAY = 0.1
COEF_A = 3.4445
COEF_B = -4.7750
COEF_C = 2.0315
NORM_EPS = 1e-7
NS_STEPS = 5
ROW_AXES = ('fsdp', 'dp')
F32 = jnp.float32
BF16 = jnp.bfloat16
MESH = pl.DeviceIdType.MESH
VMEM_MIB = 47
SIDE = 4
BLK = 128
TRI = ((0, 0), (0, 1), (1, 1), (0, 2), (0, 3), (2, 2), (2, 3), (3, 3), (1, 2), (1, 3))
HALF = len(TRI) // 2


def muon_kernel(m_hbm, g_hbm, mnew_hbm, xfin_hbm,
                gown, grecv, relay, mbuf, x0, xrow, xfull, xfin,
                nown, npair, nall, part, drecv, red, rsrecv, agbuf, amat, bmat,
                cmid, chold1, chold2, bmid, bhold1, bhold2,
                load_sem, out_sem, gsend, grcv, nsend, nrcv, csend, cmsem, ch1sem, ch2sem, cfsem,
                bsend, bmsem, bh1sem, bh2sem, bfsem,
                dsend, drcv, rssend, rsrcv, agsend, agrcv, fwsend, fwrcv):
    n_mat, rows, cols = mbuf.shape
    quarter = cols // SIDE
    half = cols // 2
    y = lax.axis_index('dp')
    x = lax.axis_index('fsdp')
    t = lax.axis_index('tp')
    partner = {'tp': 1 - t}
    up = lax.rem(y + 1, SIDE)
    down = lax.rem(y + SIDE - 1, SIDE)
    far = lax.rem(y + 2, SIDE)

    def row_ds(i):
        return pl.ds(pl.multiple_of(i * rows, rows), rows)

    def quarter_ds(i):
        return pl.ds(pl.multiple_of(i * quarter, quarter), quarter)

    def mat_of(yy, xx):
        return (yy // 2) * 2 + xx // 2

    def pos_of(yy, xx):
        return (yy % 2) * 2 + xx % 2

    loads = []
    for k in range(n_mat):
        loads.append((pltpu.make_async_copy(g_hbm.at[k, row_ds(y), :], gown.at[k], load_sem.at[0, k]),
                      pltpu.make_async_copy(m_hbm.at[k], mbuf.at[k], load_sem.at[1, k])))
        for c in loads[-1]:
            c.start()

    others = [(oy, ox) for oy in range(SIDE) for ox in range(SIDE) if (oy, ox) != (0, 0)]

    def peer(off):
        return lax.rem(y + off[0], SIDE), lax.rem(x + off[1], SIDE)

    barrier = pltpu.get_barrier_semaphore()
    pl.semaphore_signal(barrier, inc=1, device_id=partner, device_id_type=MESH)
    for off in others:
        py, px = peer(off)
        pl.semaphore_signal(barrier, inc=1, device_id={'dp': py, 'fsdp': px}, device_id_type=MESH)
    pl.semaphore_wait(barrier, 1 + len(others))

    def remote(src, dst, ssem, rsem, dev):
        return pltpu.make_async_remote_copy(src_ref=src, dst_ref=dst, send_sem=ssem, recv_sem=rsem,
                                            device_id=dev, device_id_type=MESH)

    lo, hi = pl.ds(0, half), pl.ds(half, half)

    def grad_copies(k):
        to_up, to_down = {'dp': up}, {'dp': down}
        return (
            remote(g_hbm.at[k, row_ds(up), :], grecv.at[k, 0], gsend.at[k, 0], grcv.at[k, 0], to_up),
            remote(g_hbm.at[k, row_ds(down), :], grecv.at[k, 1], gsend.at[k, 1], grcv.at[k, 1], to_down),
            remote(g_hbm.at[k, row_ds(far), lo], relay.at[k, 0], gsend.at[k, 2], grcv.at[k, 2], to_up),
            remote(g_hbm.at[k, row_ds(far), hi], relay.at[k, 1], gsend.at[k, 3], grcv.at[k, 3], to_down),
            remote(relay.at[k, 0], grecv.at[k, 2, :, lo], gsend.at[k, 4], grcv.at[k, 4], to_up),
            remote(relay.at[k, 1], grecv.at[k, 2, :, hi], gsend.at[k, 5], grcv.at[k, 5], to_down),
        )

    gcopies = [grad_copies(k) for k in range(n_mat)]

    def issue_grad(k):
        for j in (2, 3, 0, 1):
            gcopies[k][j].start()

    issue_grad(0)
    issue_grad(1)
    step = min(512, cols)
    out_copies = []
    tile_rows = lax.broadcasted_iota(jnp.int32, (8, 128), 0)
    norm_tile = jnp.zeros((8, 128), F32)
    for k in range(n_mat):
        gcopies[k][2].wait_recv()
        gcopies[k][4].start()
        gcopies[k][3].wait_recv()
        gcopies[k][5].start()
        if k + 2 < n_mat:
            issue_grad(k + 2)
        for c in loads[k]:
            c.wait()
        for j in (0, 1, 4, 5):
            gcopies[k][j].wait_recv()

        def col_step(i, acc, k=k):
            cs = pl.ds(pl.multiple_of(i * step, step), step)
            g_sum = (gown[k, :, cs].astype(F32) + grecv[k, 0, :, cs].astype(F32)) + (
                grecv[k, 1, :, cs].astype(F32) + grecv[k, 2, :, cs].astype(F32))
            m_new = MOMENTUM * mbuf[k, :, cs] + g_sum
            mbuf[k, :, cs] = m_new
            x_zero = g_sum + MOMENTUM * m_new
            x0[k, :, cs] = x_zero
            return acc + x_zero * x_zero

        acc = lax.fori_loop(0, cols // step, col_step, jnp.zeros((rows, step), F32))
        norm_tile = jnp.where(tile_rows == k, jnp.sum(acc), norm_tile)
        oc = pltpu.make_async_copy(mbuf.at[k], mnew_hbm.at[k], out_sem.at[k])
        oc.start()
        out_copies.append(oc)

    nown[...] = norm_tile
    pair_copy = remote(nown, npair, nsend.at[0], nrcv.at[0], partner)
    pair_copy.start()
    pair_copy.wait_recv()
    here = y * SIDE + x
    nall[here] = nown[...] + npair[...]
    norm_copies = []
    for n, off in enumerate(others):
        py, px = peer(off)
        c = remote(nall.at[here], nall.at[here], nsend.at[1 + n], nrcv.at[1 + n], {'dp': py, 'fsdp': px})
        c.start()
        norm_copies.append(c)
    for c in norm_copies:
        c.wait_recv()
    sq_all = jnp.sum(nall[...], axis=0)
    denom_all = jnp.sqrt(sq_all) + NORM_EPS

    for k in range(n_mat):
        denom = denom_all[k:k + 1, 0:1]

        def div_step(i, carry, k=k, denom=denom):
            cs = pl.ds(pl.multiple_of(i * step, step), step)
            xrow[k, :, cs] = (x0[k, :, cs] / denom).astype(BF16)
            return carry

        lax.fori_loop(0, cols // step, div_step, 0)

    def exchange(src_of, dst_of, dst_all, mid, hold1, hold2, ssem, msem, h1sem, h2sem, fsem):
        sends = []

        def send(src, dst, rsem, dev):
            c = remote(src, dst, ssem.at[len(sends)], rsem, dev)
            c.start()
            sends.append(c)

        locals_ = []
        ways = []
        for h in range(2):
            p, q = (x, y) if h == 0 else (y, x)
            near = [(lax.rem(c + 1, SIDE), lax.rem(c + SIDE - 1, SIDE), lax.rem(c + 2, SIDE)) for c in (p, q)]

            def yx(pp, qq, h=h):
                return (qq, pp) if h == 0 else (pp, qq)

            def dev(pp, qq, yx=yx):
                return dict(zip(('dp', 'fsdp'), yx(pp, qq)))

            def src(pp, qq, h=h, yx=yx):
                return src_of(*yx(pp, qq), h)

            def dst(pp, qq, h=h, yx=yx):
                return dst_of(*yx(pp, qq), h)

            ways.append((p, q, near[0], near[1], dev, src, dst))

        def second(h, o, piece):
            p, q, (pu, pd, pf), (qu, qd, qf), dev, src, dst = ways[h]
            start_p = (pd, pu, pf, p)[o]
            send(piece(qu), dst(start_p, q), fsem, dev(p, qu))
            send(piece(qd), dst(start_p, q), fsem, dev(p, qd))
            side, i = ((0, 1), (1, 0), (1, 1), (0, 0))[o]
            send(piece(qf), hold2.at[h, side, i], h2sem.at[h, side, i], dev(p, (qu, qd)[side]))
            c = pltpu.make_async_copy(piece(q), dst(start_p, q), fsem)
            c.start()

        def relay2(h, o):
            p, q, (pu, pd, pf), (qu, qd, qf), dev, src, dst = ways[h]
            start_p = (pd, pu, pf, p)[o]
            side, i = ((0, 1), (1, 0), (1, 1), (0, 0))[o]
            held = hold2.at[h, side, i]
            pltpu.make_async_copy(held, held, h2sem.at[h, side, i]).wait()
            send(held, dst(start_p, (qd, qu)[side]), fsem, dev(p, (qu, qd)[side]))

        for h in range(2):
            p, q, (pu, pd, pf), _, dev, src, dst = ways[h]
            for side, to in ((0, pu), (1, pd)):
                for i in range(2):
                    send(src(pf, 2 * side + i), hold1.at[h, side, i], h1sem.at[h, side], dev(to, q))
        for i in range(SIDE):
            for h in range(2):
                p, q, (pu, pd, pf), _, dev, src, dst = ways[h]
                for side, to in ((0, pu), (1, pd)):
                    send(src(to, i), mid.at[h, side, i], msem.at[h, side], dev(to, q))
        for h in range(2):
            second(h, 3, lambda qq, h=h: ways[h][5](ways[h][0], qq))
        for h in range(2):
            p, q, (pu, pd, pf), _, dev, src, dst = ways[h]
            for side, to in ((0, pu), (1, pd)):
                held = hold1.at[h, side]
                pltpu.make_async_copy(held, held, h1sem.at[h, side]).wait()
                send(held, mid.at[h, 2, 2 * side:2 * side + 2], msem.at[h, 2 + side], dev(to, q))
        for side in range(2):
            for h in range(2):
                got = mid.at[h, side]
                pltpu.make_async_copy(got, got, msem.at[h, side]).wait()
                second(h, side, lambda qq, h=h, side=side: mid.at[h, side, qq])
        for h in range(2):
            relay2(h, 3)
        for h in range(2):
            for side in range(2):
                got = mid.at[h, 2, 2 * side:2 * side + 2]
                pltpu.make_async_copy(got, got, msem.at[h, 2 + side]).wait()
            second(h, 2, lambda qq, h=h: mid.at[h, 2, qq])
        for o in (0, 1, 2):
            for h in range(2):
                relay2(h, o)
        pltpu.make_async_copy(dst_all, dst_all, fsem).wait()
        return sends

    half_piece = quarter // 2

    def piece_ds(pos, h):
        return pl.ds(pl.multiple_of(pos * quarter + h * half_piece, half_piece), half_piece)

    my_mat, my_pos = mat_of(y, x), pos_of(y, x)
    col_copies = exchange(lambda py, px, h: xrow.at[mat_of(py, px), :, piece_ds(pos_of(py, px), h)],
                          lambda oy, ox, h: xfull.at[row_ds(ox * SIDE + oy), h * half_piece:(h + 1) * half_piece],
                          xfull, cmid, chold1, chold2, csend, cmsem, ch1sem, ch2sem, cfsem)

    fy, fx = y + 1 - 2 * (y % 2), x + 1 - 2 * (x % 2)
    square = ((y, fx), (fy, x), (fy, fx))
    chunk = HALF * BLK // 4

    def chunk_ds(pos):
        return pl.ds(pl.multiple_of(pos * chunk, chunk), chunk)

    def packed_ds(core, pos):
        return pl.ds(pl.multiple_of(core * (HALF * BLK) + pos * chunk, chunk), chunk)

    bcol = min(256, quarter)

    def pair_of(it):
        return remote(part.at[it, 1 - t], drecv.at[it], dsend.at[it], drcv.at[it], partner)

    def scatter_of(it, n):
        py, px = square[n]
        return remote(red.at[it, chunk_ds(pos_of(py, px)), :], rsrecv.at[it, n], rssend.at[it, n], rsrcv.at[it, n],
                      {'dp': py, 'fsdp': px})

    def gather_of(it, n):
        mine = agbuf.at[it, packed_ds(t, my_pos), :]
        py, px = square[n]
        return remote(mine, mine, agsend.at[it, n], agrcv.at[it, n], {'dp': py, 'fsdp': px})

    def forward_of(it, n):
        pos = my_pos if n == 0 else pos_of(*square[n - 1])
        held = agbuf.at[it, packed_ds(t, pos), :]
        return remote(held, held, fwsend.at[it, n], fwrcv.at[it, n], partner)

    def half_gram(it, h):
        nt = (((1,), (1,)), ((), ()))
        pair_rows = xfull[pl.ds(pl.multiple_of(h * 2 * BLK, 2 * BLK), 2 * BLK), :]
        square_gram = lax.dot_general(pair_rows, pair_rows, nt, preferred_element_type=F32)
        cross_gram = lax.dot_general(xfull[pl.ds(pl.multiple_of(h * BLK, BLK), BLK), :], xfull[2 * BLK:, :], nt,
                                     preferred_element_type=F32)
        blocks = (square_gram[:BLK, :BLK], square_gram[:BLK, BLK:], square_gram[BLK:, BLK:],
                  cross_gram[:, :BLK], cross_gram[:, BLK:])
        for n, block in enumerate(blocks):
            part[it, h, n * BLK:(n + 1) * BLK, :] = block

    def iteration(it, carry):
        half_gram(it, 1 - t)
        pair = pair_of(it)
        pair.start()
        half_gram(it, t)
        pair.wait_recv()
        red[it] = part[it, t] + drecv[it]
        for n in range(3):
            scatter_of(it, n).start()
        for n in range(3):
            scatter_of(it, n).wait_recv()
        total = (red[it, chunk_ds(my_pos), :] + rsrecv[it, 0]) + (rsrecv[it, 1] + rsrecv[it, 2])
        agbuf[it, packed_ds(t, my_pos), :] = total.astype(BF16)
        for n in range(3):
            gather_of(it, n).start()
        forward_of(it, 0).start()
        for n in range(3):
            gather_of(it, n).wait_recv()
            forward_of(it, n + 1).start()
        for n in range(4):
            forward_of(it, n).wait_recv()
        for n, (bi, bj) in enumerate(TRI):
            block = agbuf[it, n * BLK:(n + 1) * BLK, :]
            amat[bi * BLK:(bi + 1) * BLK, bj * BLK:(bj + 1) * BLK] = block
            if bi != bj:
                amat[bj * BLK:(bj + 1) * BLK, bi * BLK:(bi + 1) * BLK] = block.astype(F32).T.astype(BF16)
        for bi in range(2):
            rs = slice(2 * BLK * bi, 2 * BLK * (bi + 1))
            sq = jnp.dot(amat[rs, :], amat[...], preferred_element_type=F32).astype(BF16)
            bmat[rs, :] = (COEF_B * amat[rs, :].astype(F32) + COEF_C * sq.astype(F32)).astype(BF16)

        for i in range(quarter // bcol):
            cs = slice(i * bcol, (i + 1) * bcol)
            x_old = xfull[:, cs]
            prod = jnp.dot(bmat[...], x_old, preferred_element_type=F32)
            xfull[:, cs] = (COEF_A * x_old.astype(F32) + prod).astype(BF16)
        return carry

    for c in col_copies:
        c.wait_send()
    lax.fori_loop(0, NS_STEPS, iteration, 0)

    back_copies = exchange(lambda py, px, h: xfull.at[row_ds(px * SIDE + py), h * half_piece:(h + 1) * half_piece],
                           lambda oy, ox, h: xfin.at[mat_of(oy, ox), :, piece_ds(pos_of(oy, ox), h)],
                           xfin, bmid, bhold1, bhold2, bsend, bmsem, bh1sem, bh2sem, bfsem)
    fin = pltpu.make_async_copy(xfin, xfin_hbm, load_sem.at[0, 0])
    fin.start()

    for k in range(n_mat):
        for c in gcopies[k]:
            c.wait_send()
        out_copies[k].wait()
    pair_copy.wait_send()
    for c in norm_copies + back_copies:
        c.wait_send()

    def drain(it, carry):
        pair_of(it).wait_send()
        for n in range(3):
            scatter_of(it, n).wait_send()
            gather_of(it, n).wait_send()
        for n in range(4):
            forward_of(it, n).wait_send()
        return carry

    lax.fori_loop(0, NS_STEPS, drain, 0)
    fin.wait()


def run_kernel(m_blk, g_blk):
    n_mat, rows, cols = m_blk.shape
    all_rows = rows * SIDE * SIDE
    quarter = cols // SIDE
    packed = len(TRI) * BLK
    chunk = packed // 8
    n_oth = SIDE * SIDE - 1
    dma = pltpu.SemaphoreType.DMA
    half_piece = (rows, quarter // 2)
    relays = [
        pltpu.VMEM((2, 3, SIDE) + half_piece, BF16),
        pltpu.VMEM((2, 2, 2) + half_piece, BF16),
        pltpu.VMEM((2, 2, 2) + half_piece, BF16),
    ]
    relay_sems = [dma((60,)), dma((2, 4)), dma((2, 2)), dma((2, 2, 2)), dma]
    scratch = [
        pltpu.VMEM((n_mat, rows, cols), BF16),
        pltpu.VMEM((n_mat, 3, rows, cols), BF16),
        pltpu.VMEM((n_mat, 2, rows, cols // 2), BF16),
        pltpu.VMEM((n_mat, rows, cols), F32),
        pltpu.VMEM((n_mat, rows, cols), F32),
        pltpu.VMEM((n_mat, rows, cols), BF16),
        pltpu.VMEM((all_rows, quarter), BF16),
        pltpu.VMEM((n_mat, rows, cols), BF16),
        pltpu.VMEM((8, 128), F32),
        pltpu.VMEM((8, 128), F32),
        pltpu.VMEM((SIDE * SIDE, 8, 128), F32),
        pltpu.VMEM((NS_STEPS, 2, packed // 2, BLK), F32),
        pltpu.VMEM((NS_STEPS, packed // 2, BLK), F32),
        pltpu.VMEM((NS_STEPS, packed // 2, BLK), F32),
        pltpu.VMEM((NS_STEPS, 3, chunk, BLK), F32),
        pltpu.VMEM((NS_STEPS, packed, BLK), BF16),
        pltpu.VMEM((all_rows, all_rows), BF16),
        pltpu.VMEM((all_rows, all_rows), BF16),
        *relays, *relays,
        dma((2, n_mat)), dma((n_mat,)), dma((n_mat, 6)), dma((n_mat, 6)),
        dma((n_oth + 1,)), dma((n_oth + 1,)), *relay_sems, *relay_sems,
        dma((NS_STEPS,)), dma((NS_STEPS,)), dma((NS_STEPS, 3)), dma((NS_STEPS, 3)),
        dma((NS_STEPS, 3)), dma((NS_STEPS, 3)), dma((NS_STEPS, 4)), dma((NS_STEPS, 4)),
    ]
    anyspace = pl.BlockSpec(memory_space=pl.ANY)
    return pl.pallas_call(
        muon_kernel,
        out_shape=(jax.ShapeDtypeStruct(m_blk.shape, F32), jax.ShapeDtypeStruct(m_blk.shape, BF16)),
        in_specs=[anyspace, anyspace],
        out_specs=(anyspace, anyspace),
        scratch_shapes=scratch,
        compiler_params=pltpu.CompilerParams(collective_id=0, has_side_effects=True, vmem_limit_bytes=VMEM_MIB * 2 ** 20),
        name='muon_group',
    )(m_blk, g_blk)


def solution(mesh):
    mat_spec = P('stage', ROW_AXES, 'tp')
    grad_spec = P(('stage', 'dp'), None, 'fsdp', 'tp')
    tp_size = mesh.shape['tp']

    def local_step(w_blk, m_blk, g_blk):
        m_new, x_fin = run_kernel(m_blk, g_blk.reshape(g_blk.shape[1:]))
        col_count = w_blk.shape[2] * tp_size
        update_scale = LEARN_RATE * 0.2 * math.sqrt(col_count)
        decay_factor = 1.0 - LEARN_RATE * WEIGHT_DECAY
        w_new = decay_factor * w_blk - update_scale * x_fin.astype(F32)
        return w_new, m_new

    return jax.shard_map(local_step, mesh=mesh, in_specs=(mat_spec, mat_spec, grad_spec), out_specs=(mat_spec, mat_spec), check_vma=False)
```

```python
import functools
import math
import jax
import jax.numpy as jnp
from jax import lax
from jax.experimental import pallas as pl
from jax.experimental.pallas import tpu as pltpu
from jax.sharding import PartitionSpec as P

MOMENTUM = 0.95
LEARN_RATE = 0.1
WEIGHT_DECAY = 0.1
COEF_A = 3.4445
COEF_B = -4.7750
COEF_C = 2.0315
NORM_EPS = 1e-7
NS_STEPS = 5
ROW_AXES = ('fsdp', 'dp')
F32 = jnp.float32
BF16 = jnp.bfloat16
MESH = pl.DeviceIdType.MESH
VMEM_MIB = 47
SIDE = 4
BLK = 128
TRI = ((0, 0), (0, 1), (1, 1), (0, 2), (0, 3), (2, 2), (2, 3), (3, 3), (1, 2), (1, 3))
HALF = len(TRI) // 2
PLACE = ((0, 1), (1, 0), (1, 1), (0, 0))


def muon_kernel(m_hbm, g_hbm, mnew_hbm, xfin_hbm,
                gown, grecv, relay, mbuf, x0, xrow, xfull,
                nown, npair, nall, part, drecv, red, rsrecv, agbuf, amat, bmat,
                cmid, chold1, chold2, bmid, bhold1, bhold2,
                load_sem, out_sem, gsend, grcv, nsend, nrcv, csend, cmsem, ch1sem, ch2sem, cfsem,
                bsend, bmsem, bh1sem, bh2sem, bfsem,
                dsend, drcv, rssend, rsrcv, agsend, agrcv, fwsend, fwrcv, round_sem):
    n_mat, rows, cols = mbuf.shape
    quarter = cols // SIDE
    half = cols // 2
    y = lax.axis_index('dp')
    x = lax.axis_index('fsdp')
    t = lax.axis_index('tp')
    partner = {'tp': 1 - t}
    up = lax.rem(y + 1, SIDE)
    down = lax.rem(y + SIDE - 1, SIDE)
    far = lax.rem(y + 2, SIDE)

    def row_ds(i):
        return pl.ds(pl.multiple_of(i * rows, rows), rows)

    def quarter_ds(i):
        return pl.ds(pl.multiple_of(i * quarter, quarter), quarter)

    def mat_of(yy, xx):
        return (yy // 2) * 2 + xx // 2

    def pos_of(yy, xx):
        return (yy % 2) * 2 + xx % 2

    loads = []
    for k in range(n_mat):
        loads.append((pltpu.make_async_copy(g_hbm.at[k, row_ds(y), :], gown.at[k], load_sem.at[0, k]),
                      pltpu.make_async_copy(m_hbm.at[k], mbuf.at[k], load_sem.at[1, k])))
        for c in loads[-1]:
            c.start()

    others = [(oy, ox) for oy in range(SIDE) for ox in range(SIDE) if (oy, ox) != (0, 0)]

    def peer(off):
        return lax.rem(y + off[0], SIDE), lax.rem(x + off[1], SIDE)

    xup, xdown = lax.rem(x + 1, SIDE), lax.rem(x + SIDE - 1, SIDE)
    neighbours = ({'dp': up}, {'dp': down}, {'fsdp': xup}, {'fsdp': xdown})
    barrier = pltpu.get_barrier_semaphore()
    for dev in neighbours + (partner,):
        pl.semaphore_signal(barrier, inc=1, device_id=dev, device_id_type=MESH)
    pl.semaphore_wait(barrier, 5)

    def remote(src, dst, ssem, rsem, dev):
        return pltpu.make_async_remote_copy(src_ref=src, dst_ref=dst, send_sem=ssem, recv_sem=rsem,
                                            device_id=dev, device_id_type=MESH)

    lo, hi = pl.ds(0, half), pl.ds(half, half)

    def grad_copies(k):
        to_up, to_down = {'dp': up}, {'dp': down}
        return (
            remote(g_hbm.at[k, row_ds(up), :], grecv.at[k, 0], gsend.at[k, 0], grcv.at[k, 0], to_up),
            remote(g_hbm.at[k, row_ds(down), :], grecv.at[k, 1], gsend.at[k, 1], grcv.at[k, 1], to_down),
            remote(g_hbm.at[k, row_ds(far), lo], relay.at[k, 0], gsend.at[k, 2], grcv.at[k, 2], to_up),
            remote(g_hbm.at[k, row_ds(far), hi], relay.at[k, 1], gsend.at[k, 3], grcv.at[k, 3], to_down),
            remote(relay.at[k, 0], grecv.at[k, 2, :, lo], gsend.at[k, 4], grcv.at[k, 4], to_up),
            remote(relay.at[k, 1], grecv.at[k, 2, :, hi], gsend.at[k, 5], grcv.at[k, 5], to_down),
        )

    gcopies = [grad_copies(k) for k in range(n_mat)]

    def issue_grad(k):
        for j in (2, 3, 0, 1):
            gcopies[k][j].start()

    issue_grad(0)
    issue_grad(1)
    for n in range(3):
        for dev in neighbours:
            pl.semaphore_signal(round_sem.at[n], inc=1, device_id=dev, device_id_type=MESH)
        pl.semaphore_wait(round_sem.at[n], 4)
    step = min(512, cols)
    out_copies = []
    tile_rows = lax.broadcasted_iota(jnp.int32, (8, 128), 0)
    norm_tile = jnp.zeros((8, 128), F32)
    for k in range(n_mat):
        gcopies[k][2].wait_recv()
        gcopies[k][4].start()
        gcopies[k][3].wait_recv()
        gcopies[k][5].start()
        if k + 2 < n_mat:
            issue_grad(k + 2)
        for c in loads[k]:
            c.wait()
        for j in (0, 1, 4, 5):
            gcopies[k][j].wait_recv()

        def col_step(i, acc, k=k):
            cs = pl.ds(pl.multiple_of(i * step, step), step)
            g_sum = (gown[k, :, cs].astype(F32) + grecv[k, 0, :, cs].astype(F32)) + (
                grecv[k, 1, :, cs].astype(F32) + grecv[k, 2, :, cs].astype(F32))
            m_new = MOMENTUM * mbuf[k, :, cs] + g_sum
            mbuf[k, :, cs] = m_new
            x_zero = g_sum + MOMENTUM * m_new
            x0[k, :, cs] = x_zero
            return acc + x_zero * x_zero

        acc = lax.fori_loop(0, cols // step, col_step, jnp.zeros((rows, step), F32))
        norm_tile = jnp.where(tile_rows == k, jnp.sum(acc), norm_tile)
        oc = pltpu.make_async_copy(mbuf.at[k], mnew_hbm.at[k], out_sem.at[k])
        oc.start()
        out_copies.append(oc)

    nown[...] = norm_tile
    pair_copy = remote(nown, npair, nsend.at[0], nrcv.at[0], partner)
    pair_copy.start()
    pair_copy.wait_recv()
    here = y * SIDE + x
    nall[here] = nown[...] + npair[...]
    norm_copies = []
    for n, off in enumerate(others):
        py, px = peer(off)
        c = remote(nall.at[here], nall.at[here], nsend.at[1 + n], nrcv.at[1 + n], {'dp': py, 'fsdp': px})
        c.start()
        norm_copies.append(c)
    for c in norm_copies:
        c.wait_recv()
    sq_all = jnp.sum(nall[...], axis=0)
    denom_all = jnp.sqrt(sq_all) + NORM_EPS

    for k in range(n_mat):
        denom = denom_all[k:k + 1, 0:1]

        def div_step(i, carry, k=k, denom=denom):
            cs = pl.ds(pl.multiple_of(i * step, step), step)
            xrow[k, :, cs] = (x0[k, :, cs] / denom).astype(BF16)
            return carry

        lax.fori_loop(0, cols // step, div_step, 0)

    def exchange(src_of, dst_of, dst_all, mid, hold1, hold2, ssem, msem, h1sem, h2sem, fsem, idle):
        sends = []

        def send(src, dst, rsem, dev):
            c = remote(src, dst, ssem.at[len(sends)], rsem, dev)
            c.start()
            sends.append(c)

        ways = []
        for h in range(2):
            p, q = (x, y) if h == 0 else (y, x)
            near = [(lax.rem(c + 1, SIDE), lax.rem(c + SIDE - 1, SIDE), lax.rem(c + 2, SIDE)) for c in (p, q)]

            def yx(pp, qq, h=h):
                return (qq, pp) if h == 0 else (pp, qq)

            def dev(pp, qq, yx=yx):
                return dict(zip(('dp', 'fsdp'), yx(pp, qq)))

            def src(pp, qq, h=h, yx=yx):
                return src_of(*yx(pp, qq), h)

            def dst(pp, qq, h=h, yx=yx):
                return dst_of(*yx(pp, qq), h)

            ways.append((p, q, near[0], near[1], dev, src, dst))

        def second(h, o, piece):
            p, q, (pu, pd, pf), (qu, qd, qf), dev, src, dst = ways[h]
            start_p = (pd, pu, pf, p)[o]
            side, i = PLACE[o]
            send(piece(qf), hold2.at[h, side, i], h2sem.at[h, side, i], dev(p, (qu, qd)[side]))
            send(piece(qu), dst(start_p, q), fsem, dev(p, qu))
            send(piece(qd), dst(start_p, q), fsem, dev(p, qd))
            pltpu.make_async_copy(piece(q), dst(start_p, q), fsem).start()

        def relay2(h, o):
            p, q, (pu, pd, pf), (qu, qd, qf), dev, src, dst = ways[h]
            side, i = PLACE[o]
            held = hold2.at[h, side, i]
            pltpu.make_async_copy(held, held, h2sem.at[h, side, i]).wait()
            send(held, dst((pd, pu, pf, p)[o], (qd, qu)[side]), fsem, dev(p, (qu, qd)[side]))

        def near_pieces(i):
            for h in range(2):
                p, q, (pu, pd, pf), _, dev, src, dst = ways[h]
                for side, to in ((0, pu), (1, pd)):
                    send(src(to, i), mid.at[h, side, i], msem.at[h, side], dev(to, q))

        for h in range(2):
            p, q, (pu, pd, pf), _, dev, src, dst = ways[h]
            for side, to in ((0, pu), (1, pd)):
                for i in range(2):
                    send(src(pf, 2 * side + i), hold1.at[h, side, i], h1sem.at[h, side], dev(to, q))
        near_pieces(0)
        near_pieces(1)
        idle()
        for h in range(2):
            p, q, (pu, pd, pf), _, dev, src, dst = ways[h]
            for side, to in ((0, pu), (1, pd)):
                held = hold1.at[h, side]
                pltpu.make_async_copy(held, held, h1sem.at[h, side]).wait()
                send(held, mid.at[h, 2, 2 * side:2 * side + 2], msem.at[h, 2 + side], dev(to, q))
        near_pieces(2)
        near_pieces(3)
        for h in range(2):
            second(h, 3, lambda qq, h=h: ways[h][5](ways[h][0], qq))
        for h in range(2):
            for side in range(2):
                got = mid.at[h, 2, 2 * side:2 * side + 2]
                pltpu.make_async_copy(got, got, msem.at[h, 2 + side]).wait()
            second(h, 2, lambda qq, h=h: mid.at[h, 2, qq])
        for side in range(2):
            for h in range(2):
                got = mid.at[h, side]
                pltpu.make_async_copy(got, got, msem.at[h, side]).wait()
                second(h, side, lambda qq, h=h, side=side: mid.at[h, side, qq])
        for o in (3, 2, 0, 1):
            for h in range(2):
                relay2(h, o)
        pltpu.make_async_copy(dst_all, dst_all, fsem).wait()
        return sends

    half_piece = quarter // 2

    def piece_ds(pos, h):
        return pl.ds(pl.multiple_of(pos * quarter + h * half_piece, half_piece), half_piece)

    def idle_first():
        for k in range(n_mat):
            for c in gcopies[k]:
                c.wait_send()
            out_copies[k].wait()
        for c in [pair_copy] + norm_copies:
            c.wait_send()

    my_mat, my_pos = mat_of(y, x), pos_of(y, x)
    col_copies = exchange(lambda py, px, h: xrow.at[mat_of(py, px), :, piece_ds(pos_of(py, px), h)],
                          lambda oy, ox, h: xfull.at[row_ds(ox * SIDE + oy), h * half_piece:(h + 1) * half_piece],
                          xfull, cmid, chold1, chold2, csend, cmsem, ch1sem, ch2sem, cfsem, idle_first)

    fy, fx = y + 1 - 2 * (y % 2), x + 1 - 2 * (x % 2)
    square = ((y, fx), (fy, x), (fy, fx))
    chunk = HALF * BLK // 4

    def chunk_ds(pos):
        return pl.ds(pl.multiple_of(pos * chunk, chunk), chunk)

    def packed_ds(core, pos):
        return pl.ds(pl.multiple_of(core * (HALF * BLK) + pos * chunk, chunk), chunk)

    bcol = min(256, quarter)

    def pair_of(it):
        return remote(part.at[it, 1 - t], drecv.at[it], dsend.at[it], drcv.at[it], partner)

    def scatter_of(it, n):
        py, px = square[n]
        return remote(red.at[it, chunk_ds(pos_of(py, px)), :], rsrecv.at[it, n], rssend.at[it, n], rsrcv.at[it, n],
                      {'dp': py, 'fsdp': px})

    def gather_of(it, n):
        mine = agbuf.at[it, packed_ds(t, my_pos), :]
        py, px = square[n]
        return remote(mine, mine, agsend.at[it, n], agrcv.at[it, n], {'dp': py, 'fsdp': px})

    def forward_of(it, n):
        pos = my_pos if n == 0 else pos_of(*square[n - 1])
        held = agbuf.at[it, packed_ds(t, pos), :]
        return remote(held, held, fwsend.at[it, n], fwrcv.at[it, n], partner)

    def drain(it):
        pair_of(it).wait_send()
        for n in range(3):
            scatter_of(it, n).wait_send()
            gather_of(it, n).wait_send()
        for n in range(4):
            forward_of(it, n).wait_send()

    def half_gram(it, h):
        nt = (((1,), (1,)), ((), ()))
        pair_rows = xfull[pl.ds(pl.multiple_of(h * 2 * BLK, 2 * BLK), 2 * BLK), :]
        square_gram = lax.dot_general(pair_rows, pair_rows, nt, preferred_element_type=F32)
        cross_gram = lax.dot_general(xfull[pl.ds(pl.multiple_of(h * BLK, BLK), BLK), :], xfull[2 * BLK:, :], nt,
                                     preferred_element_type=F32)
        blocks = (square_gram[:BLK, :BLK], square_gram[:BLK, BLK:], square_gram[BLK:, BLK:],
                  cross_gram[:, :BLK], cross_gram[:, BLK:])
        for n, block in enumerate(blocks):
            part[it, h, n * BLK:(n + 1) * BLK, :] = block

    def iteration(it, carry):
        half_gram(it, 1 - t)
        pair = pair_of(it)
        pair.start()
        half_gram(it, t)
        pair.wait_recv()
        red[it] = part[it, t] + drecv[it]
        for n in range(3):
            scatter_of(it, n).start()

        @pl.when(it > 0)
        def _():
            drain(it - 1)

        for n in range(3):
            scatter_of(it, n).wait_recv()
        total = (red[it, chunk_ds(my_pos), :] + rsrecv[it, 0]) + (rsrecv[it, 1] + rsrecv[it, 2])
        agbuf[it, packed_ds(t, my_pos), :] = total.astype(BF16)
        for n in range(3):
            gather_of(it, n).start()
        forward_of(it, 0).start()
        for n in range(3):
            gather_of(it, n).wait_recv()
            forward_of(it, n + 1).start()
        for n in range(4):
            forward_of(it, n).wait_recv()
        for n, (bi, bj) in enumerate(TRI):
            block = agbuf[it, n * BLK:(n + 1) * BLK, :]
            amat[bi * BLK:(bi + 1) * BLK, bj * BLK:(bj + 1) * BLK] = block
            if bi != bj:
                amat[bj * BLK:(bj + 1) * BLK, bi * BLK:(bi + 1) * BLK] = block.astype(F32).T.astype(BF16)
        for bi in range(2):
            rs = slice(2 * BLK * bi, 2 * BLK * (bi + 1))
            sq = jnp.dot(amat[rs, :], amat[...], preferred_element_type=F32).astype(BF16)
            bmat[rs, :] = (COEF_B * amat[rs, :].astype(F32) + COEF_C * sq.astype(F32)).astype(BF16)

        for i in range(quarter // bcol):
            cs = slice(i * bcol, (i + 1) * bcol)
            x_old = xfull[:, cs]
            prod = jnp.dot(bmat[...], x_old, preferred_element_type=F32)
            xfull[:, cs] = (COEF_A * x_old.astype(F32) + prod).astype(BF16)
        return carry

    for c in col_copies:
        c.wait_send()
    lax.fori_loop(0, NS_STEPS, iteration, 0)

    back_copies = exchange(lambda py, px, h: xfull.at[row_ds(px * SIDE + py), h * half_piece:(h + 1) * half_piece],
                           lambda oy, ox, h: xfin_hbm.at[mat_of(oy, ox), :, piece_ds(pos_of(oy, ox), h)],
                           xfin_hbm, bmid, bhold1, bhold2, bsend, bmsem, bh1sem, bh2sem, bfsem, lambda: drain(NS_STEPS - 1))

    for c in back_copies:
        c.wait_send()


def run_kernel(m_blk, g_blk):
    n_mat, rows, cols = m_blk.shape
    all_rows = rows * SIDE * SIDE
    quarter = cols // SIDE
    packed = len(TRI) * BLK
    chunk = packed // 8
    n_oth = SIDE * SIDE - 1
    dma = pltpu.SemaphoreType.DMA
    half_piece = (rows, quarter // 2)
    relays = [
        pltpu.VMEM((2, 3, SIDE) + half_piece, BF16),
        pltpu.VMEM((2, 2, 2) + half_piece, BF16),
        pltpu.VMEM((2, 2, 2) + half_piece, BF16),
    ]
    relay_sems = [dma((60,)), dma((2, 4)), dma((2, 2)), dma((2, 2, 2)), dma]
    scratch = [
        pltpu.VMEM((n_mat, rows, cols), BF16),
        pltpu.VMEM((n_mat, 3, rows, cols), BF16),
        pltpu.VMEM((n_mat, 2, rows, cols // 2), BF16),
        pltpu.VMEM((n_mat, rows, cols), F32),
        pltpu.VMEM((n_mat, rows, cols), F32),
        pltpu.VMEM((n_mat, rows, cols), BF16),
        pltpu.VMEM((all_rows, quarter), BF16),
        pltpu.VMEM((8, 128), F32),
        pltpu.VMEM((8, 128), F32),
        pltpu.VMEM((SIDE * SIDE, 8, 128), F32),
        pltpu.VMEM((NS_STEPS, 2, packed // 2, BLK), F32),
        pltpu.VMEM((NS_STEPS, packed // 2, BLK), F32),
        pltpu.VMEM((NS_STEPS, packed // 2, BLK), F32),
        pltpu.VMEM((NS_STEPS, 3, chunk, BLK), F32),
        pltpu.VMEM((NS_STEPS, packed, BLK), BF16),
        pltpu.VMEM((all_rows, all_rows), BF16),
        pltpu.VMEM((all_rows, all_rows), BF16),
        *relays, *relays,
        dma((2, n_mat)), dma((n_mat,)), dma((n_mat, 6)), dma((n_mat, 6)),
        dma((n_oth + 1,)), dma((n_oth + 1,)), *relay_sems, *relay_sems,
        dma((NS_STEPS,)), dma((NS_STEPS,)), dma((NS_STEPS, 3)), dma((NS_STEPS, 3)),
        dma((NS_STEPS, 3)), dma((NS_STEPS, 3)), dma((NS_STEPS, 4)), dma((NS_STEPS, 4)), pltpu.SemaphoreType.REGULAR((3,)),
    ]
    anyspace = pl.BlockSpec(memory_space=pl.ANY)
    return pl.pallas_call(
        muon_kernel,
        out_shape=(jax.ShapeDtypeStruct(m_blk.shape, F32), jax.ShapeDtypeStruct(m_blk.shape, BF16)),
        in_specs=[anyspace, anyspace],
        out_specs=(anyspace, anyspace),
        scratch_shapes=scratch,
        compiler_params=pltpu.CompilerParams(collective_id=0, has_side_effects=True, vmem_limit_bytes=VMEM_MIB * 2 ** 20),
        name='muon_group',
    )(m_blk, g_blk)


def solution(mesh):
    mat_spec = P('stage', ROW_AXES, 'tp')
    grad_spec = P(('stage', 'dp'), None, 'fsdp', 'tp')
    tp_size = mesh.shape['tp']

    def local_step(w_blk, m_blk, g_blk):
        m_new, x_fin = run_kernel(m_blk, g_blk.reshape(g_blk.shape[1:]))
        col_count = w_blk.shape[2] * tp_size
        update_scale = LEARN_RATE * 0.2 * math.sqrt(col_count)
        decay_factor = 1.0 - LEARN_RATE * WEIGHT_DECAY
        w_new = decay_factor * w_blk - update_scale * x_fin.astype(F32)
        return w_new, m_new

    return jax.shard_map(local_step, mesh=mesh, in_specs=(mat_spec, mat_spec, grad_spec), out_specs=(mat_spec, mat_spec), check_vma=False)
```

```python
import functools
import math
import jax
import jax.numpy as jnp
from jax import lax
from jax.experimental import pallas as pl
from jax.experimental.pallas import tpu as pltpu
from jax.sharding import PartitionSpec as P

MOMENTUM = 0.95
LEARN_RATE = 0.1
WEIGHT_DECAY = 0.1
COEF_A = 3.4445
COEF_B = -4.7750
COEF_C = 2.0315
NORM_EPS = 1e-7
NS_STEPS = 5
ROW_AXES = ('fsdp', 'dp')
F32 = jnp.float32
BF16 = jnp.bfloat16
MESH = pl.DeviceIdType.MESH
VMEM_MIB = 47
SIDE = 4
BLK = 128
TRI = ((0, 0), (0, 1), (1, 1), (0, 2), (0, 3), (2, 2), (2, 3), (3, 3), (1, 2), (1, 3))
HALF = len(TRI) // 2
PLACE = ((0, 1), (1, 0), (1, 1), (0, 0))


def muon_kernel(m_hbm, g_hbm, mnew_hbm, xfin_hbm,
                gown, grecv, relay, mbuf, x0, xrow, xfull,
                nown, npair, nall, part, drecv, red, comb, rsrecv, agbuf, amat, bmat,
                cmid, chold1, chold2, bmid, bhold1, bhold2,
                load_sem, out_sem, gsend, grcv, nsend, nrcv, csend, cmsem, ch1sem, ch2sem, cfsem,
                bsend, bmsem, bh1sem, bh2sem, bfsem,
                dsend, drcv, rssend, rsrcv, agsend, agrcv, fwsend, fwrcv, round_sem):
    n_mat, rows, cols = mbuf.shape
    quarter = cols // SIDE
    half = cols // 2
    y = lax.axis_index('dp')
    x = lax.axis_index('fsdp')
    t = lax.axis_index('tp')
    partner = {'tp': 1 - t}
    up = lax.rem(y + 1, SIDE)
    down = lax.rem(y + SIDE - 1, SIDE)
    far = lax.rem(y + 2, SIDE)

    def row_ds(i):
        return pl.ds(pl.multiple_of(i * rows, rows), rows)

    def quarter_ds(i):
        return pl.ds(pl.multiple_of(i * quarter, quarter), quarter)

    def mat_of(yy, xx):
        return (yy // 2) * 2 + xx // 2

    def pos_of(yy, xx):
        return (yy % 2) * 2 + xx % 2

    loads = []
    for k in range(n_mat):
        loads.append((pltpu.make_async_copy(g_hbm.at[k, row_ds(y), :], gown.at[k], load_sem.at[0, k]),
                      pltpu.make_async_copy(m_hbm.at[k], mbuf.at[k], load_sem.at[1, k])))
        for c in loads[-1]:
            c.start()

    others = [(oy, ox) for oy in range(SIDE) for ox in range(SIDE) if (oy, ox) != (0, 0)]

    def peer(off):
        return lax.rem(y + off[0], SIDE), lax.rem(x + off[1], SIDE)

    xup, xdown = lax.rem(x + 1, SIDE), lax.rem(x + SIDE - 1, SIDE)
    neighbours = ({'dp': up}, {'dp': down}, {'fsdp': xup}, {'fsdp': xdown})
    barrier = pltpu.get_barrier_semaphore()
    for dev in neighbours + (partner,):
        pl.semaphore_signal(barrier, inc=1, device_id=dev, device_id_type=MESH)
    pl.semaphore_wait(barrier, 5)

    def remote(src, dst, ssem, rsem, dev):
        return pltpu.make_async_remote_copy(src_ref=src, dst_ref=dst, send_sem=ssem, recv_sem=rsem,
                                            device_id=dev, device_id_type=MESH)

    lo, hi = pl.ds(0, half), pl.ds(half, half)

    def grad_copies(k):
        to_up, to_down = {'dp': up}, {'dp': down}
        return (
            remote(g_hbm.at[k, row_ds(up), :], grecv.at[k, 0], gsend.at[k, 0], grcv.at[k, 0], to_up),
            remote(g_hbm.at[k, row_ds(down), :], grecv.at[k, 1], gsend.at[k, 1], grcv.at[k, 1], to_down),
            remote(g_hbm.at[k, row_ds(far), lo], relay.at[k, 0], gsend.at[k, 2], grcv.at[k, 2], to_up),
            remote(g_hbm.at[k, row_ds(far), hi], relay.at[k, 1], gsend.at[k, 3], grcv.at[k, 3], to_down),
            remote(relay.at[k, 0], grecv.at[k, 2, :, lo], gsend.at[k, 4], grcv.at[k, 4], to_up),
            remote(relay.at[k, 1], grecv.at[k, 2, :, hi], gsend.at[k, 5], grcv.at[k, 5], to_down),
        )

    gcopies = [grad_copies(k) for k in range(n_mat)]

    def issue_grad(k):
        for j in (2, 3, 0, 1):
            gcopies[k][j].start()

    issue_grad(0)
    issue_grad(1)
    for n in range(3):
        for dev in neighbours:
            pl.semaphore_signal(round_sem.at[n], inc=1, device_id=dev, device_id_type=MESH)
        pl.semaphore_wait(round_sem.at[n], 4)
    step = min(512, cols)
    out_copies = []
    tile_rows = lax.broadcasted_iota(jnp.int32, (8, 128), 0)
    norm_tile = jnp.zeros((8, 128), F32)

    def momentum_step(k, norm_tile):
        for c in loads[k]:
            c.wait()
        for j in (0, 1, 4, 5):
            gcopies[k][j].wait_recv()

        def col_step(i, acc):
            cs = pl.ds(pl.multiple_of(i * step, step), step)
            g_sum = (gown[k, :, cs].astype(F32) + grecv[k, 0, :, cs].astype(F32)) + (
                grecv[k, 1, :, cs].astype(F32) + grecv[k, 2, :, cs].astype(F32))
            m_new = MOMENTUM * mbuf[k, :, cs] + g_sum
            mbuf[k, :, cs] = m_new
            x_zero = g_sum + MOMENTUM * m_new
            x0[k, :, cs] = x_zero
            return acc + x_zero * x_zero

        acc = lax.fori_loop(0, cols // step, col_step, jnp.zeros((rows, step), F32))
        oc = pltpu.make_async_copy(mbuf.at[k], mnew_hbm.at[k], out_sem.at[k])
        oc.start()
        out_copies.append(oc)
        return jnp.where(tile_rows == k, jnp.sum(acc), norm_tile)

    for k in range(n_mat):
        for j in (2, 3):
            gcopies[k][j].wait_recv()
            gcopies[k][j + 2].start()
        if k + 2 < n_mat:
            issue_grad(k + 2)
        if k > 0:
            norm_tile = momentum_step(k - 1, norm_tile)
    norm_tile = momentum_step(n_mat - 1, norm_tile)

    nown[...] = norm_tile
    pair_copy = remote(nown, npair, nsend.at[0], nrcv.at[0], partner)
    pair_copy.start()
    pair_copy.wait_recv()
    here = y * SIDE + x
    nall[here] = nown[...] + npair[...]
    norm_copies = []
    for n, off in enumerate(others):
        py, px = peer(off)
        c = remote(nall.at[here], nall.at[here], nsend.at[1 + n], nrcv.at[1 + n], {'dp': py, 'fsdp': px})
        c.start()
        norm_copies.append(c)
    for c in norm_copies:
        c.wait_recv()
    sq_all = jnp.sum(nall[...], axis=0)
    denom_all = jnp.sqrt(sq_all) + NORM_EPS

    for k in range(n_mat):
        denom = denom_all[k:k + 1, 0:1]

        def div_step(i, carry, k=k, denom=denom):
            cs = pl.ds(pl.multiple_of(i * step, step), step)
            xrow[k, :, cs] = (x0[k, :, cs] / denom).astype(BF16)
            return carry

        lax.fori_loop(0, cols // step, div_step, 0)

    def exchange(src_of, dst_of, dst_all, mid, hold1, hold2, ssem, msem, h1sem, h2sem, fsem, idle):
        sends = []

        def send(src, dst, rsem, dev):
            c = remote(src, dst, ssem.at[len(sends)], rsem, dev)
            c.start()
            sends.append(c)

        ways = []
        for h in range(2):
            p, q = (x, y) if h == 0 else (y, x)
            near = [(lax.rem(c + 1, SIDE), lax.rem(c + SIDE - 1, SIDE), lax.rem(c + 2, SIDE)) for c in (p, q)]

            def yx(pp, qq, h=h):
                return (qq, pp) if h == 0 else (pp, qq)

            def dev(pp, qq, yx=yx):
                return dict(zip(('dp', 'fsdp'), yx(pp, qq)))

            def src(pp, qq, h=h, yx=yx):
                return src_of(*yx(pp, qq), h)

            def dst(pp, qq, h=h, yx=yx):
                return dst_of(*yx(pp, qq), h)

            ways.append((p, q, near[0], near[1], dev, src, dst))

        def second(h, o, piece):
            p, q, (pu, pd, pf), (qu, qd, qf), dev, src, dst = ways[h]
            start_p = (pd, pu, pf, p)[o]
            side, i = PLACE[o]
            send(piece(qf), hold2.at[h, side, i], h2sem.at[h, side, i], dev(p, (qu, qd)[side]))
            send(piece(qu), dst(start_p, q), fsem, dev(p, qu))
            send(piece(qd), dst(start_p, q), fsem, dev(p, qd))
            pltpu.make_async_copy(piece(q), dst(start_p, q), fsem).start()

        def relay2(h, o):
            p, q, (pu, pd, pf), (qu, qd, qf), dev, src, dst = ways[h]
            side, i = PLACE[o]
            held = hold2.at[h, side, i]
            pltpu.make_async_copy(held, held, h2sem.at[h, side, i]).wait()
            send(held, dst((pd, pu, pf, p)[o], (qd, qu)[side]), fsem, dev(p, (qu, qd)[side]))

        def near_pieces(i):
            for h in range(2):
                p, q, (pu, pd, pf), _, dev, src, dst = ways[h]
                for side, to in ((0, pu), (1, pd)):
                    send(src(to, i), mid.at[h, side, i], msem.at[h, side], dev(to, q))

        for h in range(2):
            p, q, (pu, pd, pf), _, dev, src, dst = ways[h]
            for side, to in ((0, pu), (1, pd)):
                for i in range(2):
                    send(src(pf, 2 * side + i), hold1.at[h, side, i], h1sem.at[h, side], dev(to, q))
        near_pieces(0)
        near_pieces(1)
        idle()
        for h in range(2):
            p, q, (pu, pd, pf), _, dev, src, dst = ways[h]
            for side, to in ((0, pu), (1, pd)):
                held = hold1.at[h, side]
                pltpu.make_async_copy(held, held, h1sem.at[h, side]).wait()
                send(held, mid.at[h, 2, 2 * side:2 * side + 2], msem.at[h, 2 + side], dev(to, q))
        near_pieces(2)
        near_pieces(3)
        for h in range(2):
            second(h, 3, lambda qq, h=h: ways[h][5](ways[h][0], qq))
        for h in range(2):
            for side in range(2):
                got = mid.at[h, 2, 2 * side:2 * side + 2]
                pltpu.make_async_copy(got, got, msem.at[h, 2 + side]).wait()
            second(h, 2, lambda qq, h=h: mid.at[h, 2, qq])
        for side in range(2):
            for h in range(2):
                got = mid.at[h, side]
                pltpu.make_async_copy(got, got, msem.at[h, side]).wait()
                second(h, side, lambda qq, h=h, side=side: mid.at[h, side, qq])
        for o in (3, 2, 0, 1):
            for h in range(2):
                relay2(h, o)
        pltpu.make_async_copy(dst_all, dst_all, fsem).wait()
        return sends

    half_piece = quarter // 2

    def piece_ds(pos, h):
        return pl.ds(pl.multiple_of(pos * quarter + h * half_piece, half_piece), half_piece)

    def idle_first():
        for k in range(n_mat):
            for c in gcopies[k]:
                c.wait_send()
            out_copies[k].wait()
        for c in [pair_copy] + norm_copies:
            c.wait_send()

    my_mat, my_pos = mat_of(y, x), pos_of(y, x)
    col_copies = exchange(lambda py, px, h: xrow.at[mat_of(py, px), :, piece_ds(pos_of(py, px), h)],
                          lambda oy, ox, h: xfull.at[row_ds(ox * SIDE + oy), h * half_piece:(h + 1) * half_piece],
                          xfull, cmid, chold1, chold2, csend, cmsem, ch1sem, ch2sem, cfsem, idle_first)

    fy, fx = y + 1 - 2 * (y % 2), x + 1 - 2 * (x % 2)
    square = ((y, fx), (fy, x), (fy, fx))
    chunk = HALF * BLK // 4

    def chunk_ds(pos):
        return pl.ds(pl.multiple_of(pos * chunk, chunk), chunk)

    def packed_ds(core, pos):
        return pl.ds(pl.multiple_of(core * (HALF * BLK) + pos * chunk, chunk), chunk)

    bcol = min(256, quarter)

    near_x, near_y, diagonal = (pos_of(*c) for c in square)
    to_x, to_y = {'fsdp': fx}, {'dp': fy}
    sub = chunk // 2

    def sub_ds(pos, h):
        return pl.ds(pl.multiple_of(pos * chunk + h * sub, sub), sub)

    def pair_of(it, n):
        cs = chunk_ds((diagonal, near_x, near_y, my_pos)[n])
        return remote(part.at[it, 1 - t, cs, :], drecv.at[it, cs, :], dsend.at[it, n], drcv.at[it, n], partner)

    def reduce_of(it, n):
        src = (red.at[it, sub_ds(diagonal, 0), :], red.at[it, sub_ds(diagonal, 1), :],
               red.at[it, sub_ds(near_x, 0), :], red.at[it, sub_ds(near_y, 1), :],
               comb.at[it, 0], comb.at[it, 1])[n]
        to = (to_x, to_y, to_x, to_y, to_y, to_x)[n]
        return remote(src, rsrecv.at[it, n], rssend.at[it, n], rsrcv.at[it, n], to)

    def gather_of(it, n):
        mine = agbuf.at[it, packed_ds(t, my_pos), :]
        py, px = square[n]
        return remote(mine, mine, agsend.at[it, n], agrcv.at[it, n], {'dp': py, 'fsdp': px})

    def forward_of(it, n):
        pos = my_pos if n == 0 else pos_of(*square[n - 1])
        held = agbuf.at[it, packed_ds(t, pos), :]
        return remote(held, held, fwsend.at[it, n], fwrcv.at[it, n], partner)

    def drain(it):
        for n in range(4):
            pair_of(it, n).wait_send()
            forward_of(it, n).wait_send()
        for n in range(6):
            reduce_of(it, n).wait_send()
        for n in range(3):
            gather_of(it, n).wait_send()

    def half_gram(it, h):
        nt = (((1,), (1,)), ((), ()))
        pair_rows = xfull[pl.ds(pl.multiple_of(h * 2 * BLK, 2 * BLK), 2 * BLK), :]
        square_gram = lax.dot_general(pair_rows, pair_rows, nt, preferred_element_type=F32)
        cross_gram = lax.dot_general(xfull[pl.ds(pl.multiple_of(h * BLK, BLK), BLK), :], xfull[2 * BLK:, :], nt,
                                     preferred_element_type=F32)
        blocks = (square_gram[:BLK, :BLK], square_gram[:BLK, BLK:], square_gram[BLK:, BLK:],
                  cross_gram[:, :BLK], cross_gram[:, BLK:])
        for n, block in enumerate(blocks):
            part[it, h, n * BLK:(n + 1) * BLK, :] = block

    def iteration(it, carry):
        half_gram(it, 1 - t)
        for n in range(4):
            pair_of(it, n).start()
        half_gram(it, t)
        for n, pos in enumerate((diagonal, near_x, near_y, my_pos)):
            pair_of(it, n).wait_recv()
            cs = chunk_ds(pos)
            red[it, cs, :] = part[it, t, cs, :] + drecv[it, cs, :]
            for m in ((0, 1), (2,), (3,), ())[n]:
                reduce_of(it, m).start()
        reduce_of(it, 0).wait_recv()
        comb[it, 0] = red[it, sub_ds(near_y, 0), :] + rsrecv[it, 0]
        reduce_of(it, 4).start()
        reduce_of(it, 1).wait_recv()
        comb[it, 1] = red[it, sub_ds(near_x, 1), :] + rsrecv[it, 1]
        reduce_of(it, 5).start()

        @pl.when(it > 0)
        def _():
            drain(it - 1)

        for h in range(2):
            reduce_of(it, 2 + h).wait_recv()
            reduce_of(it, 4 + h).wait_recv()
            total = (red[it, sub_ds(my_pos, h), :] + rsrecv[it, 2 + h]) + rsrecv[it, 4 + h]
            mine = pl.ds(pl.multiple_of(t * (HALF * BLK) + my_pos * chunk + h * sub, sub), sub)
            agbuf[it, mine, :] = total.astype(BF16)
        for n in (2, 0, 1):
            gather_of(it, n).start()
        forward_of(it, 0).start()
        for n in range(3):
            gather_of(it, n).wait_recv()
            forward_of(it, n + 1).start()
        for n in range(4):
            forward_of(it, n).wait_recv()
        for n, (bi, bj) in enumerate(TRI):
            block = agbuf[it, n * BLK:(n + 1) * BLK, :]
            amat[bi * BLK:(bi + 1) * BLK, bj * BLK:(bj + 1) * BLK] = block
            if bi != bj:
                amat[bj * BLK:(bj + 1) * BLK, bi * BLK:(bi + 1) * BLK] = block.astype(F32).T.astype(BF16)
        for bi in range(2):
            rs = slice(2 * BLK * bi, 2 * BLK * (bi + 1))
            sq = jnp.dot(amat[rs, :], amat[...], preferred_element_type=F32).astype(BF16)
            bmat[rs, :] = (COEF_B * amat[rs, :].astype(F32) + COEF_C * sq.astype(F32)).astype(BF16)

        for i in range(quarter // bcol):
            cs = slice(i * bcol, (i + 1) * bcol)
            x_old = xfull[:, cs]
            prod = jnp.dot(bmat[...], x_old, preferred_element_type=F32)
            xfull[:, cs] = (COEF_A * x_old.astype(F32) + prod).astype(BF16)
        return carry

    for c in col_copies:
        c.wait_send()
    lax.fori_loop(0, NS_STEPS, iteration, 0)

    back_copies = exchange(lambda py, px, h: xfull.at[row_ds(px * SIDE + py), h * half_piece:(h + 1) * half_piece],
                           lambda oy, ox, h: xfin_hbm.at[mat_of(oy, ox), :, piece_ds(pos_of(oy, ox), h)],
                           xfin_hbm, bmid, bhold1, bhold2, bsend, bmsem, bh1sem, bh2sem, bfsem, lambda: drain(NS_STEPS - 1))

    for c in back_copies:
        c.wait_send()


def run_kernel(m_blk, g_blk):
    n_mat, rows, cols = m_blk.shape
    all_rows = rows * SIDE * SIDE
    quarter = cols // SIDE
    packed = len(TRI) * BLK
    chunk = packed // 8
    n_oth = SIDE * SIDE - 1
    dma = pltpu.SemaphoreType.DMA
    half_piece = (rows, quarter // 2)
    relays = [
        pltpu.VMEM((2, 3, SIDE) + half_piece, BF16),
        pltpu.VMEM((2, 2, 2) + half_piece, BF16),
        pltpu.VMEM((2, 2, 2) + half_piece, BF16),
    ]
    relay_sems = [dma((60,)), dma((2, 4)), dma((2, 2)), dma((2, 2, 2)), dma]
    scratch = [
        pltpu.VMEM((n_mat, rows, cols), BF16),
        pltpu.VMEM((n_mat, 3, rows, cols), BF16),
        pltpu.VMEM((n_mat, 2, rows, cols // 2), BF16),
        pltpu.VMEM((n_mat, rows, cols), F32),
        pltpu.VMEM((n_mat, rows, cols), F32),
        pltpu.VMEM((n_mat, rows, cols), BF16),
        pltpu.VMEM((all_rows, quarter), BF16),
        pltpu.VMEM((8, 128), F32),
        pltpu.VMEM((8, 128), F32),
        pltpu.VMEM((SIDE * SIDE, 8, 128), F32),
        pltpu.VMEM((NS_STEPS, 2, packed // 2, BLK), F32),
        pltpu.VMEM((NS_STEPS, packed // 2, BLK), F32),
        pltpu.VMEM((NS_STEPS, packed // 2, BLK), F32),
        pltpu.VMEM((NS_STEPS, 2, chunk // 2, BLK), F32),
        pltpu.VMEM((NS_STEPS, 6, chunk // 2, BLK), F32),
        pltpu.VMEM((NS_STEPS, packed, BLK), BF16),
        pltpu.VMEM((all_rows, all_rows), BF16),
        pltpu.VMEM((all_rows, all_rows), BF16),
        *relays, *relays,
        dma((2, n_mat)), dma((n_mat,)), dma((n_mat, 6)), dma((n_mat, 6)),
        dma((n_oth + 1,)), dma((n_oth + 1,)), *relay_sems, *relay_sems,
        dma((NS_STEPS, 4)), dma((NS_STEPS, 4)), dma((NS_STEPS, 6)), dma((NS_STEPS, 6)),
        dma((NS_STEPS, 3)), dma((NS_STEPS, 3)), dma((NS_STEPS, 4)), dma((NS_STEPS, 4)), pltpu.SemaphoreType.REGULAR((3,)),
    ]
    anyspace = pl.BlockSpec(memory_space=pl.ANY)
    return pl.pallas_call(
        muon_kernel,
        out_shape=(jax.ShapeDtypeStruct(m_blk.shape, F32), jax.ShapeDtypeStruct(m_blk.shape, BF16)),
        in_specs=[anyspace, anyspace],
        out_specs=(anyspace, anyspace),
        scratch_shapes=scratch,
        compiler_params=pltpu.CompilerParams(collective_id=0, has_side_effects=True, vmem_limit_bytes=VMEM_MIB * 2 ** 20),
        name='muon_group',
    )(m_blk, g_blk)


def solution(mesh):
    mat_spec = P('stage', ROW_AXES, 'tp')
    grad_spec = P(('stage', 'dp'), None, 'fsdp', 'tp')
    tp_size = mesh.shape['tp']

    def local_step(w_blk, m_blk, g_blk):
        m_new, x_fin = run_kernel(m_blk, g_blk.reshape(g_blk.shape[1:]))
        col_count = w_blk.shape[2] * tp_size
        update_scale = LEARN_RATE * 0.2 * math.sqrt(col_count)
        decay_factor = 1.0 - LEARN_RATE * WEIGHT_DECAY
        w_new = decay_factor * w_blk - update_scale * x_fin.astype(F32)
        return w_new, m_new

    return jax.shard_map(local_step, mesh=mesh, in_specs=(mat_spec, mat_spec, grad_spec), out_specs=(mat_spec, mat_spec), check_vma=False)
```

```python
import functools
import math
import jax
import jax.numpy as jnp
from jax import lax
from jax.experimental import pallas as pl
from jax.experimental.pallas import tpu as pltpu
from jax.sharding import PartitionSpec as P

MOMENTUM = 0.95
LEARN_RATE = 0.1
WEIGHT_DECAY = 0.1
COEF_A = 3.4445
COEF_B = -4.7750
COEF_C = 2.0315
NORM_EPS = 1e-7
NS_STEPS = 5
ROW_AXES = ('fsdp', 'dp')
F32 = jnp.float32
BF16 = jnp.bfloat16
MESH = pl.DeviceIdType.MESH
VMEM_MIB = 47
SIDE = 4
BLK = 128
TRI = ((0, 0), (0, 1), (1, 1), (0, 2), (0, 3), (2, 2), (2, 3), (3, 3), (1, 2), (1, 3))
HALF = len(TRI) // 2
PLACE = ((0, 1), (1, 0), (1, 1), (0, 0))


def muon_kernel(m_hbm, g_hbm, mnew_hbm, xfin_hbm,
                gown, grecv, relay, mbuf, x0, xrow, xfull,
                nown, npair, nall, part, drecv, comb, rsrecv, agbuf, amat, bmat,
                cmid, chold1, chold2, bmid, bhold1, bhold2,
                load_sem, out_sem, gsend, grcv, nsend, nrcv, csend, cmsem, ch1sem, ch2sem, cfsem,
                bsend, bmsem, bh1sem, bh2sem, bfsem,
                dsend, drcv, rssend, rsrcv, agsend, agrcv, fwsend, fwrcv, round_sem):
    n_mat, rows, cols = mbuf.shape
    quarter = cols // SIDE
    half = cols // 2
    y = lax.axis_index('dp')
    x = lax.axis_index('fsdp')
    t = lax.axis_index('tp')
    partner = {'tp': 1 - t}
    up = lax.rem(y + 1, SIDE)
    down = lax.rem(y + SIDE - 1, SIDE)
    far = lax.rem(y + 2, SIDE)

    def row_ds(i):
        return pl.ds(pl.multiple_of(i * rows, rows), rows)

    def quarter_ds(i):
        return pl.ds(pl.multiple_of(i * quarter, quarter), quarter)

    def mat_of(yy, xx):
        return (yy // 2) * 2 + xx // 2

    def pos_of(yy, xx):
        return (yy % 2) * 2 + xx % 2

    loads = []
    for k in range(n_mat):
        loads.append((pltpu.make_async_copy(g_hbm.at[k, row_ds(y), :], gown.at[k], load_sem.at[0, k]),
                      pltpu.make_async_copy(m_hbm.at[k], mbuf.at[k], load_sem.at[1, k])))
        for c in loads[-1]:
            c.start()

    others = [(oy, ox) for oy in range(SIDE) for ox in range(SIDE) if (oy, ox) != (0, 0)]

    def peer(off):
        return lax.rem(y + off[0], SIDE), lax.rem(x + off[1], SIDE)

    xup, xdown = lax.rem(x + 1, SIDE), lax.rem(x + SIDE - 1, SIDE)
    neighbours = ({'dp': up}, {'dp': down}, {'fsdp': xup}, {'fsdp': xdown})
    barrier = pltpu.get_barrier_semaphore()
    for dev in neighbours + (partner,):
        pl.semaphore_signal(barrier, inc=1, device_id=dev, device_id_type=MESH)
    pl.semaphore_wait(barrier, 5)

    def remote(src, dst, ssem, rsem, dev):
        return pltpu.make_async_remote_copy(src_ref=src, dst_ref=dst, send_sem=ssem, recv_sem=rsem,
                                            device_id=dev, device_id_type=MESH)

    lo, hi = pl.ds(0, half), pl.ds(half, half)

    def grad_copies(k):
        to_up, to_down = {'dp': up}, {'dp': down}
        return (
            remote(g_hbm.at[k, row_ds(up), :], grecv.at[k, 0], gsend.at[k, 0], grcv.at[k, 0], to_up),
            remote(g_hbm.at[k, row_ds(down), :], grecv.at[k, 1], gsend.at[k, 1], grcv.at[k, 1], to_down),
            remote(g_hbm.at[k, row_ds(far), lo], relay.at[k, 0], gsend.at[k, 2], grcv.at[k, 2], to_up),
            remote(g_hbm.at[k, row_ds(far), hi], relay.at[k, 1], gsend.at[k, 3], grcv.at[k, 3], to_down),
            remote(relay.at[k, 0], grecv.at[k, 2, :, lo], gsend.at[k, 4], grcv.at[k, 4], to_up),
            remote(relay.at[k, 1], grecv.at[k, 2, :, hi], gsend.at[k, 5], grcv.at[k, 5], to_down),
        )

    gcopies = [grad_copies(k) for k in range(n_mat)]

    def issue_grad(k):
        for j in (2, 3, 0, 1):
            gcopies[k][j].start()

    issue_grad(0)
    issue_grad(1)
    for n in range(3):
        for dev in neighbours:
            pl.semaphore_signal(round_sem.at[n], inc=1, device_id=dev, device_id_type=MESH)
        pl.semaphore_wait(round_sem.at[n], 4)
    step = min(512, cols)
    out_copies = []
    tile_rows = lax.broadcasted_iota(jnp.int32, (8, 128), 0)
    norm_tile = jnp.zeros((8, 128), F32)

    def momentum_step(k, norm_tile):
        for c in loads[k]:
            c.wait()
        for j in (0, 1, 4, 5):
            gcopies[k][j].wait_recv()

        def col_step(i, acc):
            cs = pl.ds(pl.multiple_of(i * step, step), step)
            g_sum = (gown[k, :, cs].astype(F32) + grecv[k, 0, :, cs].astype(F32)) + (
                grecv[k, 1, :, cs].astype(F32) + grecv[k, 2, :, cs].astype(F32))
            m_new = MOMENTUM * mbuf[k, :, cs] + g_sum
            mbuf[k, :, cs] = m_new
            x_zero = g_sum + MOMENTUM * m_new
            x0[k, :, cs] = x_zero
            return acc + x_zero * x_zero

        acc = lax.fori_loop(0, cols // step, col_step, jnp.zeros((rows, step), F32))
        oc = pltpu.make_async_copy(mbuf.at[k], mnew_hbm.at[k], out_sem.at[k])
        oc.start()
        out_copies.append(oc)
        return jnp.where(tile_rows == k, jnp.sum(acc), norm_tile)

    for k in range(n_mat):
        for j in (2, 3):
            gcopies[k][j].wait_recv()
            gcopies[k][j + 2].start()
        if k + 2 < n_mat:
            issue_grad(k + 2)
        if k > 0:
            norm_tile = momentum_step(k - 1, norm_tile)
    norm_tile = momentum_step(n_mat - 1, norm_tile)

    nown[...] = norm_tile
    pair_copy = remote(nown, npair, nsend.at[0], nrcv.at[0], partner)
    pair_copy.start()
    pair_copy.wait_recv()
    here = y * SIDE + x
    nall[here] = nown[...] + npair[...]
    norm_copies = []
    for n, off in enumerate(others):
        py, px = peer(off)
        c = remote(nall.at[here], nall.at[here], nsend.at[1 + n], nrcv.at[1 + n], {'dp': py, 'fsdp': px})
        c.start()
        norm_copies.append(c)
    for c in norm_copies:
        c.wait_recv()
    sq_all = jnp.sum(nall[...], axis=0)
    denom_all = jnp.sqrt(sq_all) + NORM_EPS

    for k in range(n_mat):
        denom = denom_all[k:k + 1, 0:1]

        def div_step(i, carry, k=k, denom=denom):
            cs = pl.ds(pl.multiple_of(i * step, step), step)
            xrow[k, :, cs] = (x0[k, :, cs] / denom).astype(BF16)
            return carry

        lax.fori_loop(0, cols // step, div_step, 0)

    def exchange(src_of, dst_of, dst_all, mid, hold1, hold2, ssem, msem, h1sem, h2sem, fsem, idle):
        sends = []

        def send(src, dst, rsem, dev):
            c = remote(src, dst, ssem.at[len(sends)], rsem, dev)
            c.start()
            sends.append(c)

        ways = []
        for h in range(2):
            p, q = (x, y) if h == 0 else (y, x)
            near = [(lax.rem(c + 1, SIDE), lax.rem(c + SIDE - 1, SIDE), lax.rem(c + 2, SIDE)) for c in (p, q)]

            def yx(pp, qq, h=h):
                return (qq, pp) if h == 0 else (pp, qq)

            def dev(pp, qq, yx=yx):
                return dict(zip(('dp', 'fsdp'), yx(pp, qq)))

            def src(pp, qq, h=h, yx=yx):
                return src_of(*yx(pp, qq), h)

            def dst(pp, qq, h=h, yx=yx):
                return dst_of(*yx(pp, qq), h)

            ways.append((p, q, near[0], near[1], dev, src, dst))

        def second(h, o, piece):
            p, q, (pu, pd, pf), (qu, qd, qf), dev, src, dst = ways[h]
            start_p = (pd, pu, pf, p)[o]
            side, i = PLACE[o]
            send(piece(qf), hold2.at[h, side, i], h2sem.at[h, side, i], dev(p, (qu, qd)[side]))
            send(piece(qu), dst(start_p, q), fsem, dev(p, qu))
            send(piece(qd), dst(start_p, q), fsem, dev(p, qd))
            pltpu.make_async_copy(piece(q), dst(start_p, q), fsem).start()

        def relay2(h, o):
            p, q, (pu, pd, pf), (qu, qd, qf), dev, src, dst = ways[h]
            side, i = PLACE[o]
            held = hold2.at[h, side, i]
            pltpu.make_async_copy(held, held, h2sem.at[h, side, i]).wait()
            send(held, dst((pd, pu, pf, p)[o], (qd, qu)[side]), fsem, dev(p, (qu, qd)[side]))

        def near_pieces(i):
            for h in range(2):
                p, q, (pu, pd, pf), _, dev, src, dst = ways[h]
                for side, to in ((0, pu), (1, pd)):
                    send(src(to, i), mid.at[h, side, i], msem.at[h, side], dev(to, q))

        for h in range(2):
            p, q, (pu, pd, pf), _, dev, src, dst = ways[h]
            for side, to in ((0, pu), (1, pd)):
                for i in range(2):
                    send(src(pf, 2 * side + i), hold1.at[h, side, i], h1sem.at[h, side], dev(to, q))
        near_pieces(0)
        near_pieces(1)
        idle()
        for h in range(2):
            p, q, (pu, pd, pf), _, dev, src, dst = ways[h]
            for side, to in ((0, pu), (1, pd)):
                held = hold1.at[h, side]
                pltpu.make_async_copy(held, held, h1sem.at[h, side]).wait()
                send(held, mid.at[h, 2, 2 * side:2 * side + 2], msem.at[h, 2 + side], dev(to, q))
        near_pieces(2)
        near_pieces(3)
        for h in range(2):
            second(h, 3, lambda qq, h=h: ways[h][5](ways[h][0], qq))
        for h in range(2):
            for side in range(2):
                got = mid.at[h, 2, 2 * side:2 * side + 2]
                pltpu.make_async_copy(got, got, msem.at[h, 2 + side]).wait()
            second(h, 2, lambda qq, h=h: mid.at[h, 2, qq])
        for side in range(2):
            for h in range(2):
                got = mid.at[h, side]
                pltpu.make_async_copy(got, got, msem.at[h, side]).wait()
                second(h, side, lambda qq, h=h, side=side: mid.at[h, side, qq])
        for o in (3, 2, 0, 1):
            for h in range(2):
                relay2(h, o)
        pltpu.make_async_copy(dst_all, dst_all, fsem).wait()
        return sends

    half_piece = quarter // 2

    def piece_ds(pos, h):
        return pl.ds(pl.multiple_of(pos * quarter + h * half_piece, half_piece), half_piece)

    def idle_first():
        for k in range(n_mat):
            for c in gcopies[k]:
                c.wait_send()
            out_copies[k].wait()
        for c in [pair_copy] + norm_copies:
            c.wait_send()

    my_mat, my_pos = mat_of(y, x), pos_of(y, x)
    col_copies = exchange(lambda py, px, h: xrow.at[mat_of(py, px), :, piece_ds(pos_of(py, px), h)],
                          lambda oy, ox, h: xfull.at[row_ds(ox * SIDE + oy), h * half_piece:(h + 1) * half_piece],
                          xfull, cmid, chold1, chold2, csend, cmsem, ch1sem, ch2sem, cfsem, idle_first)

    fy, fx = y + 1 - 2 * (y % 2), x + 1 - 2 * (x % 2)
    square = ((y, fx), (fy, x), (fy, fx))
    packed = len(TRI) * BLK
    chunk = packed // 4

    def chunk_ds(pos):
        return pl.ds(pl.multiple_of(pos * chunk, chunk), chunk)

    bcol = min(256, quarter)

    near_x, near_y, diagonal = (pos_of(*c) for c in square)
    to_x, to_y = {'fsdp': fx}, {'dp': fy}
    sub = chunk // 2

    def sub_ds(pos, h):
        return pl.ds(pl.multiple_of(pos * chunk + h * sub, sub), sub)

    pieces = [slice(h * HALF * BLK + lo_ * BLK, h * HALF * BLK + hi_ * BLK) for h in range(2) for lo_, hi_ in ((0, 3), (3, HALF))]

    def pair_of(it, n):
        return remote(part.at[it, pieces[n], :], drecv.at[it, pieces[n], :], dsend.at[it, n], drcv.at[it, n], partner)

    def reduce_of(it, n):
        src = (part.at[it, sub_ds(diagonal, 0), :], part.at[it, sub_ds(diagonal, 1), :],
               part.at[it, sub_ds(near_x, 0), :], part.at[it, sub_ds(near_y, 1), :],
               comb.at[it, 0], comb.at[it, 1])[n]
        to = (to_x, to_y, to_x, to_y, to_y, to_x)[n]
        return remote(src, rsrecv.at[it, n], rssend.at[it, n], rsrcv.at[it, n], to)

    def gather_of(it, n):
        mine = agbuf.at[it, chunk_ds(my_pos), :]
        py, px = square[n]
        return remote(mine, mine, agsend.at[it, n], agrcv.at[it, n], {'dp': py, 'fsdp': px})

    def forward_of(it, n):
        pos = my_pos if n == 0 else pos_of(*square[n - 1])
        held = agbuf.at[it, chunk_ds(pos), :]
        return remote(held, held, fwsend.at[it, n], fwrcv.at[it, n], partner)

    leads = t == 1

    def drain(it):
        @pl.when(leads)
        def _():
            for n in range(6):
                reduce_of(it, n).wait_send()
            for n in range(3):
                gather_of(it, n).wait_send()
            for n in range(4):
                forward_of(it, n).wait_send()

        @pl.when(t == 0)
        def _():
            for n in range(4):
                pair_of(it, n).wait_send()

    def gram_piece(it, n):
        nt = (((1,), (1,)), ((), ()))
        h = n // 2
        if n % 2 == 0:
            pair_rows = xfull[2 * BLK * h:2 * BLK * (h + 1), :]
            gram = lax.dot_general(pair_rows, pair_rows, nt, preferred_element_type=F32)
            blocks = (gram[:BLK, :BLK], gram[:BLK, BLK:], gram[BLK:, BLK:])
        else:
            gram = lax.dot_general(xfull[h * BLK:(h + 1) * BLK, :], xfull[2 * BLK:, :], nt, preferred_element_type=F32)
            blocks = (gram[:, :BLK], gram[:, BLK:])
        for i, block in enumerate(blocks):
            part[it, pieces[n].start + i * BLK:pieces[n].start + (i + 1) * BLK, :] = block

    def lead(it):
        for n in range(4):
            pair_of(it, n).wait_recv()
            part[it, pieces[n], :] += drecv[it, pieces[n], :]
        for n in range(4):
            reduce_of(it, n).start()
        reduce_of(it, 0).wait_recv()
        comb[it, 0] = part[it, sub_ds(near_y, 0), :] + rsrecv[it, 0]
        reduce_of(it, 4).start()
        reduce_of(it, 1).wait_recv()
        comb[it, 1] = part[it, sub_ds(near_x, 1), :] + rsrecv[it, 1]
        reduce_of(it, 5).start()
        for h in range(2):
            reduce_of(it, 2 + h).wait_recv()
            reduce_of(it, 4 + h).wait_recv()
            total = (part[it, sub_ds(my_pos, h), :] + rsrecv[it, 2 + h]) + rsrecv[it, 4 + h]
            agbuf[it, sub_ds(my_pos, h), :] = total.astype(BF16)
        for n in (2, 0, 1):
            gather_of(it, n).start()
        forward_of(it, 0).start()
        for n in range(3):
            gather_of(it, n).wait_recv()
            forward_of(it, n + 1).start()

    def iteration(it, carry):
        for n in range(4):
            gram_piece(it, n)

            @pl.when(t == 0)
            def _(n=n):
                pair_of(it, n).start()

        @pl.when(it > 0)
        def _():
            drain(it - 1)

        @pl.when(leads)
        def _():
            lead(it)

        @pl.when(t == 0)
        def _():
            for n in range(4):
                forward_of(it, n).wait_recv()

        for n, (bi, bj) in enumerate(TRI):
            block = agbuf[it, n * BLK:(n + 1) * BLK, :]
            amat[bi * BLK:(bi + 1) * BLK, bj * BLK:(bj + 1) * BLK] = block
            if bi != bj:
                amat[bj * BLK:(bj + 1) * BLK, bi * BLK:(bi + 1) * BLK] = block.astype(F32).T.astype(BF16)
        for bi in range(2):
            rs = slice(2 * BLK * bi, 2 * BLK * (bi + 1))
            sq = jnp.dot(amat[rs, :], amat[...], preferred_element_type=F32).astype(BF16)
            bmat[rs, :] = (COEF_B * amat[rs, :].astype(F32) + COEF_C * sq.astype(F32)).astype(BF16)

        for i in range(quarter // bcol):
            cs = slice(i * bcol, (i + 1) * bcol)
            x_old = xfull[:, cs]
            prod = jnp.dot(bmat[...], x_old, preferred_element_type=F32)
            xfull[:, cs] = (COEF_A * x_old.astype(F32) + prod).astype(BF16)
        return carry

    for c in col_copies:
        c.wait_send()
    lax.fori_loop(0, NS_STEPS, iteration, 0)

    back_copies = exchange(lambda py, px, h: xfull.at[row_ds(px * SIDE + py), h * half_piece:(h + 1) * half_piece],
                           lambda oy, ox, h: xfin_hbm.at[mat_of(oy, ox), :, piece_ds(pos_of(oy, ox), h)],
                           xfin_hbm, bmid, bhold1, bhold2, bsend, bmsem, bh1sem, bh2sem, bfsem, lambda: drain(NS_STEPS - 1))

    for c in back_copies:
        c.wait_send()


def run_kernel(m_blk, g_blk):
    n_mat, rows, cols = m_blk.shape
    all_rows = rows * SIDE * SIDE
    quarter = cols // SIDE
    packed = len(TRI) * BLK
    chunk = packed // 4
    n_oth = SIDE * SIDE - 1
    dma = pltpu.SemaphoreType.DMA
    half_piece = (rows, quarter // 2)
    relays = [
        pltpu.VMEM((2, 3, SIDE) + half_piece, BF16),
        pltpu.VMEM((2, 2, 2) + half_piece, BF16),
        pltpu.VMEM((2, 2, 2) + half_piece, BF16),
    ]
    relay_sems = [dma((60,)), dma((2, 4)), dma((2, 2)), dma((2, 2, 2)), dma]
    scratch = [
        pltpu.VMEM((n_mat, rows, cols), BF16),
        pltpu.VMEM((n_mat, 3, rows, cols), BF16),
        pltpu.VMEM((n_mat, 2, rows, cols // 2), BF16),
        pltpu.VMEM((n_mat, rows, cols), F32),
        pltpu.VMEM((n_mat, rows, cols), F32),
        pltpu.VMEM((n_mat, rows, cols), BF16),
        pltpu.VMEM((all_rows, quarter), BF16),
        pltpu.VMEM((8, 128), F32),
        pltpu.VMEM((8, 128), F32),
        pltpu.VMEM((SIDE * SIDE, 8, 128), F32),
        pltpu.VMEM((NS_STEPS, packed, BLK), F32),
        pltpu.VMEM((NS_STEPS, packed, BLK), F32),
        pltpu.VMEM((NS_STEPS, 2, chunk // 2, BLK), F32),
        pltpu.VMEM((NS_STEPS, 6, chunk // 2, BLK), F32),
        pltpu.VMEM((NS_STEPS, packed, BLK), BF16),
        pltpu.VMEM((all_rows, all_rows), BF16),
        pltpu.VMEM((all_rows, all_rows), BF16),
        *relays, *relays,
        dma((2, n_mat)), dma((n_mat,)), dma((n_mat, 6)), dma((n_mat, 6)),
        dma((n_oth + 1,)), dma((n_oth + 1,)), *relay_sems, *relay_sems,
        dma((NS_STEPS, 4)), dma((NS_STEPS, 4)), dma((NS_STEPS, 6)), dma((NS_STEPS, 6)),
        dma((NS_STEPS, 3)), dma((NS_STEPS, 3)), dma((NS_STEPS, 4)), dma((NS_STEPS, 4)), pltpu.SemaphoreType.REGULAR((3,)),
    ]
    anyspace = pl.BlockSpec(memory_space=pl.ANY)
    return pl.pallas_call(
        muon_kernel,
        out_shape=(jax.ShapeDtypeStruct(m_blk.shape, F32), jax.ShapeDtypeStruct(m_blk.shape, BF16)),
        in_specs=[anyspace, anyspace],
        out_specs=(anyspace, anyspace),
        scratch_shapes=scratch,
        compiler_params=pltpu.CompilerParams(collective_id=0, has_side_effects=True, vmem_limit_bytes=VMEM_MIB * 2 ** 20),
        name='muon_group',
    )(m_blk, g_blk)


def solution(mesh):
    mat_spec = P('stage', ROW_AXES, 'tp')
    grad_spec = P(('stage', 'dp'), None, 'fsdp', 'tp')
    tp_size = mesh.shape['tp']

    def local_step(w_blk, m_blk, g_blk):
        m_new, x_fin = run_kernel(m_blk, g_blk.reshape(g_blk.shape[1:]))
        col_count = w_blk.shape[2] * tp_size
        update_scale = LEARN_RATE * 0.2 * math.sqrt(col_count)
        decay_factor = 1.0 - LEARN_RATE * WEIGHT_DECAY
        w_new = decay_factor * w_blk - update_scale * x_fin.astype(F32)
        return w_new, m_new

    return jax.shard_map(local_step, mesh=mesh, in_specs=(mat_spec, mat_spec, grad_spec), out_specs=(mat_spec, mat_spec), check_vma=False)
```

```python
import functools
import math
import jax
import jax.numpy as jnp
from jax import lax
from jax.experimental import pallas as pl
from jax.experimental.pallas import tpu as pltpu
from jax.sharding import PartitionSpec as P

MOMENTUM = 0.95
LEARN_RATE = 0.1
WEIGHT_DECAY = 0.1
COEF_A = 3.4445
COEF_B = -4.7750
COEF_C = 2.0315
NORM_EPS = 1e-7
NS_STEPS = 5
ROW_AXES = ('fsdp', 'dp')
F32 = jnp.float32
BF16 = jnp.bfloat16
MESH = pl.DeviceIdType.MESH
VMEM_MIB = 46
SIDE = 4
BLK = 128
TRI = ((0, 0), (0, 1), (1, 1), (0, 2), (0, 3), (2, 2), (2, 3), (3, 3), (1, 2), (1, 3))
HALF = len(TRI) // 2
PLACE = ((0, 1), (1, 0), (1, 1), (0, 0))


def muon_kernel(m_hbm, g_hbm, mnew_hbm, xfin_hbm,
                gown, grecv, relay, mbuf, x0, xrow, xfull,
                nown, npair, nall, part, drecv, red, comb, rsrecv, agbuf, amat, bmat,
                cmid, chold1, chold2, bmid, bhold1, bhold2,
                load_sem, out_sem, gsend, grcv, nsend, nrcv, csend, cmsem, ch1sem, ch2sem, cfsem,
                bsend, bmsem, bh1sem, bh2sem, bfsem,
                dsend, drcv, rssend, rsrcv, agsend, agrcv, fwsend, fwrcv, round_sem):
    n_mat, rows, cols = mbuf.shape
    quarter = cols // SIDE
    half = cols // 2
    y = lax.axis_index('dp')
    x = lax.axis_index('fsdp')
    t = lax.axis_index('tp')
    partner = {'tp': 1 - t}
    up = lax.rem(y + 1, SIDE)
    down = lax.rem(y + SIDE - 1, SIDE)
    far = lax.rem(y + 2, SIDE)

    def row_ds(i):
        return pl.ds(pl.multiple_of(i * rows, rows), rows)

    def quarter_ds(i):
        return pl.ds(pl.multiple_of(i * quarter, quarter), quarter)

    def mat_of(yy, xx):
        return (yy // 2) * 2 + xx // 2

    def pos_of(yy, xx):
        return (yy % 2) * 2 + xx % 2

    loads = []
    for k in range(n_mat):
        loads.append((pltpu.make_async_copy(g_hbm.at[k, row_ds(y), :], gown.at[k], load_sem.at[0, k]),
                      pltpu.make_async_copy(m_hbm.at[k], mbuf.at[k], load_sem.at[1, k])))
        for c in loads[-1]:
            c.start()

    others = [(oy, ox) for oy in range(SIDE) for ox in range(SIDE) if (oy, ox) != (0, 0)]

    def peer(off):
        return lax.rem(y + off[0], SIDE), lax.rem(x + off[1], SIDE)

    xup, xdown = lax.rem(x + 1, SIDE), lax.rem(x + SIDE - 1, SIDE)
    neighbours = ({'dp': up}, {'dp': down}, {'fsdp': xup}, {'fsdp': xdown})
    barrier = pltpu.get_barrier_semaphore()
    for dev in neighbours + (partner,):
        pl.semaphore_signal(barrier, inc=1, device_id=dev, device_id_type=MESH)
    pl.semaphore_wait(barrier, 5)

    def remote(src, dst, ssem, rsem, dev):
        return pltpu.make_async_remote_copy(src_ref=src, dst_ref=dst, send_sem=ssem, recv_sem=rsem,
                                            device_id=dev, device_id_type=MESH)

    lo, hi = pl.ds(0, half), pl.ds(half, half)

    def grad_copies(k):
        to_up, to_down = {'dp': up}, {'dp': down}
        return (
            remote(g_hbm.at[k, row_ds(up), :], grecv.at[k, 0], gsend.at[k, 0], grcv.at[k, 0], to_up),
            remote(g_hbm.at[k, row_ds(down), :], grecv.at[k, 1], gsend.at[k, 1], grcv.at[k, 1], to_down),
            remote(g_hbm.at[k, row_ds(far), lo], relay.at[k, 0], gsend.at[k, 2], grcv.at[k, 2], to_up),
            remote(g_hbm.at[k, row_ds(far), hi], relay.at[k, 1], gsend.at[k, 3], grcv.at[k, 3], to_down),
            remote(relay.at[k, 0], grecv.at[k, 2, :, lo], gsend.at[k, 4], grcv.at[k, 4], to_up),
            remote(relay.at[k, 1], grecv.at[k, 2, :, hi], gsend.at[k, 5], grcv.at[k, 5], to_down),
        )

    gcopies = [grad_copies(k) for k in range(n_mat)]

    def issue_grad(k):
        for j in (2, 3, 0, 1):
            gcopies[k][j].start()

    issue_grad(0)
    issue_grad(1)
    for n in range(3):
        for dev in neighbours:
            pl.semaphore_signal(round_sem.at[n], inc=1, device_id=dev, device_id_type=MESH)
        pl.semaphore_wait(round_sem.at[n], 4)
    step = min(512, cols)
    out_copies = []
    tile_rows = lax.broadcasted_iota(jnp.int32, (8, 128), 0)
    norm_tile = jnp.zeros((8, 128), F32)

    def momentum_step(k, norm_tile):
        for c in loads[k]:
            c.wait()
        for j in (0, 1, 4, 5):
            gcopies[k][j].wait_recv()

        def col_step(i, acc):
            cs = pl.ds(pl.multiple_of(i * step, step), step)
            g_sum = (gown[k, :, cs].astype(F32) + grecv[k, 0, :, cs].astype(F32)) + (
                grecv[k, 1, :, cs].astype(F32) + grecv[k, 2, :, cs].astype(F32))
            m_new = MOMENTUM * mbuf[k, :, cs] + g_sum
            mbuf[k, :, cs] = m_new
            x_zero = g_sum + MOMENTUM * m_new
            x0[k, :, cs] = x_zero
            return acc + x_zero * x_zero

        acc = lax.fori_loop(0, cols // step, col_step, jnp.zeros((rows, step), F32))
        oc = pltpu.make_async_copy(mbuf.at[k], mnew_hbm.at[k], out_sem.at[k])
        oc.start()
        out_copies.append(oc)
        return jnp.where(tile_rows == k, jnp.sum(acc), norm_tile)

    norm_copies = []
    here = y * SIDE + x

    def normalise(r, mats, tile):
        nown[r] = tile
        pair_copy = remote(nown.at[r], npair.at[r], nsend.at[r, 0], nrcv.at[r, 0], partner)
        pair_copy.start()
        pair_copy.wait_recv()
        nall[r, here] = nown[r] + npair[r]
        copies = []
        for n, off in enumerate(others):
            py, px = peer(off)
            c = remote(nall.at[r, here], nall.at[r, here], nsend.at[r, 1 + n], nrcv.at[r, 1 + n], {'dp': py, 'fsdp': px})
            c.start()
            copies.append(c)
        for c in copies:
            c.wait_recv()
        norm_copies.extend(copies + [pair_copy])
        denom_all = jnp.sqrt(jnp.sum(nall[r], axis=0)) + NORM_EPS
        for k in mats:
            denom = denom_all[k:k + 1, 0:1]

            def div_step(i, carry, k=k, denom=denom):
                cs = pl.ds(pl.multiple_of(i * step, step), step)
                xrow[k, :, cs] = (x0[k, :, cs] / denom).astype(BF16)
                return carry

            lax.fori_loop(0, cols // step, div_step, 0)

    def exchange(src_of, dst_of, dst_all, mid, hold1, hold2, ssem, msem, h1sem, h2sem, fsem, idle):
        sends = []

        def send(src, dst, rsem, dev):
            c = remote(src, dst, ssem.at[len(sends)], rsem, dev)
            c.start()
            sends.append(c)

        ways = []
        for h in range(2):
            p, q = (x, y) if h == 0 else (y, x)
            near = [(lax.rem(c + 1, SIDE), lax.rem(c + SIDE - 1, SIDE), lax.rem(c + 2, SIDE)) for c in (p, q)]

            def yx(pp, qq, h=h):
                return (qq, pp) if h == 0 else (pp, qq)

            def dev(pp, qq, yx=yx):
                return dict(zip(('dp', 'fsdp'), yx(pp, qq)))

            def src(pp, qq, h=h, yx=yx):
                return src_of(*yx(pp, qq), h)

            def dst(pp, qq, h=h, yx=yx):
                return dst_of(*yx(pp, qq), h)

            ways.append((p, q, near[0], near[1], dev, src, dst))

        def second(h, o, piece):
            p, q, (pu, pd, pf), (qu, qd, qf), dev, src, dst = ways[h]
            start_p = (pd, pu, pf, p)[o]
            side, i = PLACE[o]
            send(piece(qf), hold2.at[h, side, i], h2sem.at[h, side, i], dev(p, (qu, qd)[side]))
            send(piece(qu), dst(start_p, q), fsem, dev(p, qu))
            send(piece(qd), dst(start_p, q), fsem, dev(p, qd))
            pltpu.make_async_copy(piece(q), dst(start_p, q), fsem).start()

        def relay2(h, o):
            p, q, (pu, pd, pf), (qu, qd, qf), dev, src, dst = ways[h]
            side, i = PLACE[o]
            held = hold2.at[h, side, i]
            pltpu.make_async_copy(held, held, h2sem.at[h, side, i]).wait()
            send(held, dst((pd, pu, pf, p)[o], (qd, qu)[side]), fsem, dev(p, (qu, qd)[side]))

        def near_pieces(i):
            for h in range(2):
                p, q, (pu, pd, pf), _, dev, src, dst = ways[h]
                for side, to in ((0, pu), (1, pd)):
                    send(src(to, i), mid.at[h, side, i], msem.at[h, side], dev(to, q))

        def far_pieces(i):
            for h in range(2):
                p, q, (pu, pd, pf), _, dev, src, dst = ways[h]
                for side, to in ((0, pu), (1, pd)):
                    send(src(pf, 2 * i + side), hold1.at[h, side, i], h1sem.at[h, side], dev(to, q))

        far_pieces(0)
        near_pieces(0)
        near_pieces(1)
        yield None
        far_pieces(1)
        idle()
        for h in range(2):
            p, q, (pu, pd, pf), _, dev, src, dst = ways[h]
            for side, to in ((0, pu), (1, pd)):
                held = hold1.at[h, side]
                pltpu.make_async_copy(held, held, h1sem.at[h, side]).wait()
                send(held, mid.at[h, 2, 2 * side:2 * side + 2], msem.at[h, 2 + side], dev(to, q))
        near_pieces(2)
        near_pieces(3)
        for h in range(2):
            second(h, 3, lambda qq, h=h: ways[h][5](ways[h][0], qq))
        for h in range(2):
            for side in range(2):
                got = mid.at[h, 2, 2 * side:2 * side + 2]
                pltpu.make_async_copy(got, got, msem.at[h, 2 + side]).wait()
            second(h, 2, lambda qq, h=h: mid.at[h, 2, (qq % 2) * 2 + qq // 2])
        for side in range(2):
            for h in range(2):
                got = mid.at[h, side]
                pltpu.make_async_copy(got, got, msem.at[h, side]).wait()
                second(h, side, lambda qq, h=h, side=side: mid.at[h, side, qq])
        for o in (3, 2, 0, 1):
            for h in range(2):
                relay2(h, o)
        pltpu.make_async_copy(dst_all, dst_all, fsem).wait()
        yield sends

    half_piece = quarter // 2

    def piece_ds(pos, h):
        return pl.ds(pl.multiple_of(pos * quarter + h * half_piece, half_piece), half_piece)

    def idle_first():
        for k in range(n_mat):
            for c in gcopies[k]:
                c.wait_send()
            out_copies[k].wait()
        for c in norm_copies:
            c.wait_send()

    my_mat, my_pos = mat_of(y, x), pos_of(y, x)
    to_columns = exchange(lambda py, px, h: xrow.at[mat_of(py, px), :, piece_ds(pos_of(py, px), h)],
                          lambda oy, ox, h: xfull.at[row_ds(ox * SIDE + oy), h * half_piece:(h + 1) * half_piece],
                          xfull, cmid, chold1, chold2, csend, cmsem, ch1sem, ch2sem, cfsem, idle_first)
    for k in range(n_mat):
        for j in (2, 3):
            gcopies[k][j].wait_recv()
            gcopies[k][j + 2].start()
        if k + 2 < n_mat:
            issue_grad(k + 2)
        if k > 0:
            norm_tile = momentum_step(k - 1, norm_tile)
    normalise(0, range(n_mat - 1), norm_tile)
    next(to_columns)
    normalise(1, range(n_mat - 1, n_mat), momentum_step(n_mat - 1, norm_tile))
    col_copies = next(to_columns)


    fy, fx = y + 1 - 2 * (y % 2), x + 1 - 2 * (x % 2)
    square = ((y, fx), (fy, x), (fy, fx))
    chunk = HALF * BLK // 4

    def chunk_ds(pos):
        return pl.ds(pl.multiple_of(pos * chunk, chunk), chunk)

    def packed_ds(core, pos):
        return pl.ds(pl.multiple_of(core * (HALF * BLK) + pos * chunk, chunk), chunk)

    bcol = min(256, quarter)

    near_x, near_y, diagonal = (pos_of(*c) for c in square)
    to_x, to_y = {'fsdp': fx}, {'dp': fy}
    sub = chunk // 2

    def sub_ds(pos, h):
        return pl.ds(pl.multiple_of(pos * chunk + h * sub, sub), sub)

    def pair_of(it, n):
        cs = chunk_ds((diagonal, near_x, near_y, my_pos)[n])
        return remote(part.at[it, 1 - t, cs, :], drecv.at[it, cs, :], dsend.at[it, n], drcv.at[it, n], partner)

    def reduce_of(it, n):
        src = (red.at[it, sub_ds(diagonal, 0), :], red.at[it, sub_ds(diagonal, 1), :],
               red.at[it, sub_ds(near_x, 0), :], red.at[it, sub_ds(near_y, 1), :],
               comb.at[it, 0], comb.at[it, 1])[n]
        to = (to_x, to_y, to_x, to_y, to_y, to_x)[n]
        return remote(src, rsrecv.at[it, n], rssend.at[it, n], rsrcv.at[it, n], to)

    def gather_of(it, n):
        mine = agbuf.at[it, packed_ds(t, my_pos), :]
        py, px = square[n]
        return remote(mine, mine, agsend.at[it, n], agrcv.at[it, n], {'dp': py, 'fsdp': px})

    def forward_of(it, n):
        pos = my_pos if n == 0 else pos_of(*square[n - 1])
        held = agbuf.at[it, packed_ds(t, pos), :]
        return remote(held, held, fwsend.at[it, n], fwrcv.at[it, n], partner)

    def drain(it):
        for n in range(4):
            pair_of(it, n).wait_send()
            forward_of(it, n).wait_send()
        for n in range(6):
            reduce_of(it, n).wait_send()
        for n in range(3):
            gather_of(it, n).wait_send()

    def half_gram(it, h):
        nt = (((1,), (1,)), ((), ()))
        pair_rows = xfull[pl.ds(pl.multiple_of(h * 2 * BLK, 2 * BLK), 2 * BLK), :]
        square_gram = lax.dot_general(pair_rows, pair_rows, nt, preferred_element_type=F32)
        cross_gram = lax.dot_general(xfull[pl.ds(pl.multiple_of(h * BLK, BLK), BLK), :], xfull[2 * BLK:, :], nt,
                                     preferred_element_type=F32)
        blocks = (square_gram[:BLK, :BLK], square_gram[:BLK, BLK:], square_gram[BLK:, BLK:],
                  cross_gram[:, :BLK], cross_gram[:, BLK:])
        for n, block in enumerate(blocks):
            part[it, h, n * BLK:(n + 1) * BLK, :] = block

    def iteration(it, carry):
        half_gram(it, 1 - t)
        for n in range(4):
            pair_of(it, n).start()
        half_gram(it, t)
        for n, pos in enumerate((diagonal, near_x, near_y, my_pos)):
            pair_of(it, n).wait_recv()
            cs = chunk_ds(pos)
            red[it, cs, :] = part[it, t, cs, :] + drecv[it, cs, :]
            for m in ((0, 1), (2,), (3,), ())[n]:
                reduce_of(it, m).start()
        reduce_of(it, 0).wait_recv()
        comb[it, 0] = red[it, sub_ds(near_y, 0), :] + rsrecv[it, 0]
        reduce_of(it, 4).start()
        reduce_of(it, 1).wait_recv()
        comb[it, 1] = red[it, sub_ds(near_x, 1), :] + rsrecv[it, 1]
        reduce_of(it, 5).start()

        @pl.when(it > 0)
        def _():
            drain(it - 1)

        for h in range(2):
            reduce_of(it, 2 + h).wait_recv()
            reduce_of(it, 4 + h).wait_recv()
            total = (red[it, sub_ds(my_pos, h), :] + rsrecv[it, 2 + h]) + rsrecv[it, 4 + h]
            mine = pl.ds(pl.multiple_of(t * (HALF * BLK) + my_pos * chunk + h * sub, sub), sub)
            agbuf[it, mine, :] = total.astype(BF16)
        for n in (2, 0, 1):
            gather_of(it, n).start()
        forward_of(it, 0).start()
        for n in range(3):
            gather_of(it, n).wait_recv()
            forward_of(it, n + 1).start()
        for n in range(4):
            forward_of(it, n).wait_recv()
        for n, (bi, bj) in enumerate(TRI):
            block = agbuf[it, n * BLK:(n + 1) * BLK, :]
            amat[bi * BLK:(bi + 1) * BLK, bj * BLK:(bj + 1) * BLK] = block
            if bi != bj:
                amat[bj * BLK:(bj + 1) * BLK, bi * BLK:(bi + 1) * BLK] = block.astype(F32).T.astype(BF16)
        for bi in range(2):
            rs = slice(2 * BLK * bi, 2 * BLK * (bi + 1))
            sq = jnp.dot(amat[rs, :], amat[...], preferred_element_type=F32).astype(BF16)
            bmat[rs, :] = (COEF_B * amat[rs, :].astype(F32) + COEF_C * sq.astype(F32)).astype(BF16)

        for i in range(quarter // bcol):
            cs = slice(i * bcol, (i + 1) * bcol)
            x_old = xfull[:, cs]
            prod = jnp.dot(bmat[...], x_old, preferred_element_type=F32)
            xfull[:, cs] = (COEF_A * x_old.astype(F32) + prod).astype(BF16)
        return carry

    for c in col_copies:
        c.wait_send()
    lax.fori_loop(0, NS_STEPS, iteration, 0)

    to_rows = exchange(lambda py, px, h: xfull.at[row_ds(px * SIDE + py), h * half_piece:(h + 1) * half_piece],
                           lambda oy, ox, h: xfin_hbm.at[mat_of(oy, ox), :, piece_ds(pos_of(oy, ox), h)],
                           xfin_hbm, bmid, bhold1, bhold2, bsend, bmsem, bh1sem, bh2sem, bfsem, lambda: drain(NS_STEPS - 1))
    next(to_rows)
    back_copies = next(to_rows)

    for c in back_copies:
        c.wait_send()


def run_kernel(m_blk, g_blk):
    n_mat, rows, cols = m_blk.shape
    all_rows = rows * SIDE * SIDE
    quarter = cols // SIDE
    packed = len(TRI) * BLK
    chunk = packed // 8
    n_oth = SIDE * SIDE - 1
    dma = pltpu.SemaphoreType.DMA
    half_piece = (rows, quarter // 2)
    relays = [
        pltpu.VMEM((2, 3, SIDE) + half_piece, BF16),
        pltpu.VMEM((2, 2, 2) + half_piece, BF16),
        pltpu.VMEM((2, 2, 2) + half_piece, BF16),
    ]
    relay_sems = [dma((60,)), dma((2, 4)), dma((2, 2)), dma((2, 2, 2)), dma]
    scratch = [
        pltpu.VMEM((n_mat, rows, cols), BF16),
        pltpu.VMEM((n_mat, 3, rows, cols), BF16),
        pltpu.VMEM((n_mat, 2, rows, cols // 2), BF16),
        pltpu.VMEM((n_mat, rows, cols), F32),
        pltpu.VMEM((n_mat, rows, cols), F32),
        pltpu.VMEM((n_mat, rows, cols), BF16),
        pltpu.VMEM((all_rows, quarter), BF16),
        pltpu.VMEM((2, 8, 128), F32),
        pltpu.VMEM((2, 8, 128), F32),
        pltpu.VMEM((2, SIDE * SIDE, 8, 128), F32),
        pltpu.VMEM((NS_STEPS, 2, packed // 2, BLK), F32),
        pltpu.VMEM((NS_STEPS, packed // 2, BLK), F32),
        pltpu.VMEM((NS_STEPS, packed // 2, BLK), F32),
        pltpu.VMEM((NS_STEPS, 2, chunk // 2, BLK), F32),
        pltpu.VMEM((NS_STEPS, 6, chunk // 2, BLK), F32),
        pltpu.VMEM((NS_STEPS, packed, BLK), BF16),
        pltpu.VMEM((all_rows, all_rows), BF16),
        pltpu.VMEM((all_rows, all_rows), BF16),
        *relays, *relays,
        dma((2, n_mat)), dma((n_mat,)), dma((n_mat, 6)), dma((n_mat, 6)),
        dma((2, n_oth + 1)), dma((2, n_oth + 1)), *relay_sems, *relay_sems,
        dma((NS_STEPS, 4)), dma((NS_STEPS, 4)), dma((NS_STEPS, 6)), dma((NS_STEPS, 6)),
        dma((NS_STEPS, 3)), dma((NS_STEPS, 3)), dma((NS_STEPS, 4)), dma((NS_STEPS, 4)), pltpu.SemaphoreType.REGULAR((3,)),
    ]
    anyspace = pl.BlockSpec(memory_space=pl.ANY)
    return pl.pallas_call(
        muon_kernel,
        out_shape=(jax.ShapeDtypeStruct(m_blk.shape, F32), jax.ShapeDtypeStruct(m_blk.shape, BF16)),
        in_specs=[anyspace, anyspace],
        out_specs=(anyspace, anyspace),
        scratch_shapes=scratch,
        compiler_params=pltpu.CompilerParams(collective_id=0, has_side_effects=True, vmem_limit_bytes=VMEM_MIB * 2 ** 20),
        name='muon_group',
    )(m_blk, g_blk)


def solution(mesh):
    mat_spec = P('stage', ROW_AXES, 'tp')
    grad_spec = P(('stage', 'dp'), None, 'fsdp', 'tp')
    tp_size = mesh.shape['tp']

    def local_step(w_blk, m_blk, g_blk):
        m_new, x_fin = run_kernel(m_blk, g_blk.reshape(g_blk.shape[1:]))
        col_count = w_blk.shape[2] * tp_size
        update_scale = LEARN_RATE * 0.2 * math.sqrt(col_count)
        decay_factor = 1.0 - LEARN_RATE * WEIGHT_DECAY
        w_new = decay_factor * w_blk - update_scale * x_fin.astype(F32)
        return w_new, m_new

    return jax.shard_map(local_step, mesh=mesh, in_specs=(mat_spec, mat_spec, grad_spec), out_specs=(mat_spec, mat_spec), check_vma=False)
```

```python
import functools
import math
import jax
import jax.numpy as jnp
from jax import lax
from jax.experimental import pallas as pl
from jax.experimental.pallas import tpu as pltpu
from jax.sharding import PartitionSpec as P

MOMENTUM = 0.95
LEARN_RATE = 0.1
WEIGHT_DECAY = 0.1
COEF_A = 3.4445
COEF_B = -4.7750
COEF_C = 2.0315
NORM_EPS = 1e-7
NS_STEPS = 5
ROW_AXES = ('fsdp', 'dp')
F32 = jnp.float32
BF16 = jnp.bfloat16
MESH = pl.DeviceIdType.MESH
VMEM_MIB = 47
SIDE = 4
BLK = 128
TRI = ((0, 0), (0, 1), (1, 1), (0, 2), (0, 3), (2, 2), (2, 3), (3, 3), (1, 2), (1, 3))
HALF = len(TRI) // 2
PLACE = ((0, 1), (1, 0), (1, 1), (0, 0))


def muon_kernel(m_hbm, g_hbm, mnew_hbm, xfin_hbm,
                gown, grecv, relay, mbuf, x0, xrow, xfull,
                nown, npair, nall, part, drecv, red, comb, rsrecv, agbuf, amat, bmat,
                cmid, chold1, chold2, bmid, bhold1, bhold2,
                load_sem, out_sem, gsend, grcv, nsend, nrcv, csend, cmsem, ch1sem, ch2sem, cfsem,
                bsend, bmsem, bh1sem, bh2sem, bfsem,
                dsend, drcv, rssend, rsrcv, agsend, agrcv, fwsend, fwrcv, round_sem):
    n_mat, rows, cols = mbuf.shape
    quarter = cols // SIDE
    half = cols // 2
    y = lax.axis_index('dp')
    x = lax.axis_index('fsdp')
    t = lax.axis_index('tp')
    partner = {'tp': 1 - t}
    up = lax.rem(y + 1, SIDE)
    down = lax.rem(y + SIDE - 1, SIDE)
    far = lax.rem(y + 2, SIDE)

    def row_ds(i):
        return pl.ds(pl.multiple_of(i * rows, rows), rows)

    def quarter_ds(i):
        return pl.ds(pl.multiple_of(i * quarter, quarter), quarter)

    def mat_of(yy, xx):
        return (yy // 2) * 2 + xx // 2

    def pos_of(yy, xx):
        return (yy % 2) * 2 + xx % 2

    loads = []
    for k in range(n_mat):
        loads.append((pltpu.make_async_copy(g_hbm.at[k, row_ds(y), :], gown.at[k], load_sem.at[0, k]),
                      pltpu.make_async_copy(m_hbm.at[k], mbuf.at[k], load_sem.at[1, k])))
        for c in loads[-1]:
            c.start()

    others = [(oy, ox) for oy in range(SIDE) for ox in range(SIDE) if (oy, ox) != (0, 0)]

    def peer(off):
        return lax.rem(y + off[0], SIDE), lax.rem(x + off[1], SIDE)

    xup, xdown = lax.rem(x + 1, SIDE), lax.rem(x + SIDE - 1, SIDE)
    neighbours = ({'dp': up}, {'dp': down}, {'fsdp': xup}, {'fsdp': xdown})
    barrier = pltpu.get_barrier_semaphore()
    for dev in neighbours + (partner,):
        pl.semaphore_signal(barrier, inc=1, device_id=dev, device_id_type=MESH)
    pl.semaphore_wait(barrier, 5)

    def remote(src, dst, ssem, rsem, dev):
        return pltpu.make_async_remote_copy(src_ref=src, dst_ref=dst, send_sem=ssem, recv_sem=rsem,
                                            device_id=dev, device_id_type=MESH)

    lo, hi = pl.ds(0, half), pl.ds(half, half)

    def grad_copies(k):
        to_up, to_down = {'dp': up}, {'dp': down}
        return (
            remote(g_hbm.at[k, row_ds(up), :], grecv.at[k, 0], gsend.at[k, 0], grcv.at[k, 0], to_up),
            remote(g_hbm.at[k, row_ds(down), :], grecv.at[k, 1], gsend.at[k, 1], grcv.at[k, 1], to_down),
            remote(g_hbm.at[k, row_ds(far), lo], relay.at[k, 0], gsend.at[k, 2], grcv.at[k, 2], to_up),
            remote(g_hbm.at[k, row_ds(far), hi], relay.at[k, 1], gsend.at[k, 3], grcv.at[k, 3], to_down),
            remote(relay.at[k, 0], grecv.at[k, 2, :, lo], gsend.at[k, 4], grcv.at[k, 4], to_up),
            remote(relay.at[k, 1], grecv.at[k, 2, :, hi], gsend.at[k, 5], grcv.at[k, 5], to_down),
        )

    gcopies = [grad_copies(k) for k in range(n_mat)]

    def issue_grad(k):
        for j in (2, 3, 0, 1):
            gcopies[k][j].start()

    issue_grad(0)
    issue_grad(1)
    for n in range(3):
        for dev in neighbours:
            pl.semaphore_signal(round_sem.at[n], inc=1, device_id=dev, device_id_type=MESH)
        pl.semaphore_wait(round_sem.at[n], 4)
    step = min(512, cols)
    out_copies = []
    tile_rows = lax.broadcasted_iota(jnp.int32, (8, 128), 0)
    norm_tile = jnp.zeros((8, 128), F32)

    def momentum_step(k, norm_tile):
        for c in loads[k]:
            c.wait()
        for j in (0, 1, 4, 5):
            gcopies[k][j].wait_recv()

        def col_step(i, acc):
            cs = pl.ds(pl.multiple_of(i * step, step), step)
            g_sum = (gown[k, :, cs].astype(F32) + grecv[k, 0, :, cs].astype(F32)) + (
                grecv[k, 1, :, cs].astype(F32) + grecv[k, 2, :, cs].astype(F32))
            m_new = MOMENTUM * mbuf[k, :, cs] + g_sum
            mbuf[k, :, cs] = m_new
            x_zero = g_sum + MOMENTUM * m_new
            x0[k, :, cs] = x_zero
            return acc + x_zero * x_zero

        acc = lax.fori_loop(0, cols // step, col_step, jnp.zeros((rows, step), F32))
        oc = pltpu.make_async_copy(mbuf.at[k], mnew_hbm.at[k], out_sem.at[k])
        oc.start()
        out_copies.append(oc)
        return jnp.where(tile_rows == k, jnp.sum(acc), norm_tile)

    for k in range(n_mat):
        for j in (2, 3):
            gcopies[k][j].wait_recv()
            gcopies[k][j + 2].start()
        if k + 2 < n_mat:
            issue_grad(k + 2)
        if k > 0:
            norm_tile = momentum_step(k - 1, norm_tile)
    norm_tile = momentum_step(n_mat - 1, norm_tile)

    nown[...] = norm_tile
    pair_copy = remote(nown, npair, nsend.at[0], nrcv.at[0], partner)
    pair_copy.start()
    pair_copy.wait_recv()
    here = y * SIDE + x
    nall[here] = nown[...] + npair[...]
    norm_copies = []
    for n, off in enumerate(others):
        py, px = peer(off)
        c = remote(nall.at[here], nall.at[here], nsend.at[1 + n], nrcv.at[1 + n], {'dp': py, 'fsdp': px})
        c.start()
        norm_copies.append(c)
    for c in norm_copies:
        c.wait_recv()
    sq_all = jnp.sum(nall[...], axis=0)
    denom_all = jnp.sqrt(sq_all) + NORM_EPS

    for k in range(n_mat):
        denom = denom_all[k:k + 1, 0:1]

        def div_step(i, carry, k=k, denom=denom):
            cs = pl.ds(pl.multiple_of(i * step, step), step)
            xrow[k, :, cs] = (x0[k, :, cs] / denom).astype(BF16)
            return carry

        lax.fori_loop(0, cols // step, div_step, 0)

    def exchange(src_of, dst_of, dst_all, mid, hold1, hold2, ssem, msem, h1sem, h2sem, fsem, idle):
        sends = []

        def send(src, dst, rsem, dev):
            c = remote(src, dst, ssem.at[len(sends)], rsem, dev)
            c.start()
            sends.append(c)

        ways = []
        for h in range(2):
            p, q = (x, y) if h == 0 else (y, x)
            near = [(lax.rem(c + 1, SIDE), lax.rem(c + SIDE - 1, SIDE), lax.rem(c + 2, SIDE)) for c in (p, q)]

            def yx(pp, qq, h=h):
                return (qq, pp) if h == 0 else (pp, qq)

            def dev(pp, qq, yx=yx):
                return dict(zip(('dp', 'fsdp'), yx(pp, qq)))

            def src(pp, qq, h=h, yx=yx):
                return src_of(*yx(pp, qq), h)

            def dst(pp, qq, h=h, yx=yx):
                return dst_of(*yx(pp, qq), h)

            ways.append((p, q, near[0], near[1], dev, src, dst))

        def second(h, o, piece):
            p, q, (pu, pd, pf), (qu, qd, qf), dev, src, dst = ways[h]
            start_p = (pd, pu, pf, p)[o]
            side, i = PLACE[o]
            send(piece(qf), hold2.at[h, side, i], h2sem.at[h, side, i], dev(p, (qu, qd)[side]))
            send(piece(qu), dst(start_p, q), fsem, dev(p, qu))
            send(piece(qd), dst(start_p, q), fsem, dev(p, qd))
            pltpu.make_async_copy(piece(q), dst(start_p, q), fsem).start()

        def relay2(h, o):
            p, q, (pu, pd, pf), (qu, qd, qf), dev, src, dst = ways[h]
            side, i = PLACE[o]
            held = hold2.at[h, side, i]
            pltpu.make_async_copy(held, held, h2sem.at[h, side, i]).wait()
            send(held, dst((pd, pu, pf, p)[o], (qd, qu)[side]), fsem, dev(p, (qu, qd)[side]))

        def near_pieces(i):
            for h in range(2):
                p, q, (pu, pd, pf), _, dev, src, dst = ways[h]
                for side, to in ((0, pu), (1, pd)):
                    send(src(to, i), mid.at[h, side, i], msem.at[h, side], dev(to, q))

        for h in range(2):
            p, q, (pu, pd, pf), _, dev, src, dst = ways[h]
            for side, to in ((0, pu), (1, pd)):
                for i in range(2):
                    send(src(pf, 2 * side + i), hold1.at[h, side, i], h1sem.at[h, side], dev(to, q))
        near_pieces(0)
        near_pieces(1)
        idle()
        for h in range(2):
            p, q, (pu, pd, pf), _, dev, src, dst = ways[h]
            for side, to in ((0, pu), (1, pd)):
                held = hold1.at[h, side]
                pltpu.make_async_copy(held, held, h1sem.at[h, side]).wait()
                send(held, mid.at[h, 2, 2 * side:2 * side + 2], msem.at[h, 2 + side], dev(to, q))
        near_pieces(2)
        near_pieces(3)
        for h in range(2):
            second(h, 3, lambda qq, h=h: ways[h][5](ways[h][0], qq))
        for h in range(2):
            for side in range(2):
                got = mid.at[h, 2, 2 * side:2 * side + 2]
                pltpu.make_async_copy(got, got, msem.at[h, 2 + side]).wait()
            second(h, 2, lambda qq, h=h: mid.at[h, 2, qq])
        for side in range(2):
            for h in range(2):
                got = mid.at[h, side]
                pltpu.make_async_copy(got, got, msem.at[h, side]).wait()
                second(h, side, lambda qq, h=h, side=side: mid.at[h, side, qq])
        for o in (3, 2, 0, 1):
            for h in range(2):
                relay2(h, o)
        pltpu.make_async_copy(dst_all, dst_all, fsem).wait()
        return sends

    half_piece = quarter // 2

    def piece_ds(pos, h):
        return pl.ds(pl.multiple_of(pos * quarter + h * half_piece, half_piece), half_piece)

    def idle_first():
        for k in range(n_mat):
            for c in gcopies[k]:
                c.wait_send()
            out_copies[k].wait()
        for c in [pair_copy] + norm_copies:
            c.wait_send()

    my_mat, my_pos = mat_of(y, x), pos_of(y, x)
    col_copies = exchange(lambda py, px, h: xrow.at[mat_of(py, px), :, piece_ds(pos_of(py, px), h)],
                          lambda oy, ox, h: xfull.at[row_ds(ox * SIDE + oy), h * half_piece:(h + 1) * half_piece],
                          xfull, cmid, chold1, chold2, csend, cmsem, ch1sem, ch2sem, cfsem, idle_first)

    fy, fx = y + 1 - 2 * (y % 2), x + 1 - 2 * (x % 2)
    square = ((y, fx), (fy, x), (fy, fx))
    chunk = HALF * BLK // 4

    def chunk_ds(pos):
        return pl.ds(pl.multiple_of(pos * chunk, chunk), chunk)

    def packed_ds(core, pos):
        return pl.ds(pl.multiple_of(core * (HALF * BLK) + pos * chunk, chunk), chunk)

    bcol = min(256, quarter)

    near_x, near_y, diagonal = (pos_of(*c) for c in square)
    to_x, to_y = {'fsdp': fx}, {'dp': fy}
    sub = chunk // 2

    def sub_ds(pos, h):
        return pl.ds(pl.multiple_of(pos * chunk + h * sub, sub), sub)

    def pair_of(it):
        return remote(part.at[it, 1 - t], drecv.at[it], dsend.at[it], drcv.at[it], partner)

    def reduce_of(it, n):
        src = (red.at[it, sub_ds(diagonal, 0), :], red.at[it, sub_ds(diagonal, 1), :],
               red.at[it, sub_ds(near_x, 0), :], red.at[it, sub_ds(near_y, 1), :],
               comb.at[it, 0], comb.at[it, 1])[n]
        to = (to_x, to_y, to_x, to_y, to_y, to_x)[n]
        return remote(src, rsrecv.at[it, n], rssend.at[it, n], rsrcv.at[it, n], to)

    def gather_of(it, n):
        mine = agbuf.at[it, packed_ds(t, my_pos), :]
        py, px = square[n]
        return remote(mine, mine, agsend.at[it, n], agrcv.at[it, n], {'dp': py, 'fsdp': px})

    def forward_of(it, n):
        pos = my_pos if n == 0 else pos_of(*square[n - 1])
        held = agbuf.at[it, packed_ds(t, pos), :]
        return remote(held, held, fwsend.at[it, n], fwrcv.at[it, n], partner)

    def drain(it):
        pair_of(it).wait_send()
        for n in range(4):
            forward_of(it, n).wait_send()
        for n in range(6):
            reduce_of(it, n).wait_send()
        for n in range(3):
            gather_of(it, n).wait_send()

    def half_gram(it, h):
        nt = (((1,), (1,)), ((), ()))
        pair_rows = xfull[pl.ds(pl.multiple_of(h * 2 * BLK, 2 * BLK), 2 * BLK), :]
        square_gram = lax.dot_general(pair_rows, pair_rows, nt, preferred_element_type=F32)
        cross_gram = lax.dot_general(xfull[pl.ds(pl.multiple_of(h * BLK, BLK), BLK), :], xfull[2 * BLK:, :], nt,
                                     preferred_element_type=F32)
        blocks = (square_gram[:BLK, :BLK], square_gram[:BLK, BLK:], square_gram[BLK:, BLK:],
                  cross_gram[:, :BLK], cross_gram[:, BLK:])
        for n, block in enumerate(blocks):
            part[it, h, n * BLK:(n + 1) * BLK, :] = block

    def iteration(it, carry):
        half_gram(it, 1 - t)
        pair_of(it).start()
        half_gram(it, t)
        pair_of(it).wait_recv()
        for n, pos in enumerate((diagonal, near_x, near_y, my_pos)):
            cs = chunk_ds(pos)
            red[it, cs, :] = part[it, t, cs, :] + drecv[it, cs, :]
            for m in ((0, 1), (2,), (3,), ())[n]:
                reduce_of(it, m).start()
        reduce_of(it, 0).wait_recv()
        comb[it, 0] = red[it, sub_ds(near_y, 0), :] + rsrecv[it, 0]
        reduce_of(it, 4).start()
        reduce_of(it, 1).wait_recv()
        comb[it, 1] = red[it, sub_ds(near_x, 1), :] + rsrecv[it, 1]
        reduce_of(it, 5).start()

        @pl.when(it > 0)
        def _():
            drain(it - 1)

        for h in range(2):
            reduce_of(it, 2 + h).wait_recv()
            reduce_of(it, 4 + h).wait_recv()
            total = (red[it, sub_ds(my_pos, h), :] + rsrecv[it, 2 + h]) + rsrecv[it, 4 + h]
            mine = pl.ds(pl.multiple_of(t * (HALF * BLK) + my_pos * chunk + h * sub, sub), sub)
            agbuf[it, mine, :] = total.astype(BF16)
        for n in (2, 0, 1):
            gather_of(it, n).start()
        forward_of(it, 0).start()
        for n in range(3):
            gather_of(it, n).wait_recv()
            forward_of(it, n + 1).start()
        for n in range(4):
            forward_of(it, n).wait_recv()
        for n, (bi, bj) in enumerate(TRI):
            block = agbuf[it, n * BLK:(n + 1) * BLK, :]
            amat[bi * BLK:(bi + 1) * BLK, bj * BLK:(bj + 1) * BLK] = block
            if bi != bj:
                amat[bj * BLK:(bj + 1) * BLK, bi * BLK:(bi + 1) * BLK] = block.astype(F32).T.astype(BF16)
        for bi in range(2):
            rs = slice(2 * BLK * bi, 2 * BLK * (bi + 1))
            sq = jnp.dot(amat[rs, :], amat[...], preferred_element_type=F32).astype(BF16)
            bmat[rs, :] = (COEF_B * amat[rs, :].astype(F32) + COEF_C * sq.astype(F32)).astype(BF16)

        for i in range(quarter // bcol):
            cs = slice(i * bcol, (i + 1) * bcol)
            x_old = xfull[:, cs]
            prod = jnp.dot(bmat[...], x_old, preferred_element_type=F32)
            xfull[:, cs] = (COEF_A * x_old.astype(F32) + prod).astype(BF16)
        return carry

    for c in col_copies:
        c.wait_send()
    lax.fori_loop(0, NS_STEPS, iteration, 0)

    back_copies = exchange(lambda py, px, h: xfull.at[row_ds(px * SIDE + py), h * half_piece:(h + 1) * half_piece],
                           lambda oy, ox, h: xfin_hbm.at[mat_of(oy, ox), :, piece_ds(pos_of(oy, ox), h)],
                           xfin_hbm, bmid, bhold1, bhold2, bsend, bmsem, bh1sem, bh2sem, bfsem, lambda: drain(NS_STEPS - 1))

    for c in back_copies:
        c.wait_send()


def run_kernel(m_blk, g_blk):
    n_mat, rows, cols = m_blk.shape
    all_rows = rows * SIDE * SIDE
    quarter = cols // SIDE
    packed = len(TRI) * BLK
    chunk = packed // 8
    n_oth = SIDE * SIDE - 1
    dma = pltpu.SemaphoreType.DMA
    half_piece = (rows, quarter // 2)
    relays = [
        pltpu.VMEM((2, 3, SIDE) + half_piece, BF16),
        pltpu.VMEM((2, 2, 2) + half_piece, BF16),
        pltpu.VMEM((2, 2, 2) + half_piece, BF16),
    ]
    relay_sems = [dma((60,)), dma((2, 4)), dma((2, 2)), dma((2, 2, 2)), dma]
    scratch = [
        pltpu.VMEM((n_mat, rows, cols), BF16),
        pltpu.VMEM((n_mat, 3, rows, cols), BF16),
        pltpu.VMEM((n_mat, 2, rows, cols // 2), BF16),
        pltpu.VMEM((n_mat, rows, cols), F32),
        pltpu.VMEM((n_mat, rows, cols), F32),
        pltpu.VMEM((n_mat, rows, cols), BF16),
        pltpu.VMEM((all_rows, quarter), BF16),
        pltpu.VMEM((8, 128), F32),
        pltpu.VMEM((8, 128), F32),
        pltpu.VMEM((SIDE * SIDE, 8, 128), F32),
        pltpu.VMEM((NS_STEPS, 2, packed // 2, BLK), F32),
        pltpu.VMEM((NS_STEPS, packed // 2, BLK), F32),
        pltpu.VMEM((NS_STEPS, packed // 2, BLK), F32),
        pltpu.VMEM((NS_STEPS, 2, chunk // 2, BLK), F32),
        pltpu.VMEM((NS_STEPS, 6, chunk // 2, BLK), F32),
        pltpu.VMEM((NS_STEPS, packed, BLK), BF16),
        pltpu.VMEM((all_rows, all_rows), BF16),
        pltpu.VMEM((all_rows, all_rows), BF16),
        *relays, *relays,
        dma((2, n_mat)), dma((n_mat,)), dma((n_mat, 6)), dma((n_mat, 6)),
        dma((n_oth + 1,)), dma((n_oth + 1,)), *relay_sems, *relay_sems,
        dma((NS_STEPS,)), dma((NS_STEPS,)), dma((NS_STEPS, 6)), dma((NS_STEPS, 6)),
        dma((NS_STEPS, 3)), dma((NS_STEPS, 3)), dma((NS_STEPS, 4)), dma((NS_STEPS, 4)), pltpu.SemaphoreType.REGULAR((3,)),
    ]
    anyspace = pl.BlockSpec(memory_space=pl.ANY)
    return pl.pallas_call(
        muon_kernel,
        out_shape=(jax.ShapeDtypeStruct(m_blk.shape, F32), jax.ShapeDtypeStruct(m_blk.shape, BF16)),
        in_specs=[anyspace, anyspace],
        out_specs=(anyspace, anyspace),
        scratch_shapes=scratch,
        compiler_params=pltpu.CompilerParams(collective_id=0, has_side_effects=True, vmem_limit_bytes=VMEM_MIB * 2 ** 20),
        name='muon_group',
    )(m_blk, g_blk)


def solution(mesh):
    mat_spec = P('stage', ROW_AXES, 'tp')
    grad_spec = P(('stage', 'dp'), None, 'fsdp', 'tp')
    tp_size = mesh.shape['tp']

    def local_step(w_blk, m_blk, g_blk):
        m_new, x_fin = run_kernel(m_blk, g_blk.reshape(g_blk.shape[1:]))
        col_count = w_blk.shape[2] * tp_size
        update_scale = LEARN_RATE * 0.2 * math.sqrt(col_count)
        decay_factor = 1.0 - LEARN_RATE * WEIGHT_DECAY
        w_new = decay_factor * w_blk - update_scale * x_fin.astype(F32)
        return w_new, m_new

    return jax.shard_map(local_step, mesh=mesh, in_specs=(mat_spec, mat_spec, grad_spec), out_specs=(mat_spec, mat_spec), check_vma=False)
```

```python
import functools
import math
import jax
import jax.numpy as jnp
from jax import lax
from jax.experimental import pallas as pl
from jax.experimental.pallas import tpu as pltpu
from jax.sharding import PartitionSpec as P

MOMENTUM = 0.95
LEARN_RATE = 0.1
WEIGHT_DECAY = 0.1
COEF_A = 3.4445
COEF_B = -4.7750
COEF_C = 2.0315
NORM_EPS = 1e-7
NS_STEPS = 5
ROW_AXES = ('fsdp', 'dp')
F32 = jnp.float32
BF16 = jnp.bfloat16
MESH = pl.DeviceIdType.MESH
VMEM_MIB = 47
SIDE = 4
BLK = 128
TRI = ((0, 0), (0, 1), (1, 1), (0, 2), (0, 3), (2, 2), (2, 3), (3, 3), (1, 2), (1, 3))
HALF = len(TRI) // 2
PLACE = ((0, 1), (1, 0), (1, 1), (0, 0))


def muon_kernel(m_hbm, g_hbm, mnew_hbm, xfin_hbm,
                gown, grecv, relay, mbuf, x0, xrow, xfull,
                nown, npair, nall, part, drecv, red, rsrecv, agbuf, amat, bmat,
                cmid, chold1, chold2, bmid, bhold1, bhold2,
                load_sem, out_sem, gsend, grcv, nsend, nrcv, csend, cmsem, ch1sem, ch2sem, cfsem,
                bsend, bmsem, bh1sem, bh2sem, bfsem,
                dsend, drcv, rssend, rsrcv, agsend, agrcv, fwsend, fwrcv, round_sem):
    n_mat, rows, cols = mbuf.shape
    quarter = cols // SIDE
    half = cols // 2
    y = lax.axis_index('dp')
    x = lax.axis_index('fsdp')
    t = lax.axis_index('tp')
    partner = {'tp': 1 - t}
    up = lax.rem(y + 1, SIDE)
    down = lax.rem(y + SIDE - 1, SIDE)
    far = lax.rem(y + 2, SIDE)

    def row_ds(i):
        return pl.ds(pl.multiple_of(i * rows, rows), rows)

    def quarter_ds(i):
        return pl.ds(pl.multiple_of(i * quarter, quarter), quarter)

    def mat_of(yy, xx):
        return (yy // 2) * 2 + xx // 2

    def pos_of(yy, xx):
        return (yy % 2) * 2 + xx % 2

    loads = []
    for k in range(n_mat):
        loads.append((pltpu.make_async_copy(g_hbm.at[k, row_ds(y), :], gown.at[k], load_sem.at[0, k]),
                      pltpu.make_async_copy(m_hbm.at[k], mbuf.at[k], load_sem.at[1, k])))
        for c in loads[-1]:
            c.start()

    others = [(oy, ox) for oy in range(SIDE) for ox in range(SIDE) if (oy, ox) != (0, 0)]

    def peer(off):
        return lax.rem(y + off[0], SIDE), lax.rem(x + off[1], SIDE)

    xup, xdown = lax.rem(x + 1, SIDE), lax.rem(x + SIDE - 1, SIDE)
    neighbours = ({'dp': up}, {'dp': down}, {'fsdp': xup}, {'fsdp': xdown})
    barrier = pltpu.get_barrier_semaphore()
    for dev in neighbours + (partner,):
        pl.semaphore_signal(barrier, inc=1, device_id=dev, device_id_type=MESH)
    pl.semaphore_wait(barrier, 5)

    def remote(src, dst, ssem, rsem, dev):
        return pltpu.make_async_remote_copy(src_ref=src, dst_ref=dst, send_sem=ssem, recv_sem=rsem,
                                            device_id=dev, device_id_type=MESH)

    lo, hi = pl.ds(0, half), pl.ds(half, half)

    def grad_copies(k):
        to_up, to_down = {'dp': up}, {'dp': down}
        return (
            remote(g_hbm.at[k, row_ds(up), :], grecv.at[k, 0], gsend.at[k, 0], grcv.at[k, 0], to_up),
            remote(g_hbm.at[k, row_ds(down), :], grecv.at[k, 1], gsend.at[k, 1], grcv.at[k, 1], to_down),
            remote(g_hbm.at[k, row_ds(far), lo], relay.at[k, 0], gsend.at[k, 2], grcv.at[k, 2], to_up),
            remote(g_hbm.at[k, row_ds(far), hi], relay.at[k, 1], gsend.at[k, 3], grcv.at[k, 3], to_down),
            remote(relay.at[k, 0], grecv.at[k, 2, :, lo], gsend.at[k, 4], grcv.at[k, 4], to_up),
            remote(relay.at[k, 1], grecv.at[k, 2, :, hi], gsend.at[k, 5], grcv.at[k, 5], to_down),
        )

    gcopies = [grad_copies(k) for k in range(n_mat)]

    def issue_grad(k):
        for j in (2, 3, 0, 1):
            gcopies[k][j].start()

    issue_grad(0)
    issue_grad(1)
    for n in range(3):
        for dev in neighbours:
            pl.semaphore_signal(round_sem.at[n], inc=1, device_id=dev, device_id_type=MESH)
        pl.semaphore_wait(round_sem.at[n], 4)
    step = min(512, cols)
    out_copies = []
    tile_rows = lax.broadcasted_iota(jnp.int32, (8, 128), 0)
    norm_tile = jnp.zeros((8, 128), F32)

    def momentum_step(k, norm_tile):
        for c in loads[k]:
            c.wait()
        for j in (0, 1, 4, 5):
            gcopies[k][j].wait_recv()

        def col_step(i, acc):
            cs = pl.ds(pl.multiple_of(i * step, step), step)
            g_sum = (gown[k, :, cs].astype(F32) + grecv[k, 0, :, cs].astype(F32)) + (
                grecv[k, 1, :, cs].astype(F32) + grecv[k, 2, :, cs].astype(F32))
            m_new = MOMENTUM * mbuf[k, :, cs] + g_sum
            mbuf[k, :, cs] = m_new
            x_zero = g_sum + MOMENTUM * m_new
            x0[k, :, cs] = x_zero
            return acc + x_zero * x_zero

        acc = lax.fori_loop(0, cols // step, col_step, jnp.zeros((rows, step), F32))
        oc = pltpu.make_async_copy(mbuf.at[k], mnew_hbm.at[k], out_sem.at[k])
        oc.start()
        out_copies.append(oc)
        return jnp.where(tile_rows == k, jnp.sum(acc), norm_tile)

    for k in range(n_mat):
        for j in (2, 3):
            gcopies[k][j].wait_recv()
            gcopies[k][j + 2].start()
        if k + 2 < n_mat:
            issue_grad(k + 2)
        if k > 0:
            norm_tile = momentum_step(k - 1, norm_tile)
    norm_tile = momentum_step(n_mat - 1, norm_tile)

    nown[...] = norm_tile
    pair_copy = remote(nown, npair, nsend.at[0], nrcv.at[0], partner)
    pair_copy.start()
    pair_copy.wait_recv()
    here = y * SIDE + x
    nall[here] = nown[...] + npair[...]
    norm_copies = []
    for n, off in enumerate(others):
        py, px = peer(off)
        c = remote(nall.at[here], nall.at[here], nsend.at[1 + n], nrcv.at[1 + n], {'dp': py, 'fsdp': px})
        c.start()
        norm_copies.append(c)
    for c in norm_copies:
        c.wait_recv()
    sq_all = jnp.sum(nall[...], axis=0)
    denom_all = jnp.sqrt(sq_all) + NORM_EPS

    for k in range(n_mat):
        denom = denom_all[k:k + 1, 0:1]

        def div_step(i, carry, k=k, denom=denom):
            cs = pl.ds(pl.multiple_of(i * step, step), step)
            xrow[k, :, cs] = (x0[k, :, cs] / denom).astype(BF16)
            return carry

        lax.fori_loop(0, cols // step, div_step, 0)

    def exchange(src_of, dst_of, dst_all, mid, hold1, hold2, ssem, msem, h1sem, h2sem, fsem, idle):
        sends = []

        def send(src, dst, rsem, dev):
            c = remote(src, dst, ssem.at[len(sends)], rsem, dev)
            c.start()
            sends.append(c)

        ways = []
        for h in range(2):
            p, q = (x, y) if h == 0 else (y, x)
            near = [(lax.rem(c + 1, SIDE), lax.rem(c + SIDE - 1, SIDE), lax.rem(c + 2, SIDE)) for c in (p, q)]

            def yx(pp, qq, h=h):
                return (qq, pp) if h == 0 else (pp, qq)

            def dev(pp, qq, yx=yx):
                return dict(zip(('dp', 'fsdp'), yx(pp, qq)))

            def src(pp, qq, h=h, yx=yx):
                return src_of(*yx(pp, qq), h)

            def dst(pp, qq, h=h, yx=yx):
                return dst_of(*yx(pp, qq), h)

            ways.append((p, q, near[0], near[1], dev, src, dst))

        def second(h, o, piece):
            p, q, (pu, pd, pf), (qu, qd, qf), dev, src, dst = ways[h]
            start_p = (pd, pu, pf, p)[o]
            side, i = PLACE[o]
            send(piece(qf), hold2.at[h, side, i], h2sem.at[h, side, i], dev(p, (qu, qd)[side]))
            send(piece(qu), dst(start_p, q), fsem, dev(p, qu))
            send(piece(qd), dst(start_p, q), fsem, dev(p, qd))
            pltpu.make_async_copy(piece(q), dst(start_p, q), fsem).start()

        def relay2(h, o):
            p, q, (pu, pd, pf), (qu, qd, qf), dev, src, dst = ways[h]
            side, i = PLACE[o]
            held = hold2.at[h, side, i]
            pltpu.make_async_copy(held, held, h2sem.at[h, side, i]).wait()
            send(held, dst((pd, pu, pf, p)[o], (qd, qu)[side]), fsem, dev(p, (qu, qd)[side]))

        def near_pieces(i):
            for h in range(2):
                p, q, (pu, pd, pf), _, dev, src, dst = ways[h]
                for side, to in ((0, pu), (1, pd)):
                    send(src(to, i), mid.at[h, side, i], msem.at[h, side], dev(to, q))

        for h in range(2):
            p, q, (pu, pd, pf), _, dev, src, dst = ways[h]
            for side, to in ((0, pu), (1, pd)):
                for i in range(2):
                    send(src(pf, 2 * side + i), hold1.at[h, side, i], h1sem.at[h, side], dev(to, q))
        near_pieces(0)
        near_pieces(1)
        idle()
        for h in range(2):
            p, q, (pu, pd, pf), _, dev, src, dst = ways[h]
            for side, to in ((0, pu), (1, pd)):
                held = hold1.at[h, side]
                pltpu.make_async_copy(held, held, h1sem.at[h, side]).wait()
                send(held, mid.at[h, 2, 2 * side:2 * side + 2], msem.at[h, 2 + side], dev(to, q))
        near_pieces(2)
        near_pieces(3)
        for h in range(2):
            second(h, 3, lambda qq, h=h: ways[h][5](ways[h][0], qq))
        for h in range(2):
            for side in range(2):
                got = mid.at[h, 2, 2 * side:2 * side + 2]
                pltpu.make_async_copy(got, got, msem.at[h, 2 + side]).wait()
            second(h, 2, lambda qq, h=h: mid.at[h, 2, qq])
        for side in range(2):
            for h in range(2):
                got = mid.at[h, side]
                pltpu.make_async_copy(got, got, msem.at[h, side]).wait()
                second(h, side, lambda qq, h=h, side=side: mid.at[h, side, qq])
        for o in (3, 2, 0, 1):
            for h in range(2):
                relay2(h, o)
        pltpu.make_async_copy(dst_all, dst_all, fsem).wait()
        return sends

    half_piece = quarter // 2

    def piece_ds(pos, h):
        return pl.ds(pl.multiple_of(pos * quarter + h * half_piece, half_piece), half_piece)

    def idle_first():
        for k in range(n_mat):
            for c in gcopies[k]:
                c.wait_send()
            out_copies[k].wait()
        for c in [pair_copy] + norm_copies:
            c.wait_send()

    my_mat, my_pos = mat_of(y, x), pos_of(y, x)
    col_copies = exchange(lambda py, px, h: xrow.at[mat_of(py, px), :, piece_ds(pos_of(py, px), h)],
                          lambda oy, ox, h: xfull.at[row_ds(ox * SIDE + oy), h * half_piece:(h + 1) * half_piece],
                          xfull, cmid, chold1, chold2, csend, cmsem, ch1sem, ch2sem, cfsem, idle_first)

    fy, fx = y + 1 - 2 * (y % 2), x + 1 - 2 * (x % 2)
    square = ((y, fx), (fy, x), (fy, fx))
    chunk = HALF * BLK // 4

    def chunk_ds(pos):
        return pl.ds(pl.multiple_of(pos * chunk, chunk), chunk)

    def packed_ds(core, pos):
        return pl.ds(pl.multiple_of(core * (HALF * BLK) + pos * chunk, chunk), chunk)

    bcol = min(256, quarter)

    near_x, near_y, diagonal = (pos_of(*c) for c in square)
    def pair_of(it, n):
        cs = chunk_ds((diagonal, near_x, near_y, my_pos)[n])
        return remote(part.at[it, 1 - t, cs, :], drecv.at[it, cs, :], dsend.at[it, n], drcv.at[it, n], partner)

    def reduce_of(it, n):
        py, px = square[(2, 0, 1)[n]]
        return remote(red.at[it, chunk_ds(pos_of(py, px)), :], rsrecv.at[it, n], rssend.at[it, n], rsrcv.at[it, n],
                      {'dp': py, 'fsdp': px})

    def gather_of(it, n):
        mine = agbuf.at[it, packed_ds(t, my_pos), :]
        py, px = square[n]
        return remote(mine, mine, agsend.at[it, n], agrcv.at[it, n], {'dp': py, 'fsdp': px})

    def forward_of(it, n):
        pos = my_pos if n == 0 else pos_of(*square[n - 1])
        held = agbuf.at[it, packed_ds(t, pos), :]
        return remote(held, held, fwsend.at[it, n], fwrcv.at[it, n], partner)

    def drain(it):
        for n in range(4):
            pair_of(it, n).wait_send()
            forward_of(it, n).wait_send()
        for n in range(3):
            reduce_of(it, n).wait_send()
            gather_of(it, n).wait_send()

    def half_gram(it, h):
        nt = (((1,), (1,)), ((), ()))
        pair_rows = xfull[pl.ds(pl.multiple_of(h * 2 * BLK, 2 * BLK), 2 * BLK), :]
        square_gram = lax.dot_general(pair_rows, pair_rows, nt, preferred_element_type=F32)
        cross_gram = lax.dot_general(xfull[pl.ds(pl.multiple_of(h * BLK, BLK), BLK), :], xfull[2 * BLK:, :], nt,
                                     preferred_element_type=F32)
        blocks = (square_gram[:BLK, :BLK], square_gram[:BLK, BLK:], square_gram[BLK:, BLK:],
                  cross_gram[:, :BLK], cross_gram[:, BLK:])
        for n, block in enumerate(blocks):
            part[it, h, n * BLK:(n + 1) * BLK, :] = block

    def iteration(it, carry):
        half_gram(it, 1 - t)
        for n in range(4):
            pair_of(it, n).start()
        half_gram(it, t)
        for n, pos in enumerate((diagonal, near_x, near_y, my_pos)):
            pair_of(it, n).wait_recv()
            cs = chunk_ds(pos)
            red[it, cs, :] = part[it, t, cs, :] + drecv[it, cs, :]
            if n < 3:
                reduce_of(it, n).start()

        @pl.when(it > 0)
        def _():
            drain(it - 1)

        for n in (1, 2, 0):
            reduce_of(it, n).wait_recv()
        total = (red[it, chunk_ds(my_pos), :] + rsrecv[it, 1]) + (rsrecv[it, 2] + rsrecv[it, 0])
        agbuf[it, packed_ds(t, my_pos), :] = total.astype(BF16)
        for n in (2, 0, 1):
            gather_of(it, n).start()
        forward_of(it, 0).start()
        for n in range(3):
            gather_of(it, n).wait_recv()
            forward_of(it, n + 1).start()
        for n in range(4):
            forward_of(it, n).wait_recv()
        for n, (bi, bj) in enumerate(TRI):
            block = agbuf[it, n * BLK:(n + 1) * BLK, :]
            amat[bi * BLK:(bi + 1) * BLK, bj * BLK:(bj + 1) * BLK] = block
            if bi != bj:
                amat[bj * BLK:(bj + 1) * BLK, bi * BLK:(bi + 1) * BLK] = block.astype(F32).T.astype(BF16)
        for bi in range(2):
            rs = slice(2 * BLK * bi, 2 * BLK * (bi + 1))
            sq = jnp.dot(amat[rs, :], amat[...], preferred_element_type=F32).astype(BF16)
            bmat[rs, :] = (COEF_B * amat[rs, :].astype(F32) + COEF_C * sq.astype(F32)).astype(BF16)

        for i in range(quarter // bcol):
            cs = slice(i * bcol, (i + 1) * bcol)
            x_old = xfull[:, cs]
            prod = jnp.dot(bmat[...], x_old, preferred_element_type=F32)
            xfull[:, cs] = (COEF_A * x_old.astype(F32) + prod).astype(BF16)
        return carry

    for c in col_copies:
        c.wait_send()
    lax.fori_loop(0, NS_STEPS, iteration, 0)

    back_copies = exchange(lambda py, px, h: xfull.at[row_ds(px * SIDE + py), h * half_piece:(h + 1) * half_piece],
                           lambda oy, ox, h: xfin_hbm.at[mat_of(oy, ox), :, piece_ds(pos_of(oy, ox), h)],
                           xfin_hbm, bmid, bhold1, bhold2, bsend, bmsem, bh1sem, bh2sem, bfsem, lambda: drain(NS_STEPS - 1))

    for c in back_copies:
        c.wait_send()


def run_kernel(m_blk, g_blk):
    n_mat, rows, cols = m_blk.shape
    all_rows = rows * SIDE * SIDE
    quarter = cols // SIDE
    packed = len(TRI) * BLK
    chunk = packed // 8
    n_oth = SIDE * SIDE - 1
    dma = pltpu.SemaphoreType.DMA
    half_piece = (rows, quarter // 2)
    relays = [
        pltpu.VMEM((2, 3, SIDE) + half_piece, BF16),
        pltpu.VMEM((2, 2, 2) + half_piece, BF16),
        pltpu.VMEM((2, 2, 2) + half_piece, BF16),
    ]
    relay_sems = [dma((60,)), dma((2, 4)), dma((2, 2)), dma((2, 2, 2)), dma]
    scratch = [
        pltpu.VMEM((n_mat, rows, cols), BF16),
        pltpu.VMEM((n_mat, 3, rows, cols), BF16),
        pltpu.VMEM((n_mat, 2, rows, cols // 2), BF16),
        pltpu.VMEM((n_mat, rows, cols), F32),
        pltpu.VMEM((n_mat, rows, cols), F32),
        pltpu.VMEM((n_mat, rows, cols), BF16),
        pltpu.VMEM((all_rows, quarter), BF16),
        pltpu.VMEM((8, 128), F32),
        pltpu.VMEM((8, 128), F32),
        pltpu.VMEM((SIDE * SIDE, 8, 128), F32),
        pltpu.VMEM((NS_STEPS, 2, packed // 2, BLK), F32),
        pltpu.VMEM((NS_STEPS, packed // 2, BLK), F32),
        pltpu.VMEM((NS_STEPS, packed // 2, BLK), F32),
        pltpu.VMEM((NS_STEPS, 3, chunk, BLK), F32),
        pltpu.VMEM((NS_STEPS, packed, BLK), BF16),
        pltpu.VMEM((all_rows, all_rows), BF16),
        pltpu.VMEM((all_rows, all_rows), BF16),
        *relays, *relays,
        dma((2, n_mat)), dma((n_mat,)), dma((n_mat, 6)), dma((n_mat, 6)),
        dma((n_oth + 1,)), dma((n_oth + 1,)), *relay_sems, *relay_sems,
        dma((NS_STEPS, 4)), dma((NS_STEPS, 4)), dma((NS_STEPS, 3)), dma((NS_STEPS, 3)),
        dma((NS_STEPS, 3)), dma((NS_STEPS, 3)), dma((NS_STEPS, 4)), dma((NS_STEPS, 4)), pltpu.SemaphoreType.REGULAR((3,)),
    ]
    anyspace = pl.BlockSpec(memory_space=pl.ANY)
    return pl.pallas_call(
        muon_kernel,
        out_shape=(jax.ShapeDtypeStruct(m_blk.shape, F32), jax.ShapeDtypeStruct(m_blk.shape, BF16)),
        in_specs=[anyspace, anyspace],
        out_specs=(anyspace, anyspace),
        scratch_shapes=scratch,
        compiler_params=pltpu.CompilerParams(collective_id=0, has_side_effects=True, vmem_limit_bytes=VMEM_MIB * 2 ** 20),
        name='muon_group',
    )(m_blk, g_blk)


def solution(mesh):
    mat_spec = P('stage', ROW_AXES, 'tp')
    grad_spec = P(('stage', 'dp'), None, 'fsdp', 'tp')
    tp_size = mesh.shape['tp']

    def local_step(w_blk, m_blk, g_blk):
        m_new, x_fin = run_kernel(m_blk, g_blk.reshape(g_blk.shape[1:]))
        col_count = w_blk.shape[2] * tp_size
        update_scale = LEARN_RATE * 0.2 * math.sqrt(col_count)
        decay_factor = 1.0 - LEARN_RATE * WEIGHT_DECAY
        w_new = decay_factor * w_blk - update_scale * x_fin.astype(F32)
        return w_new, m_new

    return jax.shard_map(local_step, mesh=mesh, in_specs=(mat_spec, mat_spec, grad_spec), out_specs=(mat_spec, mat_spec), check_vma=False)
```

```python
import functools
import math
import jax
import jax.numpy as jnp
from jax import lax
from jax.experimental import pallas as pl
from jax.experimental.pallas import tpu as pltpu
from jax.sharding import PartitionSpec as P

MOMENTUM = 0.95
LEARN_RATE = 0.1
WEIGHT_DECAY = 0.1
COEF_A = 3.4445
COEF_B = -4.7750
COEF_C = 2.0315
NORM_EPS = 1e-7
NS_STEPS = 5
ROW_AXES = ('fsdp', 'dp')
F32 = jnp.float32
BF16 = jnp.bfloat16
MESH = pl.DeviceIdType.MESH
VMEM_MIB = 47
SIDE = 4
BLK = 128
SUB = BLK // 2
HALF_ROWS = 3 * BLK + 3 * SUB
PLACE = ((0, 1), (1, 0), (1, 1), (0, 0))


def muon_kernel(m_hbm, g_hbm, mnew_hbm, xfin_hbm,
                gown, grecv, relay, mbuf, x0, xrow, xfull,
                nown, npair, nall, part, drecv, red, rsrecv, agbuf, amat, bmat,
                cmid, chold1, chold2, bmid, bhold1, bhold2,
                load_sem, out_sem, gsend, grcv, nsend, nrcv, csend, cmsem, ch1sem, ch2sem, cfsem,
                bsend, bmsem, bh1sem, bh2sem, bfsem,
                dsend, drcv, rssend, rsrcv, agsend, agrcv, fwsend, fwrcv, round_sem):
    n_mat, rows, cols = mbuf.shape
    quarter = cols // SIDE
    half = cols // 2
    y = lax.axis_index('dp')
    x = lax.axis_index('fsdp')
    t = lax.axis_index('tp')
    partner = {'tp': 1 - t}
    up = lax.rem(y + 1, SIDE)
    down = lax.rem(y + SIDE - 1, SIDE)
    far = lax.rem(y + 2, SIDE)

    def row_ds(i):
        return pl.ds(pl.multiple_of(i * rows, rows), rows)

    def quarter_ds(i):
        return pl.ds(pl.multiple_of(i * quarter, quarter), quarter)

    def mat_of(yy, xx):
        return (yy // 2) * 2 + xx // 2

    def pos_of(yy, xx):
        return (yy % 2) * 2 + xx % 2

    loads = []
    for k in range(n_mat):
        loads.append((pltpu.make_async_copy(g_hbm.at[k, row_ds(y), :], gown.at[k], load_sem.at[0, k]),
                      pltpu.make_async_copy(m_hbm.at[k], mbuf.at[k], load_sem.at[1, k])))
        for c in loads[-1]:
            c.start()

    others = [(oy, ox) for oy in range(SIDE) for ox in range(SIDE) if (oy, ox) != (0, 0)]

    def peer(off):
        return lax.rem(y + off[0], SIDE), lax.rem(x + off[1], SIDE)

    xup, xdown = lax.rem(x + 1, SIDE), lax.rem(x + SIDE - 1, SIDE)
    neighbours = ({'dp': up}, {'dp': down}, {'fsdp': xup}, {'fsdp': xdown})
    barrier = pltpu.get_barrier_semaphore()
    for dev in neighbours + (partner,):
        pl.semaphore_signal(barrier, inc=1, device_id=dev, device_id_type=MESH)
    pl.semaphore_wait(barrier, 5)

    def remote(src, dst, ssem, rsem, dev):
        return pltpu.make_async_remote_copy(src_ref=src, dst_ref=dst, send_sem=ssem, recv_sem=rsem,
                                            device_id=dev, device_id_type=MESH)

    lo, hi = pl.ds(0, half), pl.ds(half, half)

    def grad_copies(k):
        to_up, to_down = {'dp': up}, {'dp': down}
        return (
            remote(g_hbm.at[k, row_ds(up), :], grecv.at[k, 0], gsend.at[k, 0], grcv.at[k, 0], to_up),
            remote(g_hbm.at[k, row_ds(down), :], grecv.at[k, 1], gsend.at[k, 1], grcv.at[k, 1], to_down),
            remote(g_hbm.at[k, row_ds(far), lo], relay.at[k, 0], gsend.at[k, 2], grcv.at[k, 2], to_up),
            remote(g_hbm.at[k, row_ds(far), hi], relay.at[k, 1], gsend.at[k, 3], grcv.at[k, 3], to_down),
            remote(relay.at[k, 0], grecv.at[k, 2, :, lo], gsend.at[k, 4], grcv.at[k, 4], to_up),
            remote(relay.at[k, 1], grecv.at[k, 2, :, hi], gsend.at[k, 5], grcv.at[k, 5], to_down),
        )

    gcopies = [grad_copies(k) for k in range(n_mat)]

    def issue_grad(k):
        for j in (2, 3, 0, 1):
            gcopies[k][j].start()

    issue_grad(0)
    issue_grad(1)
    for n in range(3):
        for dev in neighbours:
            pl.semaphore_signal(round_sem.at[n], inc=1, device_id=dev, device_id_type=MESH)
        pl.semaphore_wait(round_sem.at[n], 4)
    step = min(512, cols)
    out_copies = []
    tile_rows = lax.broadcasted_iota(jnp.int32, (8, 128), 0)
    norm_tile = jnp.zeros((8, 128), F32)

    def momentum_step(k, norm_tile):
        for c in loads[k]:
            c.wait()
        for j in (0, 1, 4, 5):
            gcopies[k][j].wait_recv()

        def col_step(i, acc):
            cs = pl.ds(pl.multiple_of(i * step, step), step)
            g_sum = (gown[k, :, cs].astype(F32) + grecv[k, 0, :, cs].astype(F32)) + (
                grecv[k, 1, :, cs].astype(F32) + grecv[k, 2, :, cs].astype(F32))
            m_new = MOMENTUM * mbuf[k, :, cs] + g_sum
            mbuf[k, :, cs] = m_new
            x_zero = g_sum + MOMENTUM * m_new
            x0[k, :, cs] = x_zero
            return acc + x_zero * x_zero

        acc = lax.fori_loop(0, cols // step, col_step, jnp.zeros((rows, step), F32))
        oc = pltpu.make_async_copy(mbuf.at[k], mnew_hbm.at[k], out_sem.at[k])
        oc.start()
        out_copies.append(oc)
        return jnp.where(tile_rows == k, jnp.sum(acc), norm_tile)

    for k in range(n_mat):
        for j in (2, 3):
            gcopies[k][j].wait_recv()
            gcopies[k][j + 2].start()
        if k + 2 < n_mat:
            issue_grad(k + 2)
        if k > 0:
            norm_tile = momentum_step(k - 1, norm_tile)
    norm_tile = momentum_step(n_mat - 1, norm_tile)

    nown[...] = norm_tile
    pair_copy = remote(nown, npair, nsend.at[0], nrcv.at[0], partner)
    pair_copy.start()
    pair_copy.wait_recv()
    here = y * SIDE + x
    nall[here] = nown[...] + npair[...]
    norm_copies = []
    for n, off in enumerate(others):
        py, px = peer(off)
        c = remote(nall.at[here], nall.at[here], nsend.at[1 + n], nrcv.at[1 + n], {'dp': py, 'fsdp': px})
        c.start()
        norm_copies.append(c)
    for c in norm_copies:
        c.wait_recv()
    sq_all = jnp.sum(nall[...], axis=0)
    denom_all = jnp.sqrt(sq_all) + NORM_EPS

    for k in range(n_mat):
        denom = denom_all[k:k + 1, 0:1]

        def div_step(i, carry, k=k, denom=denom):
            cs = pl.ds(pl.multiple_of(i * step, step), step)
            xrow[k, :, cs] = (x0[k, :, cs] / denom).astype(BF16)
            return carry

        lax.fori_loop(0, cols // step, div_step, 0)

    def exchange(src_of, dst_of, dst_all, mid, hold1, hold2, ssem, msem, h1sem, h2sem, fsem, idle):
        sends = []

        def send(src, dst, rsem, dev):
            c = remote(src, dst, ssem.at[len(sends)], rsem, dev)
            c.start()
            sends.append(c)

        ways = []
        for h in range(2):
            p, q = (x, y) if h == 0 else (y, x)
            near = [(lax.rem(c + 1, SIDE), lax.rem(c + SIDE - 1, SIDE), lax.rem(c + 2, SIDE)) for c in (p, q)]

            def yx(pp, qq, h=h):
                return (qq, pp) if h == 0 else (pp, qq)

            def dev(pp, qq, yx=yx):
                return dict(zip(('dp', 'fsdp'), yx(pp, qq)))

            def src(pp, qq, h=h, yx=yx):
                return src_of(*yx(pp, qq), h)

            def dst(pp, qq, h=h, yx=yx):
                return dst_of(*yx(pp, qq), h)

            ways.append((p, q, near[0], near[1], dev, src, dst))

        def second(h, o, piece):
            p, q, (pu, pd, pf), (qu, qd, qf), dev, src, dst = ways[h]
            start_p = (pd, pu, pf, p)[o]
            side, i = PLACE[o]
            send(piece(qf), hold2.at[h, side, i], h2sem.at[h, side, i], dev(p, (qu, qd)[side]))
            send(piece(qu), dst(start_p, q), fsem, dev(p, qu))
            send(piece(qd), dst(start_p, q), fsem, dev(p, qd))
            pltpu.make_async_copy(piece(q), dst(start_p, q), fsem).start()

        def relay2(h, o):
            p, q, (pu, pd, pf), (qu, qd, qf), dev, src, dst = ways[h]
            side, i = PLACE[o]
            held = hold2.at[h, side, i]
            pltpu.make_async_copy(held, held, h2sem.at[h, side, i]).wait()
            send(held, dst((pd, pu, pf, p)[o], (qd, qu)[side]), fsem, dev(p, (qu, qd)[side]))

        def near_pieces(i):
            for h in range(2):
                p, q, (pu, pd, pf), _, dev, src, dst = ways[h]
                for side, to in ((0, pu), (1, pd)):
                    send(src(to, i), mid.at[h, side, i], msem.at[h, side], dev(to, q))

        for h in range(2):
            p, q, (pu, pd, pf), _, dev, src, dst = ways[h]
            for side, to in ((0, pu), (1, pd)):
                for i in range(2):
                    send(src(pf, 2 * side + i), hold1.at[h, side, i], h1sem.at[h, side], dev(to, q))
        near_pieces(0)
        near_pieces(1)
        idle()
        for h in range(2):
            p, q, (pu, pd, pf), _, dev, src, dst = ways[h]
            for side, to in ((0, pu), (1, pd)):
                held = hold1.at[h, side]
                pltpu.make_async_copy(held, held, h1sem.at[h, side]).wait()
                send(held, mid.at[h, 2, 2 * side:2 * side + 2], msem.at[h, 2 + side], dev(to, q))
        near_pieces(2)
        near_pieces(3)
        for h in range(2):
            second(h, 3, lambda qq, h=h: ways[h][5](ways[h][0], qq))
        for h in range(2):
            for side in range(2):
                got = mid.at[h, 2, 2 * side:2 * side + 2]
                pltpu.make_async_copy(got, got, msem.at[h, 2 + side]).wait()
            second(h, 2, lambda qq, h=h: mid.at[h, 2, qq])
        for side in range(2):
            for h in range(2):
                got = mid.at[h, side]
                pltpu.make_async_copy(got, got, msem.at[h, side]).wait()
                second(h, side, lambda qq, h=h, side=side: mid.at[h, side, qq])
        for o in (3, 2, 0, 1):
            for h in range(2):
                relay2(h, o)
        pltpu.make_async_copy(dst_all, dst_all, fsem).wait()
        return sends

    half_piece = quarter // 2

    def piece_ds(pos, h):
        return pl.ds(pl.multiple_of(pos * quarter + h * half_piece, half_piece), half_piece)

    def idle_first():
        for k in range(n_mat):
            for c in gcopies[k]:
                c.wait_send()
            out_copies[k].wait()
        for c in [pair_copy] + norm_copies:
            c.wait_send()

    my_mat, my_pos = mat_of(y, x), pos_of(y, x)
    col_copies = exchange(lambda py, px, h: xrow.at[mat_of(py, px), :, piece_ds(pos_of(py, px), h)],
                          lambda oy, ox, h: xfull.at[row_ds(ox * SIDE + oy), h * half_piece:(h + 1) * half_piece],
                          xfull, cmid, chold1, chold2, csend, cmsem, ch1sem, ch2sem, cfsem, idle_first)

    fy, fx = y + 1 - 2 * (y % 2), x + 1 - 2 * (x % 2)
    square = ((y, fx), (fy, x), (fy, fx))
    chunk = HALF_ROWS // 4

    def chunk_ds(pos):
        return pl.ds(pl.multiple_of(pos * chunk, chunk), chunk)

    def packed_ds(core, pos):
        return pl.ds(pl.multiple_of(core * HALF_ROWS + pos * chunk, chunk), chunk)

    bcol = min(256, quarter)

    near_x, near_y, diagonal = (pos_of(*c) for c in square)
    def pair_of(it, n):
        cs = chunk_ds((diagonal, near_x, near_y, my_pos)[n])
        return remote(part.at[it, 1 - t, cs, :], drecv.at[it, cs, :], dsend.at[it, n], drcv.at[it, n], partner)

    def reduce_of(it, n):
        py, px = square[(2, 0, 1)[n]]
        return remote(red.at[it, chunk_ds(pos_of(py, px)), :], rsrecv.at[it, n], rssend.at[it, n], rsrcv.at[it, n],
                      {'dp': py, 'fsdp': px})

    def gather_of(it, n):
        mine = agbuf.at[it, packed_ds(t, my_pos), :]
        py, px = square[n]
        return remote(mine, mine, agsend.at[it, n], agrcv.at[it, n], {'dp': py, 'fsdp': px})

    def forward_of(it, n):
        pos = my_pos if n == 0 else pos_of(*square[n - 1])
        held = agbuf.at[it, packed_ds(t, pos), :]
        return remote(held, held, fwsend.at[it, n], fwrcv.at[it, n], partner)

    def drain(it):
        for n in range(4):
            pair_of(it, n).wait_send()
            forward_of(it, n).wait_send()
        for n in range(3):
            reduce_of(it, n).wait_send()
            gather_of(it, n).wait_send()

    def half_gram(it, h):
        nt = (((1,), (1,)), ((), ()))
        pair_rows = xfull[pl.ds(pl.multiple_of(h * 2 * BLK, 2 * BLK), 2 * BLK), :]
        square_gram = lax.dot_general(pair_rows, pair_rows, nt, preferred_element_type=F32)
        cross_gram = lax.dot_general(xfull[pl.ds(pl.multiple_of(h * BLK, BLK), BLK), :], xfull[2 * BLK:, :], nt,
                                     preferred_element_type=F32)
        corners = jnp.where(left_lanes, pltpu.roll(square_gram[BLK + SUB:, BLK:], SUB, 1), square_gram[SUB:BLK, :BLK])
        rows_of = (square_gram[:BLK, BLK:], cross_gram[:, :BLK], cross_gram[:, BLK:],
                   square_gram[:SUB, :BLK], square_gram[BLK:BLK + SUB, BLK:], corners)
        at = 0
        for block in rows_of:
            part[it, h, at:at + block.shape[0], :] = block
            at += block.shape[0]

    left_lanes = lax.broadcasted_iota(jnp.int32, (SUB, BLK), 1) < SUB

    def assemble(it, h):
        base = h * HALF_ROWS
        for n, (bi, bj) in enumerate(((2 * h, 2 * h + 1), (h, 2), (h, 3))):
            block = agbuf[it, base + n * BLK:base + (n + 1) * BLK, :]
            amat[bi * BLK:(bi + 1) * BLK, bj * BLK:(bj + 1) * BLK] = block
            amat[bj * BLK:(bj + 1) * BLK, bi * BLK:(bi + 1) * BLK] = block.astype(F32).T.astype(BF16)
        base += 3 * BLK
        corners = agbuf[it, base + 2 * SUB:base + 3 * SUB, :].astype(F32)
        for n, corner in enumerate((corners, pltpu.roll(corners, SUB, 1))):
            lo_, mid_, hi_ = (2 * h + n) * BLK, (2 * h + n) * BLK + SUB, (2 * h + n + 1) * BLK
            upper = agbuf[it, base + n * SUB:base + (n + 1) * SUB, :]
            amat[lo_:mid_, lo_:hi_] = upper
            flipped = jnp.concatenate([upper.astype(F32), corner], axis=0).T
            amat[mid_:hi_, lo_:hi_] = jnp.where(left_lanes, flipped[SUB:, :], corner).astype(BF16)

    def iteration(it, carry):
        half_gram(it, 1 - t)
        for n in range(4):
            pair_of(it, n).start()
        half_gram(it, t)
        for n, pos in enumerate((diagonal, near_x, near_y, my_pos)):
            pair_of(it, n).wait_recv()
            cs = chunk_ds(pos)
            red[it, cs, :] = part[it, t, cs, :] + drecv[it, cs, :]
            if n < 3:
                reduce_of(it, n).start()

        @pl.when(it > 0)
        def _():
            drain(it - 1)

        for n in (1, 2, 0):
            reduce_of(it, n).wait_recv()
        total = (red[it, chunk_ds(my_pos), :] + rsrecv[it, 1]) + (rsrecv[it, 2] + rsrecv[it, 0])
        agbuf[it, packed_ds(t, my_pos), :] = total.astype(BF16)
        for n in (2, 0, 1):
            gather_of(it, n).start()
        forward_of(it, 0).start()
        for n in range(3):
            gather_of(it, n).wait_recv()
            forward_of(it, n + 1).start()
        for n in range(4):
            forward_of(it, n).wait_recv()
        assemble(it, 0)
        assemble(it, 1)
        for bi in range(2):
            rs = slice(2 * BLK * bi, 2 * BLK * (bi + 1))
            sq = jnp.dot(amat[rs, :], amat[...], preferred_element_type=F32).astype(BF16)
            bmat[rs, :] = (COEF_B * amat[rs, :].astype(F32) + COEF_C * sq.astype(F32)).astype(BF16)

        for i in range(quarter // bcol):
            cs = slice(i * bcol, (i + 1) * bcol)
            x_old = xfull[:, cs]
            prod = jnp.dot(bmat[...], x_old, preferred_element_type=F32)
            xfull[:, cs] = (COEF_A * x_old.astype(F32) + prod).astype(BF16)
        return carry

    for c in col_copies:
        c.wait_send()
    lax.fori_loop(0, NS_STEPS, iteration, 0)

    back_copies = exchange(lambda py, px, h: xfull.at[row_ds(px * SIDE + py), h * half_piece:(h + 1) * half_piece],
                           lambda oy, ox, h: xfin_hbm.at[mat_of(oy, ox), :, piece_ds(pos_of(oy, ox), h)],
                           xfin_hbm, bmid, bhold1, bhold2, bsend, bmsem, bh1sem, bh2sem, bfsem, lambda: drain(NS_STEPS - 1))

    for c in back_copies:
        c.wait_send()


def run_kernel(m_blk, g_blk):
    n_mat, rows, cols = m_blk.shape
    all_rows = rows * SIDE * SIDE
    quarter = cols // SIDE
    packed = 2 * HALF_ROWS
    chunk = packed // 8
    n_oth = SIDE * SIDE - 1
    dma = pltpu.SemaphoreType.DMA
    half_piece = (rows, quarter // 2)
    relays = [
        pltpu.VMEM((2, 3, SIDE) + half_piece, BF16),
        pltpu.VMEM((2, 2, 2) + half_piece, BF16),
        pltpu.VMEM((2, 2, 2) + half_piece, BF16),
    ]
    relay_sems = [dma((60,)), dma((2, 4)), dma((2, 2)), dma((2, 2, 2)), dma]
    scratch = [
        pltpu.VMEM((n_mat, rows, cols), BF16),
        pltpu.VMEM((n_mat, 3, rows, cols), BF16),
        pltpu.VMEM((n_mat, 2, rows, cols // 2), BF16),
        pltpu.VMEM((n_mat, rows, cols), F32),
        pltpu.VMEM((n_mat, rows, cols), F32),
        pltpu.VMEM((n_mat, rows, cols), BF16),
        pltpu.VMEM((all_rows, quarter), BF16),
        pltpu.VMEM((8, 128), F32),
        pltpu.VMEM((8, 128), F32),
        pltpu.VMEM((SIDE * SIDE, 8, 128), F32),
        pltpu.VMEM((NS_STEPS, 2, packed // 2, BLK), F32),
        pltpu.VMEM((NS_STEPS, packed // 2, BLK), F32),
        pltpu.VMEM((NS_STEPS, packed // 2, BLK), F32),
        pltpu.VMEM((NS_STEPS, 3, chunk, BLK), F32),
        pltpu.VMEM((NS_STEPS, packed, BLK), BF16),
        pltpu.VMEM((all_rows, all_rows), BF16),
        pltpu.VMEM((all_rows, all_rows), BF16),
        *relays, *relays,
        dma((2, n_mat)), dma((n_mat,)), dma((n_mat, 6)), dma((n_mat, 6)),
        dma((n_oth + 1,)), dma((n_oth + 1,)), *relay_sems, *relay_sems,
        dma((NS_STEPS, 4)), dma((NS_STEPS, 4)), dma((NS_STEPS, 3)), dma((NS_STEPS, 3)),
        dma((NS_STEPS, 3)), dma((NS_STEPS, 3)), dma((NS_STEPS, 4)), dma((NS_STEPS, 4)), pltpu.SemaphoreType.REGULAR((3,)),
    ]
    anyspace = pl.BlockSpec(memory_space=pl.ANY)
    return pl.pallas_call(
        muon_kernel,
        out_shape=(jax.ShapeDtypeStruct(m_blk.shape, F32), jax.ShapeDtypeStruct(m_blk.shape, BF16)),
        in_specs=[anyspace, anyspace],
        out_specs=(anyspace, anyspace),
        scratch_shapes=scratch,
        compiler_params=pltpu.CompilerParams(collective_id=0, has_side_effects=True, vmem_limit_bytes=VMEM_MIB * 2 ** 20),
        name='muon_group',
    )(m_blk, g_blk)


def solution(mesh):
    mat_spec = P('stage', ROW_AXES, 'tp')
    grad_spec = P(('stage', 'dp'), None, 'fsdp', 'tp')
    tp_size = mesh.shape['tp']

    def local_step(w_blk, m_blk, g_blk):
        m_new, x_fin = run_kernel(m_blk, g_blk.reshape(g_blk.shape[1:]))
        col_count = w_blk.shape[2] * tp_size
        update_scale = LEARN_RATE * 0.2 * math.sqrt(col_count)
        decay_factor = 1.0 - LEARN_RATE * WEIGHT_DECAY
        w_new = decay_factor * w_blk - update_scale * x_fin.astype(F32)
        return w_new, m_new

    return jax.shard_map(local_step, mesh=mesh, in_specs=(mat_spec, mat_spec, grad_spec), out_specs=(mat_spec, mat_spec), check_vma=False)
```

```python
import functools
import math
import jax
import jax.numpy as jnp
from jax import lax
from jax.experimental import pallas as pl
from jax.experimental.pallas import tpu as pltpu
from jax.sharding import PartitionSpec as P

MOMENTUM = 0.95
LEARN_RATE = 0.1
WEIGHT_DECAY = 0.1
COEF_A = 3.4445
COEF_B = -4.7750
COEF_C = 2.0315
NORM_EPS = 1e-7
NS_STEPS = 5
ROW_AXES = ('fsdp', 'dp')
F32 = jnp.float32
BF16 = jnp.bfloat16
MESH = pl.DeviceIdType.MESH
VMEM_MIB = 47
SIDE = 4
BLK = 128
SUB = BLK // 2
HALF_ROWS = 3 * BLK + 3 * SUB
PLACE = ((0, 1), (1, 0), (1, 1), (0, 0))


def muon_kernel(m_hbm, g_hbm, mnew_hbm, xfin_hbm,
                gown, grecv, relay, mbuf, x0, xrow, xfull,
                nown, npair, nall, part, drecv, red, rsrecv, agbuf, amat, bmat,
                cmid, chold1, chold2, bmid, bhold1, bhold2,
                load_sem, out_sem, gsend, grcv, nsend, nrcv, csend, cmsem, ch1sem, ch2sem, cfsem,
                bsend, bmsem, bh1sem, bh2sem, bfsem,
                dsend, drcv, rssend, rsrcv, agsend, agrcv, fwsend, fwrcv, round_sem):
    n_mat, rows, cols = mbuf.shape
    quarter = cols // SIDE
    half = cols // 2
    y = lax.axis_index('dp')
    x = lax.axis_index('fsdp')
    t = lax.axis_index('tp')
    partner = {'tp': 1 - t}
    up = lax.rem(y + 1, SIDE)
    down = lax.rem(y + SIDE - 1, SIDE)
    far = lax.rem(y + 2, SIDE)

    def row_ds(i):
        return pl.ds(pl.multiple_of(i * rows, rows), rows)

    def quarter_ds(i):
        return pl.ds(pl.multiple_of(i * quarter, quarter), quarter)

    def mat_of(yy, xx):
        return (yy // 2) * 2 + xx // 2

    def pos_of(yy, xx):
        return (yy % 2) * 2 + xx % 2

    loads = []
    for k in range(n_mat):
        loads.append((pltpu.make_async_copy(g_hbm.at[k, row_ds(y), :], gown.at[k], load_sem.at[0, k]),
                      pltpu.make_async_copy(m_hbm.at[k], mbuf.at[k], load_sem.at[1, k])))
        for c in loads[-1]:
            c.start()

    others = [(oy, ox) for oy in range(SIDE) for ox in range(SIDE) if (oy, ox) != (0, 0)]

    def peer(off):
        return lax.rem(y + off[0], SIDE), lax.rem(x + off[1], SIDE)

    xup, xdown = lax.rem(x + 1, SIDE), lax.rem(x + SIDE - 1, SIDE)
    neighbours = ({'dp': up}, {'dp': down}, {'fsdp': xup}, {'fsdp': xdown})
    barrier = pltpu.get_barrier_semaphore()
    for dev in neighbours + (partner,):
        pl.semaphore_signal(barrier, inc=1, device_id=dev, device_id_type=MESH)
    pl.semaphore_wait(barrier, 5)

    def remote(src, dst, ssem, rsem, dev):
        return pltpu.make_async_remote_copy(src_ref=src, dst_ref=dst, send_sem=ssem, recv_sem=rsem,
                                            device_id=dev, device_id_type=MESH)

    lo, hi = pl.ds(0, half), pl.ds(half, half)

    def grad_copies(k):
        to_up, to_down = {'dp': up}, {'dp': down}
        return (
            remote(g_hbm.at[k, row_ds(up), :], grecv.at[k, 0], gsend.at[k, 0], grcv.at[k, 0], to_up),
            remote(g_hbm.at[k, row_ds(down), :], grecv.at[k, 1], gsend.at[k, 1], grcv.at[k, 1], to_down),
            remote(g_hbm.at[k, row_ds(far), lo], relay.at[k, 0], gsend.at[k, 2], grcv.at[k, 2], to_up),
            remote(g_hbm.at[k, row_ds(far), hi], relay.at[k, 1], gsend.at[k, 3], grcv.at[k, 3], to_down),
            remote(relay.at[k, 0], grecv.at[k, 2, :, lo], gsend.at[k, 4], grcv.at[k, 4], to_up),
            remote(relay.at[k, 1], grecv.at[k, 2, :, hi], gsend.at[k, 5], grcv.at[k, 5], to_down),
        )

    gcopies = [grad_copies(k) for k in range(n_mat)]

    def issue_grad(k):
        for j in (2, 3, 0, 1):
            gcopies[k][j].start()

    issue_grad(0)
    issue_grad(1)
    for n in range(3):
        for dev in neighbours:
            pl.semaphore_signal(round_sem.at[n], inc=1, device_id=dev, device_id_type=MESH)
        pl.semaphore_wait(round_sem.at[n], 4)
    step = min(512, cols)
    out_copies = []
    tile_rows = lax.broadcasted_iota(jnp.int32, (8, 128), 0)
    norm_tile = jnp.zeros((8, 128), F32)

    def momentum_step(k, norm_tile):
        for c in loads[k]:
            c.wait()
        for j in (0, 1, 4, 5):
            gcopies[k][j].wait_recv()

        def col_step(i, acc):
            cs = pl.ds(pl.multiple_of(i * step, step), step)
            g_sum = (gown[k, :, cs].astype(F32) + grecv[k, 0, :, cs].astype(F32)) + (
                grecv[k, 1, :, cs].astype(F32) + grecv[k, 2, :, cs].astype(F32))
            m_new = MOMENTUM * mbuf[k, :, cs] + g_sum
            mbuf[k, :, cs] = m_new
            x_zero = g_sum + MOMENTUM * m_new
            x0[k, :, cs] = x_zero
            return acc + x_zero * x_zero

        acc = lax.fori_loop(0, cols // step, col_step, jnp.zeros((rows, step), F32))
        oc = pltpu.make_async_copy(mbuf.at[k], mnew_hbm.at[k], out_sem.at[k])
        oc.start()
        out_copies.append(oc)
        return jnp.where(tile_rows == k, jnp.sum(acc), norm_tile)

    for k in range(n_mat):
        for j in (2, 3):
            gcopies[k][j].wait_recv()
            gcopies[k][j + 2].start()
        if k + 2 < n_mat:
            issue_grad(k + 2)
        if k > 0:
            norm_tile = momentum_step(k - 1, norm_tile)
    norm_tile = momentum_step(n_mat - 1, norm_tile)

    nown[...] = norm_tile
    pair_copy = remote(nown, npair, nsend.at[0], nrcv.at[0], partner)
    pair_copy.start()
    pair_copy.wait_recv()
    here = y * SIDE + x
    nall[here] = nown[...] + npair[...]
    norm_copies = []
    for n, off in enumerate(sorted(others, key=lambda o: -sum(min(c, SIDE - c) for c in o))):
        py, px = peer(off)
        c = remote(nall.at[here], nall.at[here], nsend.at[1 + n], nrcv.at[1 + n], {'dp': py, 'fsdp': px})
        c.start()
        norm_copies.append(c)
    for c in norm_copies:
        c.wait_recv()
    sq_all = jnp.sum(nall[...], axis=0)
    denom_all = jnp.sqrt(sq_all) + NORM_EPS

    for k in range(n_mat):
        denom = denom_all[k:k + 1, 0:1]

        def div_step(i, carry, k=k, denom=denom):
            cs = pl.ds(pl.multiple_of(i * step, step), step)
            xrow[k, :, cs] = (x0[k, :, cs] / denom).astype(BF16)
            return carry

        lax.fori_loop(0, cols // step, div_step, 0)

    def exchange(src_of, dst_of, dst_all, mid, hold1, hold2, ssem, msem, h1sem, h2sem, fsem, idle):
        sends = []

        def send(src, dst, rsem, dev):
            c = remote(src, dst, ssem.at[len(sends)], rsem, dev)
            c.start()
            sends.append(c)

        ways = []
        for h in range(2):
            p, q = (x, y) if h == 0 else (y, x)
            near = [(lax.rem(c + 1, SIDE), lax.rem(c + SIDE - 1, SIDE), lax.rem(c + 2, SIDE)) for c in (p, q)]

            def yx(pp, qq, h=h):
                return (qq, pp) if h == 0 else (pp, qq)

            def dev(pp, qq, yx=yx):
                return dict(zip(('dp', 'fsdp'), yx(pp, qq)))

            def src(pp, qq, h=h, yx=yx):
                return src_of(*yx(pp, qq), h)

            def dst(pp, qq, h=h, yx=yx):
                return dst_of(*yx(pp, qq), h)

            ways.append((p, q, near[0], near[1], dev, src, dst))

        def second(h, o, piece):
            p, q, (pu, pd, pf), (qu, qd, qf), dev, src, dst = ways[h]
            start_p = (pd, pu, pf, p)[o]
            side, i = PLACE[o]
            send(piece(qf), hold2.at[h, side, i], h2sem.at[h, side, i], dev(p, (qu, qd)[side]))
            send(piece(qu), dst(start_p, q), fsem, dev(p, qu))
            send(piece(qd), dst(start_p, q), fsem, dev(p, qd))
            pltpu.make_async_copy(piece(q), dst(start_p, q), fsem).start()

        def relay2(h, o):
            p, q, (pu, pd, pf), (qu, qd, qf), dev, src, dst = ways[h]
            side, i = PLACE[o]
            held = hold2.at[h, side, i]
            pltpu.make_async_copy(held, held, h2sem.at[h, side, i]).wait()
            send(held, dst((pd, pu, pf, p)[o], (qd, qu)[side]), fsem, dev(p, (qu, qd)[side]))

        def near_pieces(i):
            for h in range(2):
                p, q, (pu, pd, pf), _, dev, src, dst = ways[h]
                for side, to in ((0, pu), (1, pd)):
                    send(src(to, i), mid.at[h, side, i], msem.at[h, side], dev(to, q))

        for h in range(2):
            p, q, (pu, pd, pf), _, dev, src, dst = ways[h]
            for side, to in ((0, pu), (1, pd)):
                for i in range(2):
                    send(src(pf, 2 * side + i), hold1.at[h, side, i], h1sem.at[h, side], dev(to, q))
        near_pieces(0)
        near_pieces(1)
        idle()
        for h in range(2):
            p, q, (pu, pd, pf), _, dev, src, dst = ways[h]
            for side, to in ((0, pu), (1, pd)):
                held = hold1.at[h, side]
                pltpu.make_async_copy(held, held, h1sem.at[h, side]).wait()
                send(held, mid.at[h, 2, 2 * side:2 * side + 2], msem.at[h, 2 + side], dev(to, q))
        near_pieces(2)
        near_pieces(3)
        for h in range(2):
            second(h, 3, lambda qq, h=h: ways[h][5](ways[h][0], qq))
        for h in range(2):
            for side in range(2):
                got = mid.at[h, 2, 2 * side:2 * side + 2]
                pltpu.make_async_copy(got, got, msem.at[h, 2 + side]).wait()
            second(h, 2, lambda qq, h=h: mid.at[h, 2, qq])
        for side in range(2):
            for h in range(2):
                got = mid.at[h, side]
                pltpu.make_async_copy(got, got, msem.at[h, side]).wait()
                second(h, side, lambda qq, h=h, side=side: mid.at[h, side, qq])
        for o in (3, 2, 0, 1):
            for h in range(2):
                relay2(h, o)
        pltpu.make_async_copy(dst_all, dst_all, fsem).wait()
        return sends

    half_piece = quarter // 2

    def piece_ds(pos, h):
        return pl.ds(pl.multiple_of(pos * quarter + h * half_piece, half_piece), half_piece)

    def idle_first():
        for k in range(n_mat):
            for c in gcopies[k]:
                c.wait_send()
            out_copies[k].wait()
        for c in [pair_copy] + norm_copies:
            c.wait_send()

    my_mat, my_pos = mat_of(y, x), pos_of(y, x)
    col_copies = exchange(lambda py, px, h: xrow.at[mat_of(py, px), :, piece_ds(pos_of(py, px), h)],
                          lambda oy, ox, h: xfull.at[row_ds(ox * SIDE + oy), h * half_piece:(h + 1) * half_piece],
                          xfull, cmid, chold1, chold2, csend, cmsem, ch1sem, ch2sem, cfsem, idle_first)

    fy, fx = y + 1 - 2 * (y % 2), x + 1 - 2 * (x % 2)
    square = ((y, fx), (fy, x), (fy, fx))
    chunk = HALF_ROWS // 4

    def chunk_ds(pos):
        return pl.ds(pl.multiple_of(pos * chunk, chunk), chunk)

    def packed_ds(core, pos):
        return pl.ds(pl.multiple_of(core * HALF_ROWS + pos * chunk, chunk), chunk)

    bcol = min(256, quarter)

    near_x, near_y, diagonal = (pos_of(*c) for c in square)
    def pair_of(it, n):
        cs = chunk_ds((diagonal, near_x, near_y, my_pos)[n])
        return remote(part.at[it, 1 - t, cs, :], drecv.at[it, cs, :], dsend.at[it, n], drcv.at[it, n], partner)

    def reduce_of(it, n):
        py, px = square[(2, 0, 1)[n]]
        return remote(red.at[it, chunk_ds(pos_of(py, px)), :], rsrecv.at[it, n], rssend.at[it, n], rsrcv.at[it, n],
                      {'dp': py, 'fsdp': px})

    def gather_of(it, n):
        mine = agbuf.at[it, packed_ds(t, my_pos), :]
        py, px = square[n]
        return remote(mine, mine, agsend.at[it, n], agrcv.at[it, n], {'dp': py, 'fsdp': px})

    def forward_of(it, n):
        pos = my_pos if n == 0 else pos_of(*square[n - 1])
        held = agbuf.at[it, packed_ds(t, pos), :]
        return remote(held, held, fwsend.at[it, n], fwrcv.at[it, n], partner)

    def drain(it):
        for n in range(4):
            pair_of(it, n).wait_send()
            forward_of(it, n).wait_send()
        for n in range(3):
            reduce_of(it, n).wait_send()
            gather_of(it, n).wait_send()

    def half_gram(it, h):
        nt = (((1,), (1,)), ((), ()))
        pair_rows = xfull[pl.ds(pl.multiple_of(h * 2 * BLK, 2 * BLK), 2 * BLK), :]
        square_gram = lax.dot_general(pair_rows, pair_rows, nt, preferred_element_type=F32)
        cross_gram = lax.dot_general(xfull[pl.ds(pl.multiple_of(h * BLK, BLK), BLK), :], xfull[2 * BLK:, :], nt,
                                     preferred_element_type=F32)
        corners = jnp.where(left_lanes, pltpu.roll(square_gram[BLK + SUB:, BLK:], SUB, 1), square_gram[SUB:BLK, :BLK])
        rows_of = (square_gram[:BLK, BLK:], cross_gram[:, :BLK], cross_gram[:, BLK:],
                   square_gram[:SUB, :BLK], square_gram[BLK:BLK + SUB, BLK:], corners)
        at = 0
        for block in rows_of:
            part[it, h, at:at + block.shape[0], :] = block
            at += block.shape[0]

    left_lanes = lax.broadcasted_iota(jnp.int32, (SUB, BLK), 1) < SUB

    def assemble(it, h):
        base = h * HALF_ROWS
        for n, (bi, bj) in enumerate(((2 * h, 2 * h + 1), (h, 2), (h, 3))):
            block = agbuf[it, base + n * BLK:base + (n + 1) * BLK, :]
            amat[bi * BLK:(bi + 1) * BLK, bj * BLK:(bj + 1) * BLK] = block
            amat[bj * BLK:(bj + 1) * BLK, bi * BLK:(bi + 1) * BLK] = block.astype(F32).T.astype(BF16)
        base += 3 * BLK
        corners = agbuf[it, base + 2 * SUB:base + 3 * SUB, :].astype(F32)
        for n, corner in enumerate((corners, pltpu.roll(corners, SUB, 1))):
            lo_, mid_, hi_ = (2 * h + n) * BLK, (2 * h + n) * BLK + SUB, (2 * h + n + 1) * BLK
            upper = agbuf[it, base + n * SUB:base + (n + 1) * SUB, :]
            amat[lo_:mid_, lo_:hi_] = upper
            flipped = jnp.concatenate([upper.astype(F32), corner], axis=0).T
            amat[mid_:hi_, lo_:hi_] = jnp.where(left_lanes, flipped[SUB:, :], corner).astype(BF16)

    def iteration(it, carry):
        half_gram(it, 1 - t)
        for n in range(4):
            pair_of(it, n).start()
        half_gram(it, t)
        for n, pos in enumerate((diagonal, near_x, near_y, my_pos)):
            pair_of(it, n).wait_recv()
            cs = chunk_ds(pos)
            red[it, cs, :] = part[it, t, cs, :] + drecv[it, cs, :]
            if n < 3:
                reduce_of(it, n).start()

        @pl.when(it > 0)
        def _():
            drain(it - 1)

        for n in (1, 2, 0):
            reduce_of(it, n).wait_recv()
        total = (red[it, chunk_ds(my_pos), :] + rsrecv[it, 1]) + (rsrecv[it, 2] + rsrecv[it, 0])
        agbuf[it, packed_ds(t, my_pos), :] = total.astype(BF16)
        for n in (2, 0, 1):
            gather_of(it, n).start()
        forward_of(it, 0).start()
        for n in range(3):
            gather_of(it, n).wait_recv()
            forward_of(it, n + 1).start()
        for n in range(4):
            forward_of(it, n).wait_recv()
        assemble(it, 0)
        assemble(it, 1)
        for bi in range(2):
            rs = slice(2 * BLK * bi, 2 * BLK * (bi + 1))
            sq = jnp.dot(amat[rs, :], amat[...], preferred_element_type=F32).astype(BF16)
            bmat[rs, :] = (COEF_B * amat[rs, :].astype(F32) + COEF_C * sq.astype(F32)).astype(BF16)

        for i in range(quarter // bcol):
            cs = slice(i * bcol, (i + 1) * bcol)
            x_old = xfull[:, cs]
            prod = jnp.dot(bmat[...], x_old, preferred_element_type=F32)
            xfull[:, cs] = (COEF_A * x_old.astype(F32) + prod).astype(BF16)
        return carry

    for c in col_copies:
        c.wait_send()
    lax.fori_loop(0, NS_STEPS, iteration, 0)

    back_copies = exchange(lambda py, px, h: xfull.at[row_ds(px * SIDE + py), h * half_piece:(h + 1) * half_piece],
                           lambda oy, ox, h: xfin_hbm.at[mat_of(oy, ox), :, piece_ds(pos_of(oy, ox), h)],
                           xfin_hbm, bmid, bhold1, bhold2, bsend, bmsem, bh1sem, bh2sem, bfsem, lambda: drain(NS_STEPS - 1))

    for c in back_copies:
        c.wait_send()


def run_kernel(m_blk, g_blk):
    n_mat, rows, cols = m_blk.shape
    all_rows = rows * SIDE * SIDE
    quarter = cols // SIDE
    packed = 2 * HALF_ROWS
    chunk = packed // 8
    n_oth = SIDE * SIDE - 1
    dma = pltpu.SemaphoreType.DMA
    half_piece = (rows, quarter // 2)
    relays = [
        pltpu.VMEM((2, 3, SIDE) + half_piece, BF16),
        pltpu.VMEM((2, 2, 2) + half_piece, BF16),
        pltpu.VMEM((2, 2, 2) + half_piece, BF16),
    ]
    relay_sems = [dma((60,)), dma((2, 4)), dma((2, 2)), dma((2, 2, 2)), dma]
    scratch = [
        pltpu.VMEM((n_mat, rows, cols), BF16),
        pltpu.VMEM((n_mat, 3, rows, cols), BF16),
        pltpu.VMEM((n_mat, 2, rows, cols // 2), BF16),
        pltpu.VMEM((n_mat, rows, cols), F32),
        pltpu.VMEM((n_mat, rows, cols), F32),
        pltpu.VMEM((n_mat, rows, cols), BF16),
        pltpu.VMEM((all_rows, quarter), BF16),
        pltpu.VMEM((8, 128), F32),
        pltpu.VMEM((8, 128), F32),
        pltpu.VMEM((SIDE * SIDE, 8, 128), F32),
        pltpu.VMEM((NS_STEPS, 2, packed // 2, BLK), F32),
        pltpu.VMEM((NS_STEPS, packed // 2, BLK), F32),
        pltpu.VMEM((NS_STEPS, packed // 2, BLK), F32),
        pltpu.VMEM((NS_STEPS, 3, chunk, BLK), F32),
        pltpu.VMEM((NS_STEPS, packed, BLK), BF16),
        pltpu.VMEM((all_rows, all_rows), BF16),
        pltpu.VMEM((all_rows, all_rows), BF16),
        *relays, *relays,
        dma((2, n_mat)), dma((n_mat,)), dma((n_mat, 6)), dma((n_mat, 6)),
        dma((n_oth + 1,)), dma((n_oth + 1,)), *relay_sems, *relay_sems,
        dma((NS_STEPS, 4)), dma((NS_STEPS, 4)), dma((NS_STEPS, 3)), dma((NS_STEPS, 3)),
        dma((NS_STEPS, 3)), dma((NS_STEPS, 3)), dma((NS_STEPS, 4)), dma((NS_STEPS, 4)), pltpu.SemaphoreType.REGULAR((3,)),
    ]
    anyspace = pl.BlockSpec(memory_space=pl.ANY)
    return pl.pallas_call(
        muon_kernel,
        out_shape=(jax.ShapeDtypeStruct(m_blk.shape, F32), jax.ShapeDtypeStruct(m_blk.shape, BF16)),
        in_specs=[anyspace, anyspace],
        out_specs=(anyspace, anyspace),
        scratch_shapes=scratch,
        compiler_params=pltpu.CompilerParams(collective_id=0, has_side_effects=True, vmem_limit_bytes=VMEM_MIB * 2 ** 20),
        name='muon_group',
    )(m_blk, g_blk)


def solution(mesh):
    mat_spec = P('stage', ROW_AXES, 'tp')
    grad_spec = P(('stage', 'dp'), None, 'fsdp', 'tp')
    tp_size = mesh.shape['tp']

    def local_step(w_blk, m_blk, g_blk):
        m_new, x_fin = run_kernel(m_blk, g_blk.reshape(g_blk.shape[1:]))
        col_count = w_blk.shape[2] * tp_size
        update_scale = LEARN_RATE * 0.2 * math.sqrt(col_count)
        decay_factor = 1.0 - LEARN_RATE * WEIGHT_DECAY
        w_new = decay_factor * w_blk - update_scale * x_fin.astype(F32)
        return w_new, m_new

    return jax.shard_map(local_step, mesh=mesh, in_specs=(mat_spec, mat_spec, grad_spec), out_specs=(mat_spec, mat_spec), check_vma=False)
```
